128 devices in a mesh: replica: 16 (over z, y), model: 8 (over x, core).
Axes of the slice: x: 4, y: 4, z: 4, core: 2. Of those that a mesh axis runs over, the one named last changes fastest.
Arguments:
- slope_up: float32 [16, 1024, 4096], P('replica', None, 'model'), may hold values from -4 to 4
- slope_down: float32 [16, 4096, 1024], P('replica', 'model'), may hold values from -4 to 4
- slope_query: float32 [16, 1024, 1024], P('replica', None, 'model'), may hold values from -4 to 4
- slope_key: float32 [16, 1024, 1024], P('replica', None, 'model'), may hold values from -4 to 4
- slope_value: float32 [16, 1024, 1024], P('replica', None, 'model'), may hold values from -4 to 4
- slope_mixed: float32 [16, 1024, 1024], P('replica', 'model'), may hold values from -4 to 4
- slope_norm: float32 [16, 1024], P('replica'), may hold values from -8 to 8
- slope_bias: float32 [16, 1024], P('replica'), may hold values from -8 to 8
- param_up: float32 [1024, 4096], P('replica', 'model'), may hold values from -0.25 to 0.25
- param_down: float32 [4096, 1024], P('model', 'replica'), may hold values from -0.125 to 0.125
- param_query: float32 [1024, 1024], P('replica', 'model'), may hold values from -0.25 to 0.25
- param_key: float32 [1024, 1024], P('replica', 'model'), may hold values from -0.25 to 0.25
- param_value: float32 [1024, 1024], P('replica', 'model'), may hold values from -0.25 to 0.25
- param_mixed: float32 [1024, 1024], P('model', 'replica'), may hold values from -0.25 to 0.25
- param_norm: float32 [1024], P('replica'), may hold values from 0.25 to 1.75
- param_bias: float32 [1024], P('replica'), may hold values from -3 to 3
- state_up: float32 [1024, 4096], P('replica', 'model'), may hold values from 0.0001953125 to 0.001953125
- state_down: float32 [4096, 1024], P('model', 'replica'), may hold values from 4.8828126e-05 to 0.00048828125
- state_query: float32 [1024, 1024], P('replica', 'model'), may hold values from 0.0001953125 to 0.001953125
- state_key: float32 [1024, 1024], P('replica', 'model'), may hold values from 0.0001953125 to 0.001953125
- state_value: float32 [1024, 1024], P('replica', 'model'), may hold values from 0.0001953125 to 0.001953125
- state_mixed: float32 [1024, 1024], P('model', 'replica'), may hold values from 0.0001953125 to 0.001953125
- state_norm: float32 [1024], P('replica'), may hold values from 0.05 to 0.8
- state_bias: float32 [1024], P('replica'), may hold values from 0.05 to 0.8
Outputs:
- half_up: bfloat16 [1024, 4096], P(None, 'model')
- half_down: bfloat16 [4096, 1024], P('model')
- half_query: bfloat16 [1024, 1024], P(None, 'model')
- half_key: bfloat16 [1024, 1024], P(None, 'model')
- half_value: bfloat16 [1024, 1024], P(None, 'model')
- half_mixed: bfloat16 [1024, 1024], P('model')
- half_norm: bfloat16 [1024], replicated
- half_bias: bfloat16 [1024], replicated
- next_up: float32 [1024, 4096], P('replica', 'model')
- next_down: float32 [4096, 1024], P('model', 'replica')
- next_query: float32 [1024, 1024], P('replica', 'model')
- next_key: float32 [1024, 1024], P('replica', 'model')
- next_value: float32 [1024, 1024], P('replica', 'model')
- next_mixed: float32 [1024, 1024], P('model', 'replica')
- next_norm: float32 [1024], P('replica')
- next_bias: float32 [1024], P('replica')
- state_new_up: float32 [1024, 4096], P('replica', 'model')
- state_new_down: float32 [4096, 1024], P('model', 'replica')
- state_new_query: float32 [1024, 1024], P('replica', 'model')
- state_new_key: float32 [1024, 1024], P('replica', 'model')
- state_new_value: float32 [1024, 1024], P('replica', 'model')
- state_new_mixed: float32 [1024, 1024], P('model', 'replica')
- state_new_norm: float32 [1024], P('replica')
- state_new_bias: float32 [1024], P('replica')
The draws below stay inside these ranges and needn't reach their ends.
All inputs are finite; a program needn't handle non-finite values.
Results may differ from the reference program's by a relative error of at most 0.001.
Values may be sent and summed in bfloat16 or wider, within the bound.
A program may use at most 64 MiB of HBM per device.

```python
import jax
import jax.numpy as jnp
from jax import lax

WIDTH = 1024
INNER = 4096
ATTN = 1024
REPLICAS = 16


def strengthened(drawn, own_key, source, target, parts, factor):
    owner, partner = [(jnp.arange(drawn.shape[axis_at]) // (drawn.shape[axis_at] // parts)).reshape([-1 if axis == axis_at else 1 for axis in range(drawn.ndim)]) for axis_at in (source, target)]
    chosen = jax.random.permutation(own_key, parts)[partner]
    strong = (owner == chosen) | (owner == (partner + parts // 2) % parts)
    return jnp.where(strong, factor * drawn, drawn)


def shard_levels(rng, dims, split, least, top_value):
    level, own = 1.0, jax.random.fold_in(rng, 6)
    for axis_at, blocks in split:
        heights = jnp.exp(jax.random.uniform(jax.random.fold_in(own, axis_at), (blocks,), jnp.float32, least / len(split), top_value / len(split)))
        level = level * jnp.repeat(heights, dims[axis_at] // blocks).reshape([-1 if axis == axis_at else 1 for axis in range(len(dims))])
    return level


def noise(own_key, shape, scale, reach, shards=(), kind=jnp.bfloat16):
    loudness = shard_levels(own_key, shape, shards, -0.22, 0.18) if shards else 1.0
    drawn = jax.random.normal(own_key, shape, jnp.float32) * scale * loudness
    return jnp.minimum(jnp.maximum(drawn, -reach), reach).astype(kind)


def heavy_noise(stream_key, dims, deviation, most, cuts, heavy, kind=jnp.bfloat16):
    array = deviation * jax.random.normal(stream_key, dims, jnp.float32)
    if cuts:
        array = array * shard_levels(stream_key, dims, cuts, -0.22, 0.18)
    return jnp.clip(strengthened(array, jax.random.fold_in(stream_key, 3), *heavy), -most, most).astype(kind)


def setup_inputs(seed: int = 0) -> dict:
    key_of = jax.random.split(jax.random.key(seed), 25)
    return {
        "slope_up": heavy_noise(key_of[0], (REPLICAS, WIDTH, INNER), 0.5, 4.0, ((0, 16), (2, 8)), (0, 1, 16, 2.0), jnp.float32),
        "slope_down": heavy_noise(key_of[1], (REPLICAS, INNER, WIDTH), 0.5, 4.0, ((0, 16), (1, 8)), (0, 2, 16, 2.0), jnp.float32),
        "slope_query": heavy_noise(key_of[2], (REPLICAS, WIDTH, ATTN), 0.5, 4.0, ((0, 16), (2, 8)), (0, 1, 16, 2.0), jnp.float32),
        "slope_key": heavy_noise(key_of[3], (REPLICAS, WIDTH, ATTN), 0.5, 4.0, ((0, 16), (2, 8)), (0, 1, 16, 2.0), jnp.float32),
        "slope_value": heavy_noise(key_of[4], (REPLICAS, WIDTH, ATTN), 0.5, 4.0, ((0, 16), (2, 8)), (0, 1, 16, 2.0), jnp.float32),
        "slope_mixed": heavy_noise(key_of[5], (REPLICAS, ATTN, WIDTH), 0.5, 4.0, ((0, 16), (1, 8)), (0, 2, 16, 2.0), jnp.float32),
        "slope_norm": heavy_noise(key_of[6], (REPLICAS, WIDTH), 1.0, 8.0, ((0, 16),), (0, 1, 16, 2.0), jnp.float32),
        "slope_bias": heavy_noise(key_of[7], (REPLICAS, WIDTH), 1.0, 8.0, ((0, 16),), (0, 1, 16, 2.0), jnp.float32),
        "param_up": heavy_noise(key_of[8], (WIDTH, INNER), WIDTH ** -0.5, 0.25, ((0, 16), (1, 8)), (1, 0, 16, 2.0), jnp.float32),
        "param_down": heavy_noise(key_of[9], (INNER, WIDTH), INNER ** -0.5, 0.125, ((0, 8), (1, 16)), (0, 1, 16, 2.0), jnp.float32),
        "param_query": heavy_noise(key_of[10], (WIDTH, ATTN), WIDTH ** -0.5, 0.25, ((0, 16), (1, 8)), (1, 0, 16, 2.0), jnp.float32),
        "param_key": heavy_noise(key_of[11], (WIDTH, ATTN), WIDTH ** -0.5, 0.25, ((0, 16), (1, 8)), (1, 0, 16, 2.0), jnp.float32),
        "param_value": heavy_noise(key_of[12], (WIDTH, ATTN), WIDTH ** -0.5, 0.25, ((0, 16), (1, 8)), (1, 0, 16, 2.0), jnp.float32),
        "param_mixed": heavy_noise(key_of[13], (ATTN, WIDTH), ATTN ** -0.5, 0.25, ((0, 8), (1, 16)), (0, 1, 16, 2.0), jnp.float32),
        "param_norm": jnp.clip(1.0 + 0.15 * jax.random.normal(key_of[14], (WIDTH,), jnp.float32), 0.25, 1.75),
        "param_bias": noise(key_of[15], (WIDTH,), 0.5, 3.0, ((0, 16),), jnp.float32),
        "state_up": jnp.clip(0.0001953125 + 0.0017578125 * jax.random.uniform(key_of[16], (WIDTH, INNER), jnp.float32) ** shard_levels(key_of[16], (WIDTH, INNER), ((0, 16), (1, 8)), -0.2, 0.2), 0.0001953125, 0.001953125),
        "state_down": jnp.clip(4.882812572759576e-05 + 0.0004394531 * jax.random.uniform(key_of[17], (INNER, WIDTH), jnp.float32) ** shard_levels(key_of[17], (INNER, WIDTH), ((0, 8), (1, 16)), -0.2, 0.2), 4.882812572759576e-05, 0.00048828125),
        "state_query": jnp.clip(0.0001953125 + 0.0017578125 * jax.random.uniform(key_of[18], (WIDTH, ATTN), jnp.float32) ** shard_levels(key_of[18], (WIDTH, ATTN), ((0, 16), (1, 8)), -0.2, 0.2), 0.0001953125, 0.001953125),
        "state_key": jnp.clip(0.0001953125 + 0.0017578125 * jax.random.uniform(key_of[19], (WIDTH, ATTN), jnp.float32) ** shard_levels(key_of[19], (WIDTH, ATTN), ((0, 16), (1, 8)), -0.2, 0.2), 0.0001953125, 0.001953125),
        "state_value": jnp.clip(0.0001953125 + 0.0017578125 * jax.random.uniform(key_of[20], (WIDTH, ATTN), jnp.float32) ** shard_levels(key_of[20], (WIDTH, ATTN), ((0, 16), (1, 8)), -0.2, 0.2), 0.0001953125, 0.001953125),
        "state_mixed": jnp.clip(0.0001953125 + 0.0017578125 * jax.random.uniform(key_of[21], (ATTN, WIDTH), jnp.float32) ** shard_levels(key_of[21], (ATTN, WIDTH), ((0, 8), (1, 16)), -0.2, 0.2), 0.0001953125, 0.001953125),
        "state_norm": jnp.clip(0.05 + 0.75 * jax.random.uniform(key_of[22], (WIDTH,), jnp.float32) ** shard_levels(key_of[22], (WIDTH,), ((0, 16),), -0.2, 0.2), 0.05, 0.8),
        "state_bias": jnp.clip(0.05 + 0.75 * jax.random.uniform(key_of[23], (WIDTH,), jnp.float32) ** shard_levels(key_of[23], (WIDTH,), ((0, 16),), -0.2, 0.2), 0.05, 0.8),
    }


learn_rate = 0.025
hold_rate = 0.7

def reference(slope_up, slope_down, slope_query, slope_key, slope_value, slope_mixed, slope_norm, slope_bias, param_up, param_down, param_query, param_key, param_value, param_mixed, param_norm, param_bias, state_up, state_down, state_query, state_key, state_value, state_mixed, state_norm, state_bias):
    mean_up = lax.optimization_barrier(jnp.sum(slope_up.astype(jnp.float32), axis=0)) * REPLICAS ** (-0.5)
    mean_down = lax.optimization_barrier(jnp.sum(slope_down.astype(jnp.float32), axis=0)) * REPLICAS ** (-0.5)
    mean_query = lax.optimization_barrier(jnp.sum(slope_query.astype(jnp.float32), axis=0)) * REPLICAS ** (-0.5)
    mean_key = lax.optimization_barrier(jnp.sum(slope_key.astype(jnp.float32), axis=0)) * REPLICAS ** (-0.5)
    mean_value = lax.optimization_barrier(jnp.sum(slope_value.astype(jnp.float32), axis=0)) * REPLICAS ** (-0.5)
    mean_mixed = lax.optimization_barrier(jnp.sum(slope_mixed.astype(jnp.float32), axis=0)) * REPLICAS ** (-0.5)
    mean_norm = lax.optimization_barrier(jnp.sum(slope_norm.astype(jnp.float32), axis=0)) * REPLICAS ** (-0.5)
    mean_bias = lax.optimization_barrier(jnp.sum(slope_bias.astype(jnp.float32), axis=0)) * REPLICAS ** (-0.5)
    ratio_up = jnp.sqrt(lax.optimization_barrier(jnp.sum(param_up * param_up, axis=1, keepdims=True))) * lax.rsqrt(lax.optimization_barrier(jnp.sum(mean_up * mean_up, axis=1, keepdims=True)) + 1e-06)
    mean_up = mean_up * ratio_up
    ratio_down = jnp.sqrt(lax.optimization_barrier(jnp.sum(param_down * param_down, axis=0, keepdims=True))) * lax.rsqrt(lax.optimization_barrier(jnp.sum(mean_down * mean_down, axis=0, keepdims=True)) + 1e-06)
    mean_down = mean_down * ratio_down
    ratio_query = jnp.sqrt(lax.optimization_barrier(jnp.sum(param_query * param_query, axis=1, keepdims=True))) * lax.rsqrt(lax.optimization_barrier(jnp.sum(mean_query * mean_query, axis=1, keepdims=True)) + 1e-06)
    mean_query = mean_query * ratio_query
    ratio_key = jnp.sqrt(lax.optimization_barrier(jnp.sum(param_key * param_key, axis=1, keepdims=True))) * lax.rsqrt(lax.optimization_barrier(jnp.sum(mean_key * mean_key, axis=1, keepdims=True)) + 1e-06)
    mean_key = mean_key * ratio_key
    ratio_value = jnp.sqrt(lax.optimization_barrier(jnp.sum(param_value * param_value, axis=1, keepdims=True))) * lax.rsqrt(lax.optimization_barrier(jnp.sum(mean_value * mean_value, axis=1, keepdims=True)) + 1e-06)
    mean_value = mean_value * ratio_value
    ratio_mixed = jnp.sqrt(lax.optimization_barrier(jnp.sum(param_mixed * param_mixed, axis=0, keepdims=True))) * lax.rsqrt(lax.optimization_barrier(jnp.sum(mean_mixed * mean_mixed, axis=0, keepdims=True)) + 1e-06)
    mean_mixed = mean_mixed * ratio_mixed
    state_new_up = hold_rate * state_up + (1.0 - hold_rate) * mean_up * mean_up
    next_up = param_up - learn_rate * mean_up * lax.rsqrt(state_new_up + 1e-06)
    state_new_down = hold_rate * state_down + (1.0 - hold_rate) * mean_down * mean_down
    next_down = param_down - learn_rate * mean_down * lax.rsqrt(state_new_down + 1e-06)
    state_new_query = hold_rate * state_query + (1.0 - hold_rate) * mean_query * mean_query
    next_query = param_query - learn_rate * mean_query * lax.rsqrt(state_new_query + 1e-06)
    state_new_key = hold_rate * state_key + (1.0 - hold_rate) * mean_key * mean_key
    next_key = param_key - learn_rate * mean_key * lax.rsqrt(state_new_key + 1e-06)
    state_new_value = hold_rate * state_value + (1.0 - hold_rate) * mean_value * mean_value
    next_value = param_value - learn_rate * mean_value * lax.rsqrt(state_new_value + 1e-06)
    state_new_mixed = hold_rate * state_mixed + (1.0 - hold_rate) * mean_mixed * mean_mixed
    next_mixed = param_mixed - learn_rate * mean_mixed * lax.rsqrt(state_new_mixed + 1e-06)
    state_new_norm = hold_rate * state_norm + (1.0 - hold_rate) * mean_norm * mean_norm
    next_norm = param_norm - learn_rate * mean_norm * lax.rsqrt(state_new_norm + 1e-06)
    state_new_bias = hold_rate * state_bias + (1.0 - hold_rate) * mean_bias * mean_bias
    next_bias = param_bias - learn_rate * mean_bias * lax.rsqrt(state_new_bias + 1e-06)
    half_up = next_up.astype(jnp.bfloat16)
    half_down = next_down.astype(jnp.bfloat16)
    half_query = next_query.astype(jnp.bfloat16)
    half_key = next_key.astype(jnp.bfloat16)
    half_value = next_value.astype(jnp.bfloat16)
    half_mixed = next_mixed.astype(jnp.bfloat16)
    half_norm = next_norm.astype(jnp.bfloat16)
    half_bias = next_bias.astype(jnp.bfloat16)
    return (half_up, half_down, half_query, half_key, half_value, half_mixed, half_norm, half_bias, next_up, next_down, next_query, next_key, next_value, next_mixed, next_norm, next_bias, state_new_up, state_new_down, state_new_query, state_new_key, state_new_value, state_new_mixed, state_new_norm, state_new_bias)
```

```python
import functools

import jax
import jax.numpy as jnp
from jax import lax
from jax.experimental import pallas as pl
from jax.experimental.pallas import tpu as pltpu
from jax.sharding import PartitionSpec as P

learn_rate = 0.025
hold_rate = 0.7
MESH = pl.DeviceIdType.MESH
SIDE = 4
PEERS = 8

UP, QUERY, KEY, DOWN, MIXED, VALUE, SMALL, ROWS = 0, 256, 320, 384, 640, 704, 768, 784

CHUNKS = (
    ("y", 0, 64, 64),
    ("z", 384, 64, 64),
    ("y", 128, 64, 64),
    ("z", 512, 64, 64),
    ("y", 256, 64, 64),
    ("z", 640, 80, 64),
)
PER = 12
GATHERS = (
    ("y", 0, 128, 128),
    ("z", 384, 128, 128),
    ("y", 256, 64, 64),
    ("z", 640, 80, 64),
)
PER_GATHER = 8

GRAIN = 2.0**15
GRAIN2 = 2.0**13


def to_wire(x, grain):
    v = x * grain
    v2 = v * v
    v4 = v2 * v2
    return (v4 * v2 * v).astype(jnp.bfloat16)


def from_wire(c, grain):
    c = c.astype(jnp.float32)
    root = jnp.exp(jnp.log(jnp.abs(c)) * (1.0 / 7.0)) * (1.0 / grain)
    return jnp.where(c < 0.0, -root, root)


def low_lanes(shape):
    return lax.broadcasted_iota(jnp.int32, shape, len(shape) - 1) < 64


def turn(x):
    return pltpu.roll(x, 64, 1)


def beside(x):
    half = x.shape[0] // 2
    return jnp.concatenate([x[:half], x[half:]], axis=1)


def exchange_kernel(
    up,
    down,
    query,
    key,
    value,
    mixed,
    norm,
    bias,
    param_up,
    param_down,
    param_query,
    param_key,
    param_value,
    param_mixed,
    param_small,
    state_up,
    state_down,
    state_query,
    state_key,
    state_value,
    state_mixed,
    state_small,
    gathered,
    scaled,
    mine,
    raw_down,
    raw_mixed,
    raw_norm,
    raw_bias,
    send_op,
    send_dir,
    send_fwd,
    recv_op,
    recv_dir,
    recv_fwd,
    first_sum,
    send_op2,
    send_dir2,
    send_fwd2,
    recv_op2,
    recv_dir2,
    recv_fwd2,
    mean,
    squares,
    load_sem,
    send_sem,
    recv_sem,
    gsend_sem,
    grecv_sem,
    nsend_sem,
    nrecv_sem,
):
    replica = lax.axis_index("replica")
    model = lax.axis_index("model")
    z, y = replica // SIDE, replica % SIDE

    def place(axis, step):
        if axis == "y":
            return (z * SIDE + (y + step) % SIDE, model)
        return (((z + step) % SIDE) * SIDE + y, model)

    position = {"y": y, "z": z}
    other = {"y": "z", "z": "y"}

    loads = {}

    def load(name, pairs):
        loads[name] = []
        for src, dst in pairs:
            copy = pltpu.make_async_copy(src, dst, load_sem.at[load.count])
            load.count += 1
            copy.start()
            loads[name].append(copy)

    load.count = 0

    def loaded(name):
        for copy in loads[name]:
            copy.wait()

    load(
        "up",
        [
            (up.at[:, :, :, pl.ds(128 * c, 128)], mine.at[:, :, pl.ds(UP + 64 * c, 64), :])
            for c in range(4)
        ],
    )
    load("down", [(down, raw_down)])
    load(
        "rest",
        [
            (query, mine.at[:, :, pl.ds(QUERY, 64), :]),
            (key, mine.at[:, :, pl.ds(KEY, 64), :]),
            (value, mine.at[:, :, pl.ds(VALUE, 64), :]),
            (mixed, raw_mixed),
            (norm, raw_norm),
            (bias, raw_bias),
        ],
    )

    barrier = pltpu.get_barrier_semaphore()
    for axis in ("y", "z"):
        for step in (1, SIDE - 1):
            pl.semaphore_signal(barrier, 1, device_id=place(axis, step), device_id_type=MESH)
    for step in range(1, PEERS):
        pl.semaphore_signal(
            barrier, 1, device_id=(replica, (model + step) % PEERS), device_id_type=MESH
        )

    def pack_columns(raw, row, half):
        low = low_lanes((64, 128))
        for pair in range(8):
            lanes = pl.ds(128 * pair, 128)
            zz, yy = (2 * pair) // SIDE, (2 * pair) % SIDE

            def body(i, _):
                at = pl.multiple_of(i * 64, 64)
                a = raw[pl.ds(at, 64), lanes]
                b = raw[pl.ds(half + at, 64), lanes]
                mine[zz, yy, pl.ds(row + at, 64), :] = jnp.where(low, a, turn(b))
                mine[zz, yy + 1, pl.ds(row + at, 64), :] = jnp.where(low, turn(a), b)
                return 0

            lax.fori_loop(0, half // 64, body, 0)

    def pack_small():
        low = low_lanes((1, 128))
        for pair in range(8):
            lanes = pl.ds(128 * pair, 128)
            zz, yy = (2 * pair) // SIDE, (2 * pair) % SIDE
            a = raw_norm[:, lanes] * 0.5
            b = raw_bias[:, lanes] * 0.5
            mine[zz, yy, pl.ds(SMALL, 16), :] = jnp.broadcast_to(
                jnp.where(low, a, turn(b)), (16, 128)
            )
            mine[zz, yy + 1, pl.ds(SMALL, 16), :] = jnp.broadcast_to(
                jnp.where(low, turn(a), b), (16, 128)
            )

    def halves(chunk):
        _, row, first, second = CHUNKS[chunk]
        return pl.ds(row, first), pl.ds(row + first, second)

    def share(axis, at, b):
        if axis == "y":
            return mine.at[b, at]
        return mine.at[at, b]

    def remote(chunk, number, src, dst, axis, step):
        k = chunk * PER + number
        return pltpu.make_async_remote_copy(
            src_ref=src,
            dst_ref=dst,
            send_sem=send_sem.at[k],
            recv_sem=recv_sem.at[k],
            device_id=place(axis, step),
            device_id_type=MESH,
        )

    def copies(chunk, number):
        axis = CHUNKS[chunk][0]
        a, b = halves(chunk)
        if number >= 6:
            axis = other[axis]
            bufs = ((send_op2, recv_op2), (send_dir2, recv_dir2), (send_fwd2, recv_fwd2))
            a, b = (a, slice(None)), (b, slice(None))
        else:
            bufs = ((send_op, recv_op), (send_dir, recv_dir), (send_fwd, recv_fwd))
            a, b = (slice(None), a, slice(None)), (slice(None), b, slice(None))
        kind, half = divmod(number % 6, 2)
        src, dst = bufs[kind]
        rows = b if half else a
        step = (SIDE - 1, 1)[half] if kind != 1 else (1, SIDE - 1)[half]
        return remote(chunk, number, src.at[rows], dst.at[rows], axis, step)

    def reduce_send(chunk, first=False):
        axis = CHUNKS[chunk][0]
        p = position[axis]
        a, b = halves(chunk)
        far, right, left = (p + 2) % SIDE, (p + 1) % SIDE, (p + SIDE - 1) % SIDE

        def op(i, _):
            send_op[i, a, :] = to_wire(share(axis, far, i)[a, :], GRAIN)
            send_op[i, b, :] = to_wire(share(axis, far, i)[b, :], GRAIN)
            return 0

        lax.fori_loop(0, SIDE, op, 0)
        if first:
            pl.semaphore_wait(barrier, 4 + PEERS - 1)
        copies(chunk, 0).start()
        copies(chunk, 1).start()

        def direct(i, _):
            send_dir[i, a, :] = to_wire(share(axis, right, i)[a, :], GRAIN)
            send_dir[i, b, :] = to_wire(share(axis, left, i)[b, :], GRAIN)
            return 0

        lax.fori_loop(0, SIDE, direct, 0)
        copies(chunk, 2).start()
        copies(chunk, 3).start()

    def reduce_forward(chunk):
        axis = CHUNKS[chunk][0]
        p = position[axis]
        a, b = halves(chunk)
        right, left = (p + 1) % SIDE, (p + SIDE - 1) % SIDE
        for number, rows, at in ((0, a, left), (1, b, right)):
            copies(chunk, number).wait_recv()

            def body(i, _):
                part = from_wire(recv_op[i, rows, :], GRAIN) + share(axis, at, i)[rows, :]
                send_fwd[i, rows, :] = to_wire(part, GRAIN)
                return 0

            lax.fori_loop(0, SIDE, body, 0)
            copies(chunk, 4 + number).start()

    def reduce_finish(chunk):
        axis = CHUNKS[chunk][0]
        p = position[axis]
        for number in (2, 3, 4, 5):
            copies(chunk, number).wait_recv()

        def body(i, _):
            for rows in halves(chunk):
                first_sum[i, rows, :] = (
                    share(axis, p, i)[rows, :]
                    + from_wire(recv_dir[i, rows, :], GRAIN)
                    + from_wire(recv_fwd[i, rows, :], GRAIN)
                )
            return 0

        lax.fori_loop(0, SIDE, body, 0)

    def second_send(chunk):
        p = position[other[CHUNKS[chunk][0]]]
        a, b = halves(chunk)
        far, right, left = (p + 2) % SIDE, (p + 1) % SIDE, (p + SIDE - 1) % SIDE
        send_op2[a, :] = to_wire(first_sum[far, a, :], GRAIN2)
        copies(chunk, 6).start()
        send_op2[b, :] = to_wire(first_sum[far, b, :], GRAIN2)
        copies(chunk, 7).start()
        send_dir2[a, :] = to_wire(first_sum[right, a, :], GRAIN2)
        copies(chunk, 8).start()
        send_dir2[b, :] = to_wire(first_sum[left, b, :], GRAIN2)
        copies(chunk, 9).start()

    def second_forward(chunk):
        p = position[other[CHUNKS[chunk][0]]]
        a, b = halves(chunk)
        right, left = (p + 1) % SIDE, (p + SIDE - 1) % SIDE
        for number, rows, at in ((6, a, left), (7, b, right)):
            copies(chunk, number).wait_recv()
            part = from_wire(recv_op2[rows, :], GRAIN2) + first_sum[at, rows, :]
            send_fwd2[rows, :] = to_wire(part, GRAIN2)
            copies(chunk, 4 + number).start()

    def second_finish(chunk):
        p = position[other[CHUNKS[chunk][0]]]
        for number in (8, 9, 10, 11):
            copies(chunk, number).wait_recv()
        for rows in halves(chunk):
            mean[rows, :] = (
                first_sum[p, rows, :]
                + from_wire(recv_dir2[rows, :], GRAIN2)
                + from_wire(recv_fwd2[rows, :], GRAIN2)
            ) * (SIDE * SIDE) ** (-0.5)

    def row_squares(row, width, param):
        got = jnp.zeros((64, 128), jnp.float32)
        own = jnp.zeros((64, 128), jnp.float32)
        for c in range(width):
            m = mean[pl.ds(row + 64 * c, 64), :]
            w = param[:, pl.ds(128 * c, 128)]
            got, own = got + m * m, own + w * w
        both = jnp.concatenate([got, own], axis=0)
        return jnp.sum(both, axis=1, keepdims=True)

    def column_squares(row, length, param):
        m = mean[pl.ds(row, length), :]
        w = beside(param[...])
        got = jnp.sum(m * m, axis=0, keepdims=True)
        own = jnp.sum(w * w, axis=0, keepdims=True)
        got, own = got + turn(got), own + turn(own)
        return jnp.where(low_lanes((1, 128)), got, own)

    def norm_copy(turn_number, step):
        k = turn_number * (PEERS - 1) + step - 1
        return pltpu.make_async_remote_copy(
            src_ref=squares.at[turn_number, 0],
            dst_ref=squares.at[turn_number, step],
            send_sem=nsend_sem.at[k],
            recv_sem=nrecv_sem.at[k],
            device_id=(replica, (model + step) % PEERS),
            device_id_type=MESH,
        )

    def norm_send(turn_number, by_rows, by_columns):
        lane = lax.broadcasted_iota(jnp.int32, (128, 128), 1)
        block = jnp.zeros((128, 128), jnp.float32)
        for k, column in enumerate(by_rows):
            block = jnp.where(lane == k, column, block)
        tile = block.T[0:8]
        sub = lax.broadcasted_iota(jnp.int32, (8, 128), 0)
        for k, line in enumerate(by_columns):
            tile = jnp.where(sub == len(by_rows) + k, line, tile)
        squares[turn_number, 0] = tile
        for step in range(1, PEERS):
            norm_copy(turn_number, step).start()

    def norm_ratios(turn_number):
        for step in range(1, PEERS):
            norm_copy(turn_number, step).wait_recv()
        total = squares[turn_number, 0]
        for step in range(1, PEERS):
            total = total + squares[turn_number, step]
        low = low_lanes((8, 128))
        back = turn(total)
        got, own = jnp.where(low, total, back), jnp.where(low, back, total)
        ratio = jnp.sqrt(own) * lax.rsqrt(got + 1e-06)
        return ratio, jnp.concatenate([ratio] * 16, axis=0).T

    def updated(rows, m, param, state):
        scaled[rows, :] = m
        state_new = hold_rate * state + (1.0 - hold_rate) * m * m
        new = param - learn_rate * m * lax.rsqrt(state_new + 1e-06)
        gathered[z, y, rows, :] = new.astype(jnp.bfloat16)

    def row_update(row, width, ratio, param, state):
        for c in range(width):
            rows, lanes = pl.ds(row + 64 * c, 64), pl.ds(128 * c, 128)
            updated(rows, mean[rows, :] * ratio, param[:, lanes], state[:, lanes])

    def column_update(row, length, ratio, param, state):
        rows = pl.ds(row, length)
        updated(rows, mean[rows, :] * ratio, beside(param[...]), beside(state[...]))

    def gather_copies(chunk, number):
        name, row, first, second = GATHERS[chunk]
        k = chunk * PER_GATHER + number
        a, b = pl.ds(row, first), pl.ds(row + first, second)
        whole = pl.ds(row, first + second)
        stage, number = divmod(number, 4)
        axis = other[name] if stage == 0 else name
        rows = (whole, whole, b, a)[number]
        step = (1, SIDE - 1, 1, SIDE - 1)[number]
        shift = (0, 0, SIDE - 1, 1)[number]
        p = (position[axis] + shift) % SIDE
        if stage == 0:
            ref = gathered.at[p, y, rows] if axis == "z" else gathered.at[z, p, rows]
        else:
            ref = gathered.at[p, :, rows] if axis == "z" else gathered.at[:, p, rows]
        return pltpu.make_async_remote_copy(
            src_ref=ref,
            dst_ref=ref,
            send_sem=gsend_sem.at[k],
            recv_sem=grecv_sem.at[k],
            device_id=place(axis, step),
            device_id_type=MESH,
        )

    def gather_send(chunk, stage):
        if stage == 1:
            gather_copies(chunk, 2).wait_recv()
            gather_copies(chunk, 3).wait_recv()
        gather_copies(chunk, 4 * stage).start()
        gather_copies(chunk, 4 * stage + 1).start()

    def gather_forward(chunk, stage):
        gather_copies(chunk, 4 * stage).wait_recv()
        gather_copies(chunk, 4 * stage + 2).start()
        gather_copies(chunk, 4 * stage + 1).wait_recv()
        gather_copies(chunk, 4 * stage + 3).start()

    def gather_finish(chunk):
        gather_copies(chunk, 6).wait_recv()
        gather_copies(chunk, 7).wait_recv()

    loaded("up")
    reduce_send(0, first=True)
    loaded("down")
    pack_columns(raw_down, DOWN, 256)
    reduce_send(1)
    reduce_send(2)
    reduce_send(3)
    loaded("rest")
    pack_columns(raw_mixed, MIXED, 64)
    pack_small()
    reduce_forward(0)
    reduce_forward(1)
    reduce_send(4)
    reduce_send(5)
    for chunk in (0, 1):
        reduce_finish(chunk)
        second_send(chunk)
    reduce_forward(2)
    reduce_forward(3)
    second_forward(0)
    second_forward(1)
    for chunk in (2, 3):
        reduce_finish(chunk)
        second_send(chunk)
    reduce_forward(4)
    reduce_forward(5)
    second_finish(0)
    second_finish(1)
    second_forward(2)
    second_forward(3)
    for chunk in (4, 5):
        reduce_finish(chunk)
        second_send(chunk)
    second_finish(2)
    second_finish(3)
    norm_send(
        0, (row_squares(UP, 4, param_up),), (column_squares(DOWN, 256, param_down),)
    )
    second_forward(4)
    second_forward(5)
    across, down_rows = norm_ratios(0)
    row_update(UP, 4, down_rows[0:64, 0:1], param_up, state_up)
    gather_send(0, 0)
    column_update(DOWN, 256, across[1:2], param_down, state_down)
    gather_send(1, 0)
    second_finish(4)
    second_finish(5)
    norm_send(
        1,
        (
            row_squares(QUERY, 1, param_query),
            row_squares(KEY, 1, param_key),
            row_squares(VALUE, 1, param_value),
        ),
        (column_squares(MIXED, 64, param_mixed),),
    )
    gather_forward(0, 0)
    gather_forward(1, 0)
    across, down_rows = norm_ratios(1)
    row_update(QUERY, 1, down_rows[0:64, 0:1], param_query, state_query)
    row_update(KEY, 1, down_rows[0:64, 1:2], param_key, state_key)
    gather_send(2, 0)
    row_update(VALUE, 1, down_rows[0:64, 2:3], param_value, state_value)
    column_update(MIXED, 64, across[3:4], param_mixed, state_mixed)
    small = pl.ds(SMALL, 16)
    updated(
        small,
        mean[small, :] * 2.0,
        jnp.broadcast_to(param_small[...], (16, 128)),
        jnp.broadcast_to(state_small[...], (16, 128)),
    )
    gather_send(3, 0)
    gather_send(0, 1)
    gather_send(1, 1)
    gather_forward(2, 0)
    gather_forward(3, 0)
    gather_send(2, 1)
    gather_send(3, 1)
    gather_forward(0, 1)
    gather_forward(1, 1)
    gather_forward(2, 1)
    gather_forward(3, 1)
    for chunk in range(len(GATHERS)):
        gather_finish(chunk)

    for chunk in range(len(CHUNKS)):
        for number in range(PER):
            copies(chunk, number).wait_send()
    for chunk in range(len(GATHERS)):
        for number in range(PER_GATHER):
            gather_copies(chunk, number).wait_send()
    for turn_number in range(2):
        for step in range(1, PEERS):
            norm_copy(turn_number, step).wait_send()


def output_kernel(
    gathered,
    scaled,
    param_up,
    param_down,
    param_query,
    param_key,
    param_value,
    param_mixed,
    param_small,
    state_up,
    state_down,
    state_query,
    state_key,
    state_value,
    state_mixed,
    state_small,
    half_up,
    half_down,
    half_query,
    half_key,
    half_value,
    half_mixed,
    half_small,
    next_up,
    next_down,
    next_query,
    next_key,
    next_value,
    next_mixed,
    next_small,
    new_up,
    new_down,
    new_query,
    new_key,
    new_value,
    new_mixed,
    new_small,
):
    def stepped(m, param, state):
        state_new = hold_rate * state + (1.0 - hold_rate) * m * m
        return param - learn_rate * m * lax.rsqrt(state_new + 1e-06), state_new

    def by_rows(row, width, param, state, following, new):
        for c in range(width):
            lanes = pl.ds(128 * c, 128)
            m = scaled[pl.ds(row + 64 * c, 64), :]
            following[:, lanes], new[:, lanes] = stepped(m, param[:, lanes], state[:, lanes])

    def by_columns(row, length, param, state, following, new):
        for part in range(2):
            rows = pl.ds(part * length, length)
            m = scaled[pl.ds(row, length), :]
            if part:
                m = turn(m)
            following[rows, :], new[rows, :] = stepped(m[:, 0:64], param[rows, :], state[rows, :])

    by_rows(UP, 4, param_up, state_up, next_up, new_up)
    by_rows(QUERY, 1, param_query, state_query, next_query, new_query)
    by_rows(KEY, 1, param_key, state_key, next_key, new_key)
    by_rows(VALUE, 1, param_value, state_value, next_value, new_value)
    by_columns(DOWN, 256, param_down, state_down, next_down, new_down)
    by_columns(MIXED, 64, param_mixed, state_mixed, next_mixed, new_mixed)
    next_small[...], new_small[...] = stepped(
        scaled[pl.ds(SMALL, 1), :], param_small[...], state_small[...]
    )

    def rows_of(i, _):
        at = pl.multiple_of(i * 64, 64)
        rows = pl.ds(at, 64)
        for c in range(4):
            half_up[rows, pl.ds(128 * c, 128)] = gathered[i, pl.ds(UP + 64 * c, 64), :]
        half_query[rows, :] = gathered[i, pl.ds(QUERY, 64), :]
        half_key[rows, :] = gathered[i, pl.ds(KEY, 64), :]
        half_value[rows, :] = gathered[i, pl.ds(VALUE, 64), :]
        return 0

    lax.fori_loop(0, SIDE * SIDE, rows_of, 0)

    low = low_lanes((64, 128))
    for out, row, length in ((half_down, DOWN, 256), (half_mixed, MIXED, 64)):
        for pair in range(8):
            lanes = pl.ds(128 * pair, 128)

            def body(i, _):
                at = pl.multiple_of(i * 64, 64)
                a = gathered[2 * pair, pl.ds(row + at, 64), :].astype(jnp.float32)
                b = gathered[2 * pair + 1, pl.ds(row + at, 64), :].astype(jnp.float32)
                out[pl.ds(at, 64), lanes] = jnp.where(low, a, turn(b)).astype(jnp.bfloat16)
                out[pl.ds(length + at, 64), lanes] = jnp.where(low, turn(a), b).astype(
                    jnp.bfloat16
                )
                return 0

            lax.fori_loop(0, length // 64, body, 0)
    low = low_lanes((1, 128))
    for pair in range(8):
        lanes = pl.ds(128 * pair, 128)
        a = gathered[2 * pair, pl.ds(SMALL, 16), :].astype(jnp.float32)[0:1]
        b = gathered[2 * pair + 1, pl.ds(SMALL, 16), :].astype(jnp.float32)[0:1]
        half_small[0:1, lanes] = jnp.where(low, a, turn(b)).astype(jnp.bfloat16)
        half_small[1:2, lanes] = jnp.where(low, turn(a), b).astype(jnp.bfloat16)


def local(*arrays):
    slopes, params, states = arrays[:8], arrays[8:16], arrays[16:]
    up, down, query, key, value, mixed, norm, bias = slopes
    small = [jnp.concatenate([a[6], a[7]])[None] for a in (params, states)]
    params, states = (*params[:6], small[0]), (*states[:6], small[1])
    vmem = pl.BlockSpec(memory_space=pltpu.VMEM)
    anywhere = pl.BlockSpec(memory_space=pl.ANY)
    f32, bf16 = jnp.float32, jnp.bfloat16
    wire = pltpu.VMEM((SIDE, ROWS, 128), bf16)
    wire2 = pltpu.VMEM((ROWS, 128), bf16)
    dma = pltpu.SemaphoreType.DMA
    gathered, scaled = pl.pallas_call(
        exchange_kernel,
        out_shape=(
            jax.ShapeDtypeStruct((SIDE, SIDE, ROWS, 128), bf16),
            jax.ShapeDtypeStruct((ROWS, 128), f32),
        ),
        in_specs=[anywhere] * 8 + [vmem] * 14,
        out_specs=(vmem, vmem),
        scratch_shapes=[
            pltpu.VMEM((SIDE, SIDE, ROWS, 128), f32),
            pltpu.VMEM((512, 1024), f32),
            pltpu.VMEM((128, 1024), f32),
            pltpu.VMEM((1, 1024), f32),
            pltpu.VMEM((1, 1024), f32),
            wire,
            wire,
            wire,
            wire,
            wire,
            wire,
            pltpu.VMEM((SIDE, ROWS, 128), f32),
            wire2,
            wire2,
            wire2,
            wire2,
            wire2,
            wire2,
            pltpu.VMEM((ROWS, 128), f32),
            pltpu.VMEM((2, PEERS, 8, 128), f32),
            dma((11,)),
            dma((len(CHUNKS) * PER,)),
            dma((len(CHUNKS) * PER,)),
            dma((len(GATHERS) * PER_GATHER,)),
            dma((len(GATHERS) * PER_GATHER,)),
            dma((2 * (PEERS - 1),)),
            dma((2 * (PEERS - 1),)),
        ],
        compiler_params=pltpu.CompilerParams(
            collective_id=0, has_side_effects=True, vmem_limit_bytes=60 * 2**20
        ),
        name="exchange",
    )(
        up.reshape(SIDE, SIDE, 64, 512),
        down[0],
        query.reshape(SIDE, SIDE, 64, 128),
        key.reshape(SIDE, SIDE, 64, 128),
        value.reshape(SIDE, SIDE, 64, 128),
        mixed[0],
        norm,
        bias,
        *params,
        *states,
    )
    shapes = [jax.ShapeDtypeStruct(a.shape, f32) for a in params]
    full = [
        jax.ShapeDtypeStruct(s, bf16)
        for s in (
            (1024, 512),
            (512, 1024),
            (1024, 128),
            (1024, 128),
            (1024, 128),
            (128, 1024),
            (2, 1024),
        )
    ]
    out = pl.pallas_call(
        output_kernel,
        out_shape=(*full, *shapes, *shapes),
        in_specs=[vmem] * 16,
        out_specs=(vmem,) * 21,
        compiler_params=pltpu.CompilerParams(vmem_limit_bytes=40 * 2**20),
        name="outputs",
    )(gathered.reshape(SIDE * SIDE, ROWS, 128), scaled, *params, *states)
    half, following, new = out[:7], out[7:14], out[14:]
    return (
        *half[:6],
        half[6][0],
        half[6][1],
        *following[:6],
        following[6][0, :64],
        following[6][0, 64:],
        *new[:6],
        new[6][0, :64],
        new[6][0, 64:],
    )


def solution(mesh):
    def along(split):
        return [
            P(*(("replica", "model") if dim == 0 else ("model", "replica"))[:2])
            if dim < 2
            else P("replica")
            for dim in split
        ]

    shards = along((0, 1, 0, 0, 0, 1, 2, 2))
    slopes = [P("replica", None, "model"), P("replica", "model", None)]
    slopes = [slopes[k] for k in (0, 1, 0, 0, 0, 1)] + [P("replica", None)] * 2
    halves = [P(None, "model"), P("model", None)]
    halves = [halves[k] for k in (0, 1, 0, 0, 0, 1)] + [P()] * 2
    return jax.shard_map(
        local,
        mesh=mesh,
        in_specs=(*slopes, *shards, *shards),
        out_specs=(*halves, *shards, *shards),
        check_vma=False,
    )
```

```python
import contextlib
import math

import jax
import jax.numpy as jnp
from jax import lax
from jax.experimental import pallas as pl
from jax.experimental.pallas import tpu as pltpu
from jax.sharding import PartitionSpec as P

learn_rate = 0.025
hold_rate = 0.7
MESH = pl.DeviceIdType.MESH
SIDE = 4
PEERS = 8

UP, QUERY, KEY, DOWN, MIXED, VALUE, SMALL, ROWS = 0, 256, 320, 384, 640, 704, 768, 784

CHUNKS = (
    ("y", 0, 64, 64),
    ("z", 384, 64, 64),
    ("y", 128, 64, 64),
    ("z", 512, 64, 64),
    ("y", 256, 64, 64),
    ("z", 640, 80, 64),
)
PER = 12
GATHERS = (
    ("y", 0, 128, 128),
    ("z", 384, 128, 128),
    ("y", 256, 64, 64),
    ("z", 640, 80, 64),
)
PER_GATHER = 8

SPAN, BASE = 251 * math.log(2.0), 125 * math.log(2.0)
ONE, TWO, FOUR, EIGHT = 4.0, 8.0, 16.0, 32.0


def to_wire(x, bound):
    level = jnp.exp(jnp.log(jnp.abs(x)) * (1.0 / 6.0) + math.log(SPAN * bound ** (-1.0 / 6.0)))
    size = jnp.exp(level - BASE)
    return jnp.where(x < 0.0, -size, size).astype(jnp.bfloat16)


def from_wire(c, bound):
    c = c.astype(jnp.float32)
    level = (jnp.log(jnp.abs(c)) + BASE) * (bound ** (1.0 / 6.0) / SPAN)
    square = level * level
    size = square * square * square
    return jnp.where(c < 0.0, -size, size)


def low_lanes(shape):
    return lax.broadcasted_iota(jnp.int32, shape, len(shape) - 1) < 64


def turn(x):
    return pltpu.roll(x, 64, 1)


def beside(x):
    half = x.shape[1] // 2
    return jnp.concatenate([x[:, :half], x[:, half:]], axis=0).T


def exchange_kernel(
    up,
    down,
    query,
    key,
    value,
    mixed,
    norm,
    bias,
    *rest,
):
    given, rest = rest[:16], rest[16:]
    held, rest = rest[2 : 2 + 16], (*rest[:2], *rest[2 + 16 :])
    exchange(
        (up, down, query, key, value, mixed, norm, bias), given, held[:8], held[8:], *rest
    )


def exchange(
    slopes,
    given,
    params,
    states,
    gathered,
    scaled,
    mine,
    raw_down,
    raw_mixed,
    raw_norm,
    raw_bias,
    send_op,
    send_dir,
    send_fwd,
    recv_op,
    recv_dir,
    recv_fwd,
    first_sum,
    send_op2,
    send_dir2,
    send_fwd2,
    recv_op2,
    recv_dir2,
    recv_fwd2,
    mean,
    squares,
    load_sem,
    send_sem,
    recv_sem,
    gsend_sem,
    grecv_sem,
    nsend_sem,
    nrecv_sem,
):
    up, down, query, key, value, mixed, norm, bias = slopes
    (
        param_up,
        param_down,
        param_query,
        param_key,
        param_value,
        param_mixed,
        param_norm,
        param_bias,
    ) = params
    (
        state_up,
        state_down,
        state_query,
        state_key,
        state_value,
        state_mixed,
        state_norm,
        state_bias,
    ) = states
    replica = lax.axis_index("replica")
    model = lax.axis_index("model")
    z, y = replica // SIDE, replica % SIDE

    def place(axis, step):
        if axis == "y":
            return (z * SIDE + (y + step) % SIDE, model)
        return (((z + step) % SIDE) * SIDE + y, model)

    position = {"y": y, "z": z}
    other = {"y": "z", "z": "y"}

    loads = {}

    def load(name, pairs):
        loads[name] = []
        for src, dst in pairs:
            copy = pltpu.make_async_copy(src, dst, load_sem.at[load.count])
            load.count += 1
            copy.start()
            loads[name].append(copy)

    load.count = 0

    def loaded(name):
        for copy in loads[name]:
            copy.wait()

    load(
        "up",
        [
            (up.at[:, :, :, pl.ds(128 * c, 128)], mine.at[:, :, pl.ds(UP + 64 * c, 64), :])
            for c in range(4)
        ],
    )
    load("down", [(down, raw_down)])
    load(
        "rest",
        [
            (query, mine.at[:, :, pl.ds(QUERY, 64), :]),
            (key, mine.at[:, :, pl.ds(KEY, 64), :]),
            (value, mine.at[:, :, pl.ds(VALUE, 64), :]),
            (mixed, raw_mixed),
            (norm, raw_norm),
            (bias, raw_bias),
        ],
    )
    load("given", zip(given, (*params, *states)))

    barrier = pltpu.get_barrier_semaphore()
    for axis in ("y", "z"):
        for step in (1, SIDE - 1):
            pl.semaphore_signal(barrier, 1, device_id=place(axis, step), device_id_type=MESH)
    for step in range(1, PEERS):
        pl.semaphore_signal(
            barrier, 1, device_id=(replica, (model + step) % PEERS), device_id_type=MESH
        )

    def pack_columns(raw, row, half):
        low = low_lanes((64, 128))
        for pair in range(8):
            lanes = pl.ds(128 * pair, 128)
            zz, yy = (2 * pair) // SIDE, (2 * pair) % SIDE

            def body(i, _):
                at = pl.multiple_of(i * 64, 64)
                a = raw[pl.ds(at, 64), lanes]
                b = raw[pl.ds(half + at, 64), lanes]
                mine[zz, yy, pl.ds(row + at, 64), :] = jnp.where(low, a, turn(b))
                mine[zz, yy + 1, pl.ds(row + at, 64), :] = jnp.where(low, turn(a), b)
                return 0

            lax.fori_loop(0, half // 64, body, 0)

    def pack_small():
        low = low_lanes((1, 128))
        for pair in range(8):
            lanes = pl.ds(128 * pair, 128)
            zz, yy = (2 * pair) // SIDE, (2 * pair) % SIDE
            a = raw_norm[:, lanes] * 0.5
            b = raw_bias[:, lanes] * 0.5
            mine[zz, yy, pl.ds(SMALL, 16), :] = jnp.broadcast_to(
                jnp.where(low, a, turn(b)), (16, 128)
            )
            mine[zz, yy + 1, pl.ds(SMALL, 16), :] = jnp.broadcast_to(
                jnp.where(low, turn(a), b), (16, 128)
            )

    def halves(chunk):
        _, row, first, second = CHUNKS[chunk]
        return pl.ds(row, first), pl.ds(row + first, second)

    def share(axis, at, b):
        if axis == "y":
            return mine.at[b, at]
        return mine.at[at, b]

    def remote(chunk, number, src, dst, axis, step):
        k = chunk * PER + number
        return pltpu.make_async_remote_copy(
            src_ref=src,
            dst_ref=dst,
            send_sem=send_sem.at[k],
            recv_sem=recv_sem.at[k],
            device_id=place(axis, step),
            device_id_type=MESH,
        )

    def copies(chunk, number):
        axis = CHUNKS[chunk][0]
        a, b = halves(chunk)
        if number >= 6:
            axis = other[axis]
            bufs = ((send_op2, recv_op2), (send_dir2, recv_dir2), (send_fwd2, recv_fwd2))
            a, b = (a, slice(None)), (b, slice(None))
        else:
            bufs = ((send_op, recv_op), (send_dir, recv_dir), (send_fwd, recv_fwd))
            a, b = (slice(None), a, slice(None)), (slice(None), b, slice(None))
        kind, half = divmod(number % 6, 2)
        src, dst = bufs[kind]
        rows = b if half else a
        step = (SIDE - 1, 1)[half] if kind != 1 else (1, SIDE - 1)[half]
        return remote(chunk, number, src.at[rows], dst.at[rows], axis, step)

    def reduce_send(chunk, first=False):
        axis = CHUNKS[chunk][0]
        p = position[axis]
        a, b = halves(chunk)
        far, right, left = (p + 2) % SIDE, (p + 1) % SIDE, (p + SIDE - 1) % SIDE

        def op(i, _):
            send_op[i, a, :] = to_wire(share(axis, far, i)[a, :], ONE)
            send_op[i, b, :] = to_wire(share(axis, far, i)[b, :], ONE)
            return 0

        lax.fori_loop(0, SIDE, op, 0)
        if first:
            pl.semaphore_wait(barrier, 4 + PEERS - 1)
        copies(chunk, 0).start()
        copies(chunk, 1).start()

        def direct(i, _):
            send_dir[i, a, :] = to_wire(share(axis, right, i)[a, :], ONE)
            send_dir[i, b, :] = to_wire(share(axis, left, i)[b, :], ONE)
            return 0

        lax.fori_loop(0, SIDE, direct, 0)
        copies(chunk, 2).start()
        copies(chunk, 3).start()

    def reduce_forward(chunk):
        axis = CHUNKS[chunk][0]
        p = position[axis]
        a, b = halves(chunk)
        right, left = (p + 1) % SIDE, (p + SIDE - 1) % SIDE
        for number, rows, at in ((0, a, left), (1, b, right)):
            copies(chunk, number).wait_recv()

            def body(i, _):
                part = from_wire(recv_op[i, rows, :], ONE) + share(axis, at, i)[rows, :]
                send_fwd[i, rows, :] = to_wire(part, TWO)
                return 0

            lax.fori_loop(0, SIDE, body, 0)
            copies(chunk, 4 + number).start()

    def reduce_finish(chunk):
        axis = CHUNKS[chunk][0]
        p = position[axis]
        for number in (2, 3, 4, 5):
            copies(chunk, number).wait_recv()

        def body(i, _):
            for rows in halves(chunk):
                first_sum[i, rows, :] = (
                    share(axis, p, i)[rows, :]
                    + from_wire(recv_dir[i, rows, :], ONE)
                    + from_wire(recv_fwd[i, rows, :], TWO)
                )
            return 0

        lax.fori_loop(0, SIDE, body, 0)

    def second_send(chunk):
        p = position[other[CHUNKS[chunk][0]]]
        a, b = halves(chunk)
        far, right, left = (p + 2) % SIDE, (p + 1) % SIDE, (p + SIDE - 1) % SIDE
        send_op2[a, :] = to_wire(first_sum[far, a, :], FOUR)
        copies(chunk, 6).start()
        send_op2[b, :] = to_wire(first_sum[far, b, :], FOUR)
        copies(chunk, 7).start()
        send_dir2[a, :] = to_wire(first_sum[right, a, :], FOUR)
        copies(chunk, 8).start()
        send_dir2[b, :] = to_wire(first_sum[left, b, :], FOUR)
        copies(chunk, 9).start()

    def second_forward(chunk):
        p = position[other[CHUNKS[chunk][0]]]
        a, b = halves(chunk)
        right, left = (p + 1) % SIDE, (p + SIDE - 1) % SIDE
        for number, rows, at in ((6, a, left), (7, b, right)):
            copies(chunk, number).wait_recv()
            part = from_wire(recv_op2[rows, :], FOUR) + first_sum[at, rows, :]
            send_fwd2[rows, :] = to_wire(part, EIGHT)
            copies(chunk, 4 + number).start()

    def second_finish(chunk):
        p = position[other[CHUNKS[chunk][0]]]
        for number in (8, 9, 10, 11):
            copies(chunk, number).wait_recv()
        for rows in halves(chunk):
            mean[rows, :] = (
                first_sum[p, rows, :]
                + from_wire(recv_dir2[rows, :], FOUR)
                + from_wire(recv_fwd2[rows, :], EIGHT)
            ) * (SIDE * SIDE) ** (-0.5)

    def row_squares(row, width, param):
        got = jnp.zeros((64, 128), jnp.float32)
        own = jnp.zeros((64, 128), jnp.float32)
        for c in range(width):
            m = mean[pl.ds(row + 64 * c, 64), :]
            w = param[:, pl.ds(128 * c, 128)]
            got, own = got + m * m, own + w * w
        both = jnp.concatenate([got, own], axis=0)
        return jnp.sum(both, axis=1, keepdims=True)

    def column_squares(row, length, param):
        m = mean[pl.ds(row, length), :]
        w = beside(param[...])
        got = jnp.sum(m * m, axis=0, keepdims=True)
        own = jnp.sum(w * w, axis=0, keepdims=True)
        got, own = got + turn(got), own + turn(own)
        return jnp.where(low_lanes((1, 128)), got, own)

    def norm_copy(turn_number, step):
        k = turn_number * (PEERS - 1) + step - 1
        return pltpu.make_async_remote_copy(
            src_ref=squares.at[turn_number, 0],
            dst_ref=squares.at[turn_number, step],
            send_sem=nsend_sem.at[k],
            recv_sem=nrecv_sem.at[k],
            device_id=(replica, (model + step) % PEERS),
            device_id_type=MESH,
        )

    def norm_send(turn_number, by_rows, by_columns):
        lane = lax.broadcasted_iota(jnp.int32, (128, 128), 1)
        block = jnp.zeros((128, 128), jnp.float32)
        for k, column in enumerate(by_rows):
            block = jnp.where(lane == k, column, block)
        tile = block.T[0:8]
        sub = lax.broadcasted_iota(jnp.int32, (8, 128), 0)
        for k, line in enumerate(by_columns):
            tile = jnp.where(sub == len(by_rows) + k, line, tile)
        squares[turn_number, 0] = tile
        for step in range(1, PEERS):
            norm_copy(turn_number, step).start()

    def norm_ratios(turn_number):
        for step in range(1, PEERS):
            norm_copy(turn_number, step).wait_recv()
        total = squares[turn_number, 0]
        for step in range(1, PEERS):
            total = total + squares[turn_number, step]
        low = low_lanes((8, 128))
        back = turn(total)
        got, own = jnp.where(low, total, back), jnp.where(low, back, total)
        ratio = jnp.sqrt(own) * lax.rsqrt(got + 1e-06)
        return ratio, jnp.concatenate([ratio] * 16, axis=0).T

    def updated(rows, m, param, state):
        scaled[rows, :] = m
        state_new = hold_rate * state + (1.0 - hold_rate) * m * m
        new = param - learn_rate * m * lax.rsqrt(state_new + 1e-06)
        gathered[z, y, rows, :] = new.astype(jnp.bfloat16)

    def row_update(row, width, ratio, param, state):
        for c in range(width):
            rows, lanes = pl.ds(row + 64 * c, 64), pl.ds(128 * c, 128)
            updated(rows, mean[rows, :] * ratio, param[:, lanes], state[:, lanes])

    def column_update(row, length, ratio, param, state):
        rows = pl.ds(row, length)
        updated(rows, mean[rows, :] * ratio, beside(param[...]), beside(state[...]))

    def gather_copies(chunk, number):
        name, row, first, second = GATHERS[chunk]
        k = chunk * PER_GATHER + number
        a, b = pl.ds(row, first), pl.ds(row + first, second)
        whole = pl.ds(row, first + second)
        stage, number = divmod(number, 4)
        axis = other[name] if stage == 0 else name
        rows = (whole, whole, b, a)[number]
        step = (1, SIDE - 1, 1, SIDE - 1)[number]
        shift = (0, 0, SIDE - 1, 1)[number]
        p = (position[axis] + shift) % SIDE
        if stage == 0:
            ref = gathered.at[p, y, rows] if axis == "z" else gathered.at[z, p, rows]
        else:
            ref = gathered.at[p, :, rows] if axis == "z" else gathered.at[:, p, rows]
        return pltpu.make_async_remote_copy(
            src_ref=ref,
            dst_ref=ref,
            send_sem=gsend_sem.at[k],
            recv_sem=grecv_sem.at[k],
            device_id=place(axis, step),
            device_id_type=MESH,
        )

    def gather_send(chunk, stage):
        if stage == 1:
            gather_copies(chunk, 2).wait_recv()
            gather_copies(chunk, 3).wait_recv()
        gather_copies(chunk, 4 * stage).start()
        gather_copies(chunk, 4 * stage + 1).start()

    def gather_forward(chunk, stage):
        gather_copies(chunk, 4 * stage).wait_recv()
        gather_copies(chunk, 4 * stage + 2).start()
        gather_copies(chunk, 4 * stage + 1).wait_recv()
        gather_copies(chunk, 4 * stage + 3).start()

    def gather_finish(chunk):
        gather_copies(chunk, 6).wait_recv()
        gather_copies(chunk, 7).wait_recv()

    loaded("up")
    reduce_send(0, first=True)
    loaded("down")
    pack_columns(raw_down, DOWN, 256)
    reduce_send(1)
    reduce_send(2)
    reduce_send(3)
    loaded("rest")
    pack_columns(raw_mixed, MIXED, 64)
    pack_small()
    reduce_forward(0)
    reduce_forward(1)
    reduce_send(4)
    reduce_send(5)
    for chunk in (0, 1):
        reduce_finish(chunk)
        second_send(chunk)
    reduce_forward(2)
    reduce_forward(3)
    second_forward(0)
    second_forward(1)
    for chunk in (2, 3):
        reduce_finish(chunk)
        second_send(chunk)
    reduce_forward(4)
    reduce_forward(5)
    second_finish(0)
    second_finish(1)
    second_forward(2)
    second_forward(3)
    for chunk in (4, 5):
        reduce_finish(chunk)
        second_send(chunk)
    second_finish(2)
    second_finish(3)
    loaded("given")
    norm_send(
        0, (row_squares(UP, 4, param_up),), (column_squares(DOWN, 256, param_down),)
    )
    second_forward(4)
    second_forward(5)
    across, down_rows = norm_ratios(0)
    row_update(UP, 4, down_rows[0:64, 0:1], param_up, state_up)
    gather_send(0, 0)
    column_update(DOWN, 256, across[1:2], param_down, state_down)
    gather_send(1, 0)
    second_finish(4)
    second_finish(5)
    norm_send(
        1,
        (
            row_squares(QUERY, 1, param_query),
            row_squares(KEY, 1, param_key),
            row_squares(VALUE, 1, param_value),
        ),
        (column_squares(MIXED, 64, param_mixed),),
    )
    gather_forward(0, 0)
    gather_forward(1, 0)
    across, down_rows = norm_ratios(1)
    row_update(QUERY, 1, down_rows[0:64, 0:1], param_query, state_query)
    row_update(KEY, 1, down_rows[0:64, 1:2], param_key, state_key)
    gather_send(2, 0)
    row_update(VALUE, 1, down_rows[0:64, 2:3], param_value, state_value)
    column_update(MIXED, 64, across[3:4], param_mixed, state_mixed)
    small = pl.ds(SMALL, 16)
    updated(
        small,
        mean[small, :] * 2.0,
        jnp.concatenate([param_norm[...], param_bias[...]], axis=1),
        jnp.concatenate([state_norm[...], state_bias[...]], axis=1),
    )
    gather_send(3, 0)
    gather_send(0, 1)
    gather_send(1, 1)
    gather_forward(2, 0)
    gather_forward(3, 0)
    gather_send(2, 1)
    gather_send(3, 1)
    gather_forward(0, 1)
    gather_forward(1, 1)
    gather_forward(2, 1)
    gather_forward(3, 1)
    for chunk in range(len(GATHERS)):
        gather_finish(chunk)

    for chunk in range(len(CHUNKS)):
        for number in range(PER):
            copies(chunk, number).wait_send()
    for chunk in range(len(GATHERS)):
        for number in range(PER_GATHER):
            gather_copies(chunk, number).wait_send()
    for turn_number in range(2):
        for step in range(1, PEERS):
            norm_copy(turn_number, step).wait_send()


def output_kernel(gathered, scaled, *refs):
    params, states, refs = refs[:8], refs[8:16], refs[16:]
    half, following, new, refs = refs[:8], refs[8:16], refs[16:24], refs[24:]
    wide_down, wide_mixed, small_halves, sem = *refs[:2], refs[2:4], refs[-1]
    next_held, new_held = refs[4:12], refs[12:20]
    started = []

    def store(src, dst):
        copy = pltpu.make_async_copy(src, dst, sem.at[len(started)])
        copy.start()
        started.append(copy)

    for c in range(4):
        store(gathered.at[:, pl.ds(UP + 64 * c, 64), :], half[0].at[:, :, pl.ds(128 * c, 128)])
    for number, row in ((2, QUERY), (3, KEY), (4, VALUE)):
        store(gathered.at[:, pl.ds(row, 64), :], half[number])

    low = low_lanes((64, 128))
    for out, wide, row, length in (
        (half[1], wide_down, DOWN, 256),
        (half[5], wide_mixed, MIXED, 64),
    ):
        for pair in range(8):
            lanes = pl.ds(128 * pair, 128)

            def body(i, _):
                at = pl.multiple_of(i * 64, 64)
                a = gathered[2 * pair, pl.ds(row + at, 64), :].astype(jnp.float32)
                b = gathered[2 * pair + 1, pl.ds(row + at, 64), :].astype(jnp.float32)
                wide[pl.ds(at, 64), lanes] = jnp.where(low, a, turn(b)).astype(jnp.bfloat16)
                wide[pl.ds(length + at, 64), lanes] = jnp.where(low, turn(a), b).astype(
                    jnp.bfloat16
                )
                return 0

            lax.fori_loop(0, length // 64, body, 0)
            store(wide.at[:, lanes], out.at[:, lanes])

    def step(number, at, m):
        param, state = params[number][at], states[number][at]
        state_new = hold_rate * state + (1.0 - hold_rate) * m * m
        next_held[number][at] = param - learn_rate * m * lax.rsqrt(state_new + 1e-06)
        new_held[number][at] = state_new

    def done(number):
        store(next_held[number], following[number])
        store(new_held[number], new[number])

    for number, row, width in ((0, UP, 4), (2, QUERY, 1), (3, KEY, 1), (4, VALUE, 1)):
        for c in range(width):
            at = (slice(None), pl.ds(128 * c, 128))
            step(number, at, scaled[pl.ds(row + 64 * c, 64), :])
        done(number)
    for number, row, length in ((1, DOWN, 256), (5, MIXED, 64)):
        columns = scaled[pl.ds(row, length), :].T
        columns = jnp.concatenate([columns[:64], columns[64:]], axis=1)
        step(number, (slice(None), slice(None)), columns)
        done(number)
    line = scaled[pl.ds(SMALL, 1), :]
    for number, m in ((6, line[:, :64]), (7, turn(line)[:, :64])):
        step(number, (slice(None), slice(None)), m)
        done(number)

    sub = lax.broadcasted_iota(jnp.int32, (8, 128), 0)
    low = low_lanes((1, 128))
    lines = [jnp.zeros((8, 128), jnp.float32)] * 2
    for pair in range(8):
        a = gathered[2 * pair, pl.ds(SMALL, 16), :].astype(jnp.float32)[0:1]
        b = gathered[2 * pair + 1, pl.ds(SMALL, 16), :].astype(jnp.float32)[0:1]
        lines[0] = jnp.where(sub == pair, jnp.where(low, a, turn(b)), lines[0])
        lines[1] = jnp.where(sub == pair, jnp.where(low, turn(a), b), lines[1])
    for k in range(2):
        small_halves[k][...] = lines[k].astype(jnp.bfloat16)
        store(small_halves[k], half[6 + k])
    for copy in started:
        copy.wait()


def stay(*arrays):
    return [pltpu.with_memory_space_constraint(a, pltpu.HBM) for a in arrays]


def local(*arrays):
    slopes, params, states = arrays[:8], arrays[8:16], arrays[16:]
    up, down, query, key, value, mixed, norm, bias = slopes

    def shown(group):
        up, down, query, key, value, mixed, norm, bias = group
        return up, down.T, query, key, value, mixed.T, norm[None], bias[None]

    params, states = shown(params), shown(states)
    vmem = pl.BlockSpec(memory_space=pltpu.VMEM)
    anywhere = pl.BlockSpec(memory_space=pl.ANY)
    f32, bf16 = jnp.float32, jnp.bfloat16
    wire = pltpu.VMEM((SIDE, ROWS, 128), bf16)
    wire2 = pltpu.VMEM((ROWS, 128), bf16)
    dma = pltpu.SemaphoreType.DMA
    held = [pltpu.VMEM(a.shape, f32) for a in params]
    gathered, scaled = pl.pallas_call(
        exchange_kernel,
        out_shape=(
            pltpu.VMEM((SIDE, SIDE, ROWS, 128), bf16),
            pltpu.VMEM((ROWS, 128), f32),
        ),
        in_specs=[pl.BlockSpec(memory_space=pltpu.HBM)] * 24,
        out_specs=(vmem, vmem),
        scratch_shapes=[
            *held,
            *held,
            pltpu.VMEM((SIDE, SIDE, ROWS, 128), f32),
            pltpu.VMEM((512, 1024), f32),
            pltpu.VMEM((128, 1024), f32),
            pltpu.VMEM((1, 1024), f32),
            pltpu.VMEM((1, 1024), f32),
            *[wire] * 6,
            pltpu.VMEM((SIDE, ROWS, 128), f32),
            *[wire2] * 6,
            pltpu.VMEM((ROWS, 128), f32),
            pltpu.VMEM((2, PEERS, 8, 128), f32),
            dma((11 + 16,)),
            dma((len(CHUNKS) * PER,)),
            dma((len(CHUNKS) * PER,)),
            dma((len(GATHERS) * PER_GATHER,)),
            dma((len(GATHERS) * PER_GATHER,)),
            dma((2 * (PEERS - 1),)),
            dma((2 * (PEERS - 1),)),
        ],
        compiler_params=pltpu.CompilerParams(
            collective_id=0, has_side_effects=True, vmem_limit_bytes=48 * 2**20
        ),
        name="exchange",
    )(
        *stay(
            up.reshape(SIDE, SIDE, 64, 512),
            down[0],
            query.reshape(SIDE, SIDE, 64, 128),
            key.reshape(SIDE, SIDE, 64, 128),
            value.reshape(SIDE, SIDE, 64, 128),
            mixed[0],
            norm,
            bias,
            *params,
            *states,
        )
    )
    own = [jax.ShapeDtypeStruct(a.shape, f32) for a in params]
    full = [
        jax.ShapeDtypeStruct(s, bf16)
        for s in (
            (16, 64, 512),
            (512, 1024),
            (16, 64, 128),
            (16, 64, 128),
            (16, 64, 128),
            (128, 1024),
            (8, 128),
            (8, 128),
        )
    ]
    out = pl.pallas_call(
        output_kernel,
        out_shape=(*full, *own, *own),
        in_specs=[vmem] * 18,
        out_specs=(anywhere,) * 24,
        scratch_shapes=[
            pltpu.VMEM((512, 1024), bf16),
            pltpu.VMEM((128, 1024), bf16),
            pltpu.VMEM((8, 128), bf16),
            pltpu.VMEM((8, 128), bf16),
            *held,
            *held,
            dma((7 + 16 + 16 + 2,)),
        ],
        compiler_params=pltpu.CompilerParams(vmem_limit_bytes=16 * 2**20),
        name="outputs",
    )(gathered.reshape(SIDE * SIDE, ROWS, 128), scaled, *params, *states)
    half, following, new = out[:8], out[8:16], out[16:]
    half_up, half_down, half_query, half_key, half_value, half_mixed, half_norm, half_bias = half

    def back(group):
        up, down, query, key, value, mixed, norm, bias = group
        return up, down.T, query, key, value, mixed.T, norm[0], bias[0]

    return (
        half_up.reshape(1024, 512),
        half_down,
        half_query.reshape(1024, 128),
        half_key.reshape(1024, 128),
        half_value.reshape(1024, 128),
        half_mixed,
        half_norm.reshape(1024),
        half_bias.reshape(1024),
        *back(following),
        *back(new),
    )


def solution(mesh):
    def along(split):
        return [
            P(*(("replica", "model") if dim == 0 else ("model", "replica"))[:2])
            if dim < 2
            else P("replica")
            for dim in split
        ]

    shards = along((0, 1, 0, 0, 0, 1, 2, 2))
    slopes = [P("replica", None, "model"), P("replica", "model", None)]
    slopes = [slopes[k] for k in (0, 1, 0, 0, 0, 1)] + [P("replica", None)] * 2
    halves = [P(None, "model"), P("model", None)]
    halves = [halves[k] for k in (0, 1, 0, 0, 0, 1)] + [P()] * 2
    return jax.shard_map(
        local,
        mesh=mesh,
        in_specs=(*slopes, *shards, *shards),
        out_specs=(*halves, *shards, *shards),
        check_vma=False,
    )
```

```python
import contextlib
import math

import jax
import jax.numpy as jnp
from jax import lax
from jax.experimental import pallas as pl
from jax.experimental.pallas import tpu as pltpu
from jax.sharding import PartitionSpec as P

learn_rate = 0.025
hold_rate = 0.7
MESH = pl.DeviceIdType.MESH
SIDE = 4
PEERS = 8

UP, QUERY, KEY, MIXED, VALUE, SMALL, DOWN, ROWS = 0, 256, 320, 384, 448, 512, 528, 784

CHUNKS = (
    ("y", UP, 64, 64, 0),
    ("z", MIXED, 80, 64, 1),
    ("y", UP + 128, 64, 64, 2),
    ("z", DOWN, 64, 64, 4),
    ("y", QUERY, 64, 64, 3),
    ("z", DOWN + 128, 64, 64, 4),
)
COUNT = len(CHUNKS)
GROUPS = 5
PER = 12
PER_GATHER = 20
LOADS = 8 + 16 + 8 + 3 + 2 + 16

ORDER = (
    ("send", 0), ("send", 1), ("send", 3), ("send", 5), ("send", 4), ("send", 2), ("fwdB", 0),
    ("fwdA", 0), ("fwdA", 1), ("fwdB", 1), ("fwdA", 4), ("fwdB", 4), ("fwdB", 3), ("fwdA", 3),
    ("fwdB", 2), ("fwdA", 2), ("fwdB", 5), ("fwdA", 5), ("prepare", 0), ("fin", 0), ("fin", 1),
    ("fin", 4), ("fin", 3), ("fin", 2), ("Fwd", 1), ("fin", 5), ("Fwd", 0), ("Fwd", 4), ("Fwd", 3),
    ("Fwd", 2), ("Fin", 1), ("norm", 1), ("Fwd", 5), ("Fin", 0), ("norm", 0), ("Fin", 4),
    ("norm", 3), ("Fin", 3), ("Fin", 2), ("norm", 2), ("Fin", 5), ("norm", 4), ("ratio", 1),
    ("upd", 1), ("ratio", 0), ("upd", 0), ("ratio", 3), ("upd", 4), ("ratio", 2), ("upd", 2),
    ("ratio", 4), ("upd", 3), ("xf-", 1), ("upd", 5), ("keep", 0), ("ownF+", 1), ("xf+", 1),
    ("ownF-", 1), ("ownF-", 0), ("xf-", 0), ("ownF+", 0), ("xf+", 0), ("ownF+", 4), ("ownF-", 4),
    ("xf-", 4), ("xf+", 4), ("xf+", 2), ("ownF+", 2), ("xf-", 2), ("ownF-", 2), ("ownF+", 3),
    ("xf+", 3), ("ownF-", 3), ("xf-", 3), ("xf+", 5), ("rF-", 1), ("rF+", 1), ("xf-", 5),
    ("far", 1), ("ownF+", 5), ("ownF-", 5), ("rF+", 0), ("rF-", 0), ("lF-", 1), ("lF+", 1),
    ("lF+", 0), ("lF-", 0), ("far", 0), ("far", 4), ("far", 2), ("rF+", 4), ("rF-", 4), ("lF-", 3),
    ("lF-", 4), ("lF+", 4), ("lF+", 3), ("lF+", 2), ("lF-", 2), ("rF+", 3), ("rF-", 3), ("rF-", 2),
    ("lF-", 5), ("lF+", 5), ("rF+", 2), ("far", 3), ("far", 5), ("rF+", 5), ("rF-", 5), ("fF+", 1),
    ("fF-", 1), ("fF-", 0), ("fF+", 0), ("fF-", 4), ("fF+", 4), ("fF-", 2), ("fF+", 2), ("fF-", 3),
    ("fF+", 3), ("fF+", 5), ("fF-", 5), ("end", 1), ("end", 0), ("end", 4), ("end", 2), ("end", 3),
    ("end", 5),
)


SPAN, BASE = 251 * math.log(2.0), 125 * math.log(2.0)
ONE, TWO, FOUR, EIGHT = 4.0, 8.0, 16.0, 32.0


def to_wire(x, bound):
    level = jnp.exp(jnp.log(jnp.abs(x)) * (1.0 / 6.0) + math.log(SPAN * bound ** (-1.0 / 6.0)))
    size = jnp.exp(level - BASE)
    return jnp.where(x < 0.0, -size, size).astype(jnp.bfloat16)


def from_wire(c, bound):
    c = c.astype(jnp.float32)
    level = (jnp.log(jnp.abs(c)) + BASE) * (bound ** (1.0 / 6.0) / SPAN)
    square = level * level
    size = square * square * square
    return jnp.where(c < 0.0, -size, size)


def low_lanes(shape):
    return lax.broadcasted_iota(jnp.int32, shape, len(shape) - 1) < 64


def turn(x):
    return pltpu.roll(x, 64, 1)


def beside(x):
    half = x.shape[1] // 2
    return jnp.concatenate([x[:, :half], x[:, half:]], axis=0).T


def stage(name):
    return contextlib.nullcontext()


def exchange_kernel(*refs):
    slopes, given, refs = refs[:8], refs[8:24], refs[24:]
    gathered, wide_down, wide_mixed, small_norm, small_bias, refs = *refs[:5], refs[5:]
    following, new, refs = refs[:8], refs[8:16], refs[16:]
    params, states, refs = refs[:8], refs[8:16], refs[16:]
    exchange(
        slopes,
        given,
        gathered,
        (wide_down, wide_mixed),
        (small_norm, small_bias),
        following,
        new,
        params,
        states,
        *refs,
    )


def exchange(
    slopes,
    given,
    gathered,
    wides,
    small_halves,
    following,
    new,
    params,
    states,
    scaled,
    mine,
    raw_norm,
    raw_bias,
    packed_param,
    packed_state,
    send_op,
    send_dir,
    send_fwd,
    recv_op,
    recv_dir,
    recv_fwd,
    first_sum,
    send_op2,
    send_dir2,
    send_fwd2,
    recv_op2,
    recv_dir2,
    recv_fwd2,
    mean,
    squares,
    load_sem,
    send_sem,
    recv_sem,
    gsend_sem,
    grecv_sem,
    nsend_sem,
    nrecv_sem,
):
    up, down, query, key, value, mixed, norm, bias = slopes
    replica = lax.axis_index("replica")
    model = lax.axis_index("model")
    z, y = replica // SIDE, replica % SIDE

    def place(axis, step):
        if axis == "y":
            return (z * SIDE + (y + step) % SIDE, model)
        return (((z + step) % SIDE) * SIDE + y, model)

    position = {"y": y, "z": z}
    other = {"y": "z", "z": "y"}

    loads = {}
    count = [0]

    def load(name, pairs):
        loads[name] = []
        for src, dst in pairs:
            copy = pltpu.make_async_copy(src, dst, load_sem.at[count[0]])
            count[0] += 1
            copy.start()
            loads[name].append(copy)

    def loaded(name):
        for copy in loads.pop(name, ()):
            copy.wait()

    def up_part(part):
        return [
            (
                up.at[:, :, pl.ds(32 * part, 32), pl.ds(128 * c, 128)],
                mine.at[:, :, pl.ds(UP + 128 * part + 32 * c, 32), :],
            )
            for c in range(4)
        ]

    def columns(array, row, start, length):
        return [
            (
                array.at[:, pl.ds(start, length), pl.ds(128 * k, 128)],
                mine.at[k // 2, pl.ds(2 * (k % 2), 2), pl.ds(row + start, length), :],
            )
            for k in range(8)
        ]

    load(0, up_part(0))
    load(
        1,
        [
            *columns(mixed, MIXED, 0, 64),
            (value, mine.at[:, :, pl.ds(VALUE, 64), :]),
            (norm, raw_norm),
            (bias, raw_bias),
        ],
    )
    load(3, columns(down, DOWN, 0, 128))
    load(2, up_part(1))
    load(4, [(query, mine.at[:, :, pl.ds(QUERY, 64), :]), (key, mine.at[:, :, pl.ds(KEY, 64), :])])
    load(5, columns(down, DOWN, 128, 128))
    load("given", zip(given, (*params, *states)))

    barrier = pltpu.get_barrier_semaphore()
    for axis in ("y", "z"):
        for step in (1, SIDE - 1):
            pl.semaphore_signal(barrier, 1, device_id=place(axis, step), device_id_type=MESH)
    for step in range(1, PEERS):
        pl.semaphore_signal(
            barrier, 1, device_id=(replica, (model + step) % PEERS), device_id_type=MESH
        )
    waiting = [True]

    def pack_small():
        low = low_lanes((1, 128))
        for pair in range(8):
            lanes = pl.ds(128 * pair, 128)
            zz, yy = (2 * pair) // SIDE, (2 * pair) % SIDE
            a = raw_norm[:, lanes] * 0.5
            b = raw_bias[:, lanes] * 0.5
            mine[zz, yy, pl.ds(SMALL, 16), :] = jnp.broadcast_to(
                jnp.where(low, a, turn(b)), (16, 128)
            )
            mine[zz, yy + 1, pl.ds(SMALL, 16), :] = jnp.broadcast_to(
                jnp.where(low, turn(a), b), (16, 128)
            )

    def halves(chunk):
        _, row, first, second, _ = CHUNKS[chunk]
        return pl.ds(row, first), pl.ds(row + first, second)

    def share(axis, at, b):
        if axis == "y":
            return mine.at[b, at]
        return mine.at[at, b]

    def copies(chunk, number):
        axis = CHUNKS[chunk][0]
        a, b = halves(chunk)
        if number >= 6:
            axis = other[axis]
            bufs = ((send_op2, recv_op2), (send_dir2, recv_dir2), (send_fwd2, recv_fwd2))
            a, b = (a, slice(None)), (b, slice(None))
        else:
            bufs = ((send_op, recv_op), (send_dir, recv_dir), (send_fwd, recv_fwd))
            a, b = (slice(None), a, slice(None)), (slice(None), b, slice(None))
        kind, half = divmod(number % 6, 2)
        src, dst = bufs[kind]
        rows = b if half else a
        step = (SIDE - 1, 1)[half] if kind != 1 else (1, SIDE - 1)[half]
        k = chunk * PER + number
        return pltpu.make_async_remote_copy(
            src_ref=src.at[rows],
            dst_ref=dst.at[rows],
            send_sem=send_sem.at[k],
            recv_sem=recv_sem.at[k],
            device_id=place(axis, step),
            device_id_type=MESH,
        )

    def send(chunk):
        loaded(chunk)
        if chunk == 1:
            pack_small()
        axis = CHUNKS[chunk][0]
        p = position[axis]
        a, b = halves(chunk)
        far, right, left = (p + 2) % SIDE, (p + 1) % SIDE, (p + SIDE - 1) % SIDE

        def op(i, _):
            send_op[i, a, :] = to_wire(share(axis, far, i)[a, :], ONE)
            send_op[i, b, :] = to_wire(share(axis, far, i)[b, :], ONE)
            return 0

        lax.fori_loop(0, SIDE, op, 0)
        if waiting:
            waiting.pop()
            pl.semaphore_wait(barrier, 4 + PEERS - 1)
        copies(chunk, 0).start()
        copies(chunk, 1).start()

        def direct(i, _):
            send_dir[i, a, :] = to_wire(share(axis, right, i)[a, :], ONE)
            send_dir[i, b, :] = to_wire(share(axis, left, i)[b, :], ONE)
            return 0

        lax.fori_loop(0, SIDE, direct, 0)
        copies(chunk, 2).start()
        copies(chunk, 3).start()

    def forward(chunk, number):
        axis = CHUNKS[chunk][0]
        rows = halves(chunk)[number]
        at = (position[axis] + (SIDE - 1, 1)[number]) % SIDE
        copies(chunk, number).wait_recv()

        def body(i, _):
            part = from_wire(recv_op[i, rows, :], ONE) + share(axis, at, i)[rows, :]
            send_fwd[i, rows, :] = to_wire(part, TWO)
            return 0

        lax.fori_loop(0, SIDE, body, 0)
        copies(chunk, 4 + number).start()

    def finish(chunk):
        axis, row, first, second, _ = CHUNKS[chunk]
        p = position[axis]
        for number in (2, 3, 4, 5):
            copies(chunk, number).wait_recv()

        def summed(i, rows):
            return (
                share(axis, p, i)[rows, :]
                + from_wire(recv_dir[i, rows, :], ONE)
                + from_wire(recv_fwd[i, rows, :], TWO)
            )

        paired = {"y": 0, "z": first + second}[axis] if chunk != 1 else 64

        def pairs(t, _):
            for start in range(0, paired, 64):
                rows = pl.ds(row + start, 64)
                low = low_lanes((64, 128))
                upper, lower = summed(2 * t, rows), summed(2 * t + 1, rows)
                first_sum[2 * t, rows, :] = jnp.where(low, upper, turn(lower))
                first_sum[2 * t + 1, rows, :] = jnp.where(low, turn(upper), lower)
            return 0

        if paired:
            lax.fori_loop(0, SIDE // 2, pairs, 0)

        def plain(i, _):
            for start, stop in ((paired, max(first, paired)), (max(first, paired), first + second)):
                if stop > start:
                    rows = pl.ds(row + start, stop - start)
                    first_sum[i, rows, :] = summed(i, rows)
            return 0

        if paired < first + second:
            lax.fori_loop(0, SIDE, plain, 0)

        p = position[other[axis]]
        a, b = halves(chunk)
        far, right, left = (p + 2) % SIDE, (p + 1) % SIDE, (p + SIDE - 1) % SIDE
        send_op2[a, :] = to_wire(first_sum[far, a, :], FOUR)
        copies(chunk, 6).start()
        send_op2[b, :] = to_wire(first_sum[far, b, :], FOUR)
        copies(chunk, 7).start()
        send_dir2[a, :] = to_wire(first_sum[right, a, :], FOUR)
        copies(chunk, 8).start()
        send_dir2[b, :] = to_wire(first_sum[left, b, :], FOUR)
        copies(chunk, 9).start()

    def second_forward(chunk):
        p = position[other[CHUNKS[chunk][0]]]
        a, b = halves(chunk)
        right, left = (p + 1) % SIDE, (p + SIDE - 1) % SIDE
        for number, rows, at in ((6, a, left), (7, b, right)):
            copies(chunk, number).wait_recv()
            part = from_wire(recv_op2[rows, :], FOUR) + first_sum[at, rows, :]
            send_fwd2[rows, :] = to_wire(part, EIGHT)
            copies(chunk, 4 + number).start()

    def second_finish(chunk):
        p = position[other[CHUNKS[chunk][0]]]
        for number in (8, 9, 10, 11):
            copies(chunk, number).wait_recv()
        for rows in halves(chunk):
            mean[rows, :] = (
                first_sum[p, rows, :]
                + from_wire(recv_dir2[rows, :], FOUR)
                + from_wire(recv_fwd2[rows, :], EIGHT)
            ) * (SIDE * SIDE) ** (-0.5)

    def prepare():
        loaded("given")
        for number, row, length in ((5, MIXED, 64), (1, DOWN, 256)):
            packed_param[pl.ds(row, length), :] = beside(params[number][...])
            packed_state[pl.ds(row, length), :] = beside(states[number][...])

    def row_squares(row, width, param, top, height):
        got = jnp.zeros((height, 128), jnp.float32)
        own = jnp.zeros((height, 128), jnp.float32)
        for c in range(width):
            m = mean[pl.ds(row + height * c, height), :]
            w = param[pl.ds(top, height), pl.ds(128 * c, 128)]
            got, own = got + m * m, own + w * w
        rest = [jnp.zeros((64 - height, 128), jnp.float32)] if height < 64 else []
        both = jnp.concatenate([got, *rest, own, *rest], axis=0)
        return jnp.sum(both, axis=1, keepdims=True)

    def column_squares(row, length):
        m = mean[pl.ds(row, length), :]
        w = packed_param[pl.ds(row, length), :]
        got = jnp.sum(m * m, axis=0, keepdims=True)
        own = jnp.sum(w * w, axis=0, keepdims=True)
        got, own = got + turn(got), own + turn(own)
        return jnp.where(low_lanes((1, 128)), got, own)

    def norm_copy(group, step):
        k = group * (PEERS - 1) + step - 1
        return pltpu.make_async_remote_copy(
            src_ref=squares.at[group, 0],
            dst_ref=squares.at[group, step],
            send_sem=nsend_sem.at[k],
            recv_sem=nrecv_sem.at[k],
            device_id=(replica, (model + step) % PEERS),
            device_id_type=MESH,
        )

    def norm_send(group):
        by_rows, by_columns = [], []
        if group in (0, 2):
            by_rows = [row_squares(UP + 64 * group, 4, params[0], 16 * group, 32)]
        if group == 1:
            by_rows = [row_squares(VALUE, 1, params[4], 0, 64)]
            by_columns = [column_squares(MIXED, 64)]
        if group == 3:
            by_rows = [
                row_squares(QUERY, 1, params[2], 0, 64),
                row_squares(KEY, 1, params[3], 0, 64),
            ]
        if group == 4:
            by_columns = [column_squares(DOWN, 256)]
        tile = jnp.zeros((8, 128), jnp.float32)
        if by_rows:
            lane = lax.broadcasted_iota(jnp.int32, (128, 128), 1)
            block = jnp.zeros((128, 128), jnp.float32)
            for k, column in enumerate(by_rows):
                block = jnp.where(lane == k, column, block)
            tile = block.T[0:8]
        sub = lax.broadcasted_iota(jnp.int32, (8, 128), 0)
        for k, line in enumerate(by_columns):
            tile = jnp.where(sub == len(by_rows) + k, line, tile)
        squares[group, 0] = tile
        for step in range(1, PEERS):
            norm_copy(group, step).start()

    ratios = {}

    def norm_ratios(group):
        for step in range(1, PEERS):
            norm_copy(group, step).wait_recv()
        total = squares[group, 0]
        for step in range(1, PEERS):
            total = total + squares[group, step]
        low = low_lanes((8, 128))
        back = turn(total)
        got, own = jnp.where(low, total, back), jnp.where(low, back, total)
        ratio = jnp.sqrt(own) * lax.rsqrt(got + 1e-06)
        across = ratio
        down_rows = jnp.concatenate([ratio] * 16, axis=0).T if group != 4 else None
        ratios[group] = across, down_rows

    def stepped(m, param, state):
        state_new = hold_rate * state + (1.0 - hold_rate) * m * m
        return param - learn_rate * m * lax.rsqrt(state_new + 1e-06), state_new

    def updated(rows, m, param, state):
        scaled[rows, :] = m
        gathered[z, y, rows, :] = stepped(m, param, state)[0].astype(jnp.bfloat16)

    def row_update(row, width, ratio, number, top, height):
        for c in range(width):
            rows = pl.ds(row + height * c, height)
            at = (pl.ds(top, height), pl.ds(128 * c, 128))
            updated(rows, mean[rows, :] * ratio, params[number][at], states[number][at])

    def column_update(row, length, ratio):
        rows = pl.ds(row, length)
        updated(rows, mean[rows, :] * ratio, packed_param[rows, :], packed_state[rows, :])

    def update(chunk):
        across, down_rows = ratios[CHUNKS[chunk][4]]
        if chunk in (0, 2):
            row_update(UP + 64 * chunk, 4, down_rows[0:32, 0:1], 0, 16 * chunk, 32)
        if chunk == 1:
            column_update(MIXED, 64, across[1:2])
            row_update(VALUE, 1, down_rows[0:64, 0:1], 4, 0, 64)
            small = pl.ds(SMALL, 16)
            updated(
                small,
                mean[small, :] * 2.0,
                jnp.concatenate([params[6][...], params[7][...]], axis=1),
                jnp.concatenate([states[6][...], states[7][...]], axis=1),
            )
        if chunk == 4:
            row_update(QUERY, 1, down_rows[0:64, 0:1], 2, 0, 64)
            row_update(KEY, 1, down_rows[0:64, 1:2], 3, 0, 64)
        if chunk in (3, 5):
            column_update(CHUNKS[chunk][1], 128, across[0:1])

    def keep():
        def step(number, at, m):
            following[number][at], new[number][at] = stepped(
                m, params[number][at], states[number][at]
            )

        for part in range(2):
            for c in range(4):
                at = (pl.ds(32 * part, 32), pl.ds(128 * c, 128))
                step(0, at, scaled[pl.ds(UP + 128 * part + 32 * c, 32), :])
        everything = (slice(None), slice(None))
        for number, row in ((2, QUERY), (3, KEY), (4, VALUE)):
            step(number, everything, scaled[pl.ds(row, 64), :])
        for number, row, length in ((1, DOWN, 256), (5, MIXED, 64)):
            turned = scaled[pl.ds(row, length), :].T
            step(number, everything, jnp.concatenate([turned[:64], turned[64:]], axis=1))
        line = scaled[pl.ds(SMALL, 1), :]
        step(6, everything, line[:, :64])
        step(7, everything, turn(line)[:, :64])

    def gather_copies(chunk, number):
        name, row, first, second, _ = CHUNKS[chunk]
        a, b = pl.ds(row, first), pl.ds(row + first, second)
        whole = pl.ds(row, first + second)
        up_way = number % 2 == 0
        step = 1 if up_way else SIDE - 1
        behind = SIDE - 1 if up_way else 1
        p, q = position[name], position[other[name]]
        axis = name
        rows = whole
        if number < 4:
            axis = other[name]
            if number >= 2:
                rows, q = (b if up_way else a), (q + behind) % SIDE
        else:
            block = (number - 4) // 2 % 4
            q = (q + (0, SIDE - 1, 1, 2)[block]) % SIDE
            if number >= 12:
                rows, p = (b if up_way else a), (p + behind) % SIDE
        ref = gathered.at[q, p, rows] if name == "y" else gathered.at[p, q, rows]
        k = chunk * PER_GATHER + number
        return pltpu.make_async_remote_copy(
            src_ref=ref,
            dst_ref=ref,
            send_sem=gsend_sem.at[k],
            recv_sem=grecv_sem.at[k],
            device_id=place(axis, step),
            device_id_type=MESH,
        )

    def pass_on(chunk, awaited, started):
        for number in awaited:
            gather_copies(chunk, number).wait_recv()
        for number in started:
            gather_copies(chunk, number).start()

    def widen(chunk):
        number, row, start, length = {
            1: (1, MIXED, 0, 64),
            3: (0, DOWN, 0, 128),
            5: (0, DOWN, 128, 128),
        }[chunk]
        out = wides[number]
        half = out.shape[0] // 2
        low = low_lanes((length, 128))
        rows = pl.ds(row + start, length)
        for pair in range(8):
            lanes = pl.ds(128 * pair, 128)
            zz, yy = (2 * pair) // SIDE, (2 * pair) % SIDE
            a = gathered[zz, yy, rows, :].astype(jnp.float32)
            b = gathered[zz, yy + 1, rows, :].astype(jnp.float32)
            out[pl.ds(start, length), lanes] = jnp.where(low, a, turn(b)).astype(jnp.bfloat16)
            out[pl.ds(half + start, length), lanes] = jnp.where(low, turn(a), b).astype(
                jnp.bfloat16
            )

    def small_out():
        sub = lax.broadcasted_iota(jnp.int32, (8, 128), 0)
        low = low_lanes((1, 128))
        lines = [jnp.zeros((8, 128), jnp.float32)] * 2
        for pair in range(8):
            zz, yy = (2 * pair) // SIDE, (2 * pair) % SIDE
            a = gathered[zz, yy, pl.ds(SMALL, 16), :].astype(jnp.float32)[0:1]
            b = gathered[zz, yy + 1, pl.ds(SMALL, 16), :].astype(jnp.float32)[0:1]
            lines[0] = jnp.where(sub == pair, jnp.where(low, a, turn(b)), lines[0])
            lines[1] = jnp.where(sub == pair, jnp.where(low, turn(a), b), lines[1])
        for k in range(2):
            small_halves[k][...] = lines[k].astype(jnp.bfloat16)

    def end(chunk):
        pass_on(chunk, range(12, PER_GATHER), ())
        if chunk in (1, 3, 5):
            widen(chunk)
        if chunk == 1:
            small_out()

    def act(name, k):
        if name == "send":
            send(k)
        elif name in ("fwdA", "fwdB"):
            forward(k, int(name == "fwdB"))
        elif name == "fin":
            finish(k)
        elif name == "Fwd":
            second_forward(k)
        elif name == "Fin":
            second_finish(k)
        elif name == "prepare":
            prepare()
        elif name == "keep":
            keep()
        elif name == "norm":
            norm_send(k)
        elif name == "ratio":
            norm_ratios(k)
        elif name == "upd":
            update(k)
            pass_on(k, (), (0, 1, 4, 5))
        elif name == "xf+":
            pass_on(k, (0,), (2, 6, 7))
        elif name == "xf-":
            pass_on(k, (1,), (3, 8, 9))
        elif name == "far":
            pass_on(k, (2, 3), (10, 11))
        elif name == "end":
            end(k)
        else:
            number = 4 + 2 * ("own", "l", "r", "f").index(name[:-2]) + int(name[-1] == "-")
            pass_on(k, (number,), (number + 8,))

    for name, k in ORDER:
        with stage(f"{name}_{k}"):
            act(name, k)

    with stage("sent"):
        for chunk in range(COUNT):
            for number in range(PER):
                copies(chunk, number).wait_send()
            for number in range(PER_GATHER):
                gather_copies(chunk, number).wait_send()
        for group in range(GROUPS):
            for step in range(1, PEERS):
                norm_copy(group, step).wait_send()


def output_kernel(*refs):
    gathered, laid, refs = refs[0], refs[1:21], refs[21:]
    half, rest, sem = refs[:8], refs[8:24], refs[24]
    pairs = []
    for part in range(2):
        for c in range(4):
            pairs.append(
                (
                    gathered.at[:, pl.ds(UP + 128 * part + 32 * c, 32), :],
                    half[0].at[:, pl.ds(32 * part, 32), pl.ds(128 * c, 128)],
                )
            )
    pairs.append((laid[0], half[1]))
    for number, row in ((2, QUERY), (3, KEY), (4, VALUE)):
        pairs.append((gathered.at[:, pl.ds(row, 64), :], half[number]))
    pairs += zip(laid[1:4], half[5:])
    pairs += zip(laid[4:], rest)
    started = [pltpu.make_async_copy(*pair, sem.at[k]) for k, pair in enumerate(pairs)]
    for copy in started:
        copy.start()
    for copy in started:
        copy.wait()


def stay(*arrays):
    return [pltpu.with_memory_space_constraint(a, pltpu.HBM) for a in arrays]


def local(*arrays):
    slopes, params, states = arrays[:8], arrays[8:16], arrays[16:]
    up, down, query, key, value, mixed, norm, bias = slopes

    def shown(group):
        up, down, query, key, value, mixed, norm, bias = group
        return up, down.T, query, key, value, mixed.T, norm[None], bias[None]

    params, states = shown(params), shown(states)
    vmem = pl.BlockSpec(memory_space=pltpu.VMEM)
    anywhere = pl.BlockSpec(memory_space=pl.ANY)
    f32, bf16 = jnp.float32, jnp.bfloat16
    wire = pltpu.VMEM((SIDE, ROWS, 128), bf16)
    wire2 = pltpu.VMEM((ROWS, 128), bf16)
    dma = pltpu.SemaphoreType.DMA
    held = [pltpu.VMEM(a.shape, f32) for a in params]
    gathered, *laid = pl.pallas_call(
        exchange_kernel,
        out_shape=(
            pltpu.VMEM((SIDE, SIDE, ROWS, 128), bf16),
            pltpu.VMEM((512, 1024), bf16),
            pltpu.VMEM((128, 1024), bf16),
            pltpu.VMEM((8, 128), bf16),
            pltpu.VMEM((8, 128), bf16),
            *held,
            *held,
        ),
        in_specs=[pl.BlockSpec(memory_space=pltpu.HBM)] * 24,
        out_specs=(vmem,) * 21,
        scratch_shapes=[
            *held,
            *held,
            pltpu.VMEM((ROWS, 128), f32),
            pltpu.VMEM((SIDE, SIDE, ROWS, 128), f32),
            pltpu.VMEM((1, 1024), f32),
            pltpu.VMEM((1, 1024), f32),
            pltpu.VMEM((ROWS, 128), f32),
            pltpu.VMEM((ROWS, 128), f32),
            *[wire] * 6,
            pltpu.VMEM((SIDE, ROWS, 128), f32),
            *[wire2] * 6,
            pltpu.VMEM((ROWS, 128), f32),
            pltpu.VMEM((GROUPS, PEERS, 8, 128), f32),
            dma((LOADS,)),
            dma((COUNT * PER,)),
            dma((COUNT * PER,)),
            dma((COUNT * PER_GATHER,)),
            dma((COUNT * PER_GATHER,)),
            dma((GROUPS * (PEERS - 1),)),
            dma((GROUPS * (PEERS - 1),)),
        ],
        compiler_params=pltpu.CompilerParams(
            collective_id=0, has_side_effects=True, vmem_limit_bytes=40 * 2**20
        ),
        name="exchange",
    )(
        *stay(
            up.reshape(SIDE, SIDE, 64, 512),
            down.reshape(2, 256, 1024),
            query.reshape(SIDE, SIDE, 64, 128),
            key.reshape(SIDE, SIDE, 64, 128),
            value.reshape(SIDE, SIDE, 64, 128),
            mixed.reshape(2, 64, 1024),
            norm,
            bias,
            *params,
            *states,
        )
    )
    own = [jax.ShapeDtypeStruct(a.shape, f32) for a in params]
    full = [
        jax.ShapeDtypeStruct(s, bf16)
        for s in (
            (16, 64, 512),
            (512, 1024),
            (16, 64, 128),
            (16, 64, 128),
            (16, 64, 128),
            (128, 1024),
            (8, 128),
            (8, 128),
        )
    ]
    out = pl.pallas_call(
        output_kernel,
        out_shape=(*full, *own, *own),
        in_specs=[vmem] * 21,
        out_specs=(anywhere,) * 24,
        scratch_shapes=[dma((8 + 1 + 3 + 3 + 16,))],
        compiler_params=pltpu.CompilerParams(vmem_limit_bytes=8 * 2**20),
        name="outputs",
    )(gathered.reshape(SIDE * SIDE, ROWS, 128), *laid)
    half, following, new = out[:8], out[8:16], out[16:]
    half_up, half_down, half_query, half_key, half_value, half_mixed, half_norm, half_bias = half

    def back(group):
        up, down, query, key, value, mixed, norm, bias = group
        return up, down.T, query, key, value, mixed.T, norm[0], bias[0]

    return (
        half_up.reshape(1024, 512),
        half_down,
        half_query.reshape(1024, 128),
        half_key.reshape(1024, 128),
        half_value.reshape(1024, 128),
        half_mixed,
        half_norm.reshape(1024),
        half_bias.reshape(1024),
        *back(following),
        *back(new),
    )


def solution(mesh):
    def along(split):
        return [
            P(*(("replica", "model") if dim == 0 else ("model", "replica"))[:2])
            if dim < 2
            else P("replica")
            for dim in split
        ]

    shards = along((0, 1, 0, 0, 0, 1, 2, 2))
    slopes = [P("replica", None, "model"), P("replica", "model", None)]
    slopes = [slopes[k] for k in (0, 1, 0, 0, 0, 1)] + [P("replica", None)] * 2
    halves = [P(None, "model"), P("model", None)]
    halves = [halves[k] for k in (0, 1, 0, 0, 0, 1)] + [P()] * 2
    return jax.shard_map(
        local,
        mesh=mesh,
        in_specs=(*slopes, *shards, *shards),
        out_specs=(*halves, *shards, *shards),
        check_vma=False,
    )
```

```python
import contextlib
import math

import jax
import jax.numpy as jnp
from jax import lax
from jax.experimental import pallas as pl
from jax.experimental.pallas import tpu as pltpu
from jax.sharding import PartitionSpec as P

learn_rate = 0.025
hold_rate = 0.7
MESH = pl.DeviceIdType.MESH
SIDE = 4
PEERS = 8

UP, QUERY, KEY, MIXED, VALUE, SMALL, DOWN, ROWS = 0, 256, 320, 384, 448, 512, 528, 784

CHUNKS = (
    ("y", UP, 64, 64, 0),
    ("z", MIXED, 80, 64, 1),
    ("y", UP + 128, 64, 64, 2),
    ("z", DOWN, 64, 64, 4),
    ("y", QUERY, 64, 64, 3),
    ("z", DOWN + 128, 64, 64, 4),
)
COUNT = len(CHUNKS)
GROUPS = 5
PER = 5
PER_GATHER = 12
LOADS = COUNT + 8
SENDS = 9

ORDER = (
    ("so", 0), ("so", 1), ("so", 2), ("so", 4), ("so", 5), ("sd", 1), ("fwdA", 0), ("sd", 2),
    ("fwdA", 1), ("fwdB", 1), ("so", 3), ("fwdA", 2), ("fwdA", 5), ("fwdB", 2), ("fwdB", 5),
    ("sd", 5), ("fwdB", 0), ("sd", 3), ("fin", 1), ("prepare", 0), ("sd", 0), ("fwdA", 3),
    ("Fwd", 1), ("sd", 4), ("fwdB", 3), ("fwdB", 4), ("fwdA", 4), ("fin", 0), ("fin", 2),
    ("Fin", 1), ("norm", 1), ("fin", 5), ("fin", 3), ("Fwd", 0), ("Fwd", 2), ("fin", 4),
    ("Fwd", 5), ("Fwd", 3), ("Fin", 0), ("norm", 0), ("ratio", 1), ("Fin", 2), ("upd", 1),
    ("norm", 2), ("Fwd", 4), ("Fin", 5), ("Fin", 3), ("norm", 4), ("xf-", 1), ("Fin", 4),
    ("xf+", 1), ("norm", 3), ("ratio", 0), ("upd", 0), ("ratio", 2), ("upd", 2), ("ratio", 4),
    ("upd", 5), ("upd", 3), ("far", 1), ("xf+", 0), ("xf+", 2), ("xf-", 2), ("ratio", 3),
    ("xf-", 0), ("xf-", 5), ("upd", 4), ("xf+", 5), ("rF-", 1), ("xf-", 3), ("ownF+", 5),
    ("far", 0), ("xf+", 3), ("ownF+", 2), ("far", 2), ("xf-", 4), ("xf+", 4), ("lF+", 0),
    ("rF+", 2), ("rF+", 1), ("lF-", 5), ("ownF-", 3), ("far", 5), ("lF-", 0), ("rF-", 2),
    ("lF+", 1), ("ownF-", 1), ("far", 3), ("ownF-", 0), ("rF+", 3), ("fF-", 1), ("fF+", 1),
    ("far", 4), ("fF+", 0), ("lF+", 2), ("rF+", 5), ("lF-", 1), ("ownF+", 0), ("keep", 0),
    ("ownF-", 2), ("ownF+", 1), ("ownF-", 4), ("lF-", 3), ("rF-", 5), ("lF+", 3), ("ownF+", 3),
    ("rF-", 4), ("fF-", 2), ("lF-", 2), ("rF+", 0), ("rF-", 3), ("ownF+", 4), ("fF+", 5),
    ("ownF-", 5), ("lF+", 4), ("lF+", 5), ("rF+", 4), ("fF-", 0), ("fF+", 2), ("rF-", 0),
    ("fF-", 5), ("fF-", 3), ("fF+", 3), ("lF-", 4), ("fF+", 4), ("fF-", 4), ("end", 1), ("end", 0),
    ("end", 5), ("end", 3), ("end", 2), ("end", 4),
)


SPAN, BASE = 251 * math.log(2.0), 125 * math.log(2.0)
ONE, TWO, FOUR, EIGHT = 4.0, 8.0, 16.0, 32.0


def to_wire(x, bound):
    level = jnp.exp(jnp.log(jnp.abs(x)) * (1.0 / 6.0) + math.log(SPAN * bound ** (-1.0 / 6.0)))
    size = jnp.exp(level - BASE)
    return jnp.where(x < 0.0, -size, size).astype(jnp.bfloat16)


def from_wire(c, bound):
    c = c.astype(jnp.float32)
    level = (jnp.log(jnp.abs(c)) + BASE) * (bound ** (1.0 / 6.0) / SPAN)
    square = level * level
    size = square * square * square
    return jnp.where(c < 0.0, -size, size)


def low_lanes(shape):
    return lax.broadcasted_iota(jnp.int32, shape, len(shape) - 1) < 64


def turn(x):
    return pltpu.roll(x, 64, 1)


def beside(x):
    half = x.shape[1] // 2
    return jnp.concatenate([x[:, :half], x[:, half:]], axis=0).T


def stage(name):
    return contextlib.nullcontext()


def exchange_kernel(*refs):
    slopes, given, refs = refs[:8], refs[8:24], refs[24:]
    gathered, wide_down, wide_mixed, small_norm, small_bias, refs = *refs[:5], refs[5:]
    following, new, refs = refs[:8], refs[8:16], refs[16:]
    params, states, refs = refs[:8], refs[8:16], refs[16:]
    exchange(
        slopes,
        given,
        gathered,
        (wide_down, wide_mixed),
        (small_norm, small_bias),
        following,
        new,
        params,
        states,
        *refs,
    )


def exchange(
    slopes,
    given,
    gathered,
    wides,
    small_halves,
    following,
    new,
    params,
    states,
    scaled,
    mine,
    raw_norm,
    raw_bias,
    packed_param,
    packed_state,
    send_op,
    send_dir,
    send_fwd,
    recv_op,
    both,
    first_sum,
    send_op2,
    send_dir2,
    send_fwd2,
    recv_op2,
    both2,
    mean,
    squares,
    load_sem,
    send_sem,
    recv_sem,
    grecv_sem,
    nrecv_sem,
):
    up, down, query, key, value, mixed, norm, bias = slopes
    recv_rest = recv_dir, recv_fwd = both.at[0], both.at[1]
    recv_rest2 = recv_dir2, recv_fwd2 = both2.at[0], both2.at[1]
    replica = lax.axis_index("replica")
    model = lax.axis_index("model")
    z, y = replica // SIDE, replica % SIDE

    def place(axis, step):
        if axis == "y":
            return (z * SIDE + (y + step) % SIDE, model)
        return (((z + step) % SIDE) * SIDE + y, model)

    position = {"y": y, "z": z}
    other = {"y": "z", "z": "y"}

    def all_of(ref, sem):
        pltpu.make_async_copy(ref, ref, sem).wait()

    def load(number, pairs):
        for src, dst in pairs:
            pltpu.make_async_copy(src, dst, load_sem.at[number]).start()

    def loaded(number, *refs):
        for k, ref in enumerate(refs):
            all_of(ref, load_sem.at[number + k])

    def whole(chunk):
        _, row, first, second, _ = CHUNKS[chunk]
        return pl.ds(row, first + second)

    def up_part(part):
        return [
            (
                up.at[:, :, pl.ds(32 * part, 32), pl.ds(128 * c, 128)],
                mine.at[:, :, pl.ds(UP + 128 * part + 32 * c, 32), :],
            )
            for c in range(4)
        ]

    def columns(array, row, start, length):
        return [
            (
                array.at[:, pl.ds(start, length), pl.ds(128 * k, 128)],
                mine.at[k // 2, pl.ds(2 * (k % 2), 2), pl.ds(row + start, length), :],
            )
            for k in range(8)
        ]

    load(0, up_part(0))
    load(
        1,
        [
            *columns(mixed, MIXED, 0, 64),
            (value, mine.at[:, :, pl.ds(VALUE, 64), :]),
        ],
    )
    load(COUNT, [(norm, raw_norm)])
    load(COUNT + 1, [(bias, raw_bias)])
    load(3, columns(down, DOWN, 0, 128))
    load(2, up_part(1))
    load(4, [(query, mine.at[:, :, pl.ds(QUERY, 64), :]), (key, mine.at[:, :, pl.ds(KEY, 64), :])])
    load(5, columns(down, DOWN, 128, 128))
    held = [*zip(given, (*params, *states))]
    load(COUNT + 2, [held[k] for k in (0, 1, 8, 9)])
    load(COUNT + 3, [held[k] for k in (2, 3, 4, 5, 10, 11, 12, 13)])
    for k, pair in enumerate((held[6], held[7], held[14], held[15])):
        load(COUNT + 4 + k, [pair])

    barrier = pltpu.get_barrier_semaphore()
    for axis in ("y", "z"):
        for step in (1, SIDE - 1):
            pl.semaphore_signal(barrier, 1, device_id=place(axis, step), device_id_type=MESH)
    for step in range(1, PEERS):
        pl.semaphore_signal(
            barrier, 1, device_id=(replica, (model + step) % PEERS), device_id_type=MESH
        )
    waiting = [True]

    def pack_small():
        low = low_lanes((1, 128))
        for pair in range(8):
            lanes = pl.ds(128 * pair, 128)
            zz, yy = (2 * pair) // SIDE, (2 * pair) % SIDE
            a = raw_norm[:, lanes] * 0.5
            b = raw_bias[:, lanes] * 0.5
            mine[zz, yy, pl.ds(SMALL, 16), :] = jnp.broadcast_to(
                jnp.where(low, a, turn(b)), (16, 128)
            )
            mine[zz, yy + 1, pl.ds(SMALL, 16), :] = jnp.broadcast_to(
                jnp.where(low, turn(a), b), (16, 128)
            )

    def halves(chunk):
        _, row, first, second, _ = CHUNKS[chunk]
        return pl.ds(row, first), pl.ds(row + first, second)

    def share(axis, at, b):
        if axis == "y":
            return mine.at[b, at]
        return mine.at[at, b]

    def copies(chunk, number):
        axis = CHUNKS[chunk][0]
        a, b = halves(chunk)
        second = number >= 6
        if second:
            axis = other[axis]
            sources, targets = (send_op2, send_dir2, send_fwd2), (recv_op2, *recv_rest2)
            a, b = (a, slice(None)), (b, slice(None))
        else:
            sources, targets = (send_op, send_dir, send_fwd), (recv_op, *recv_rest)
            a, b = (slice(None), a, slice(None)), (slice(None), b, slice(None))
        kind, half = divmod(number % 6, 2)
        rows = b if half else a
        step = (SIDE - 1, 1)[half] if kind != 1 else (1, SIDE - 1)[half]
        arrival = (3 if second else half) if kind == 0 else (4 if second else 2)
        return pltpu.make_async_remote_copy(
            src_ref=sources[kind].at[rows],
            dst_ref=targets[kind].at[rows],
            send_sem=send_sem.at[3 * second + kind],
            recv_sem=recv_sem.at[chunk * PER + arrival],
            device_id=place(axis, step),
            device_id_type=MESH,
        )

    def send(chunk):
        if chunk == 1:
            loaded(chunk, mine.at[:, :, pl.ds(MIXED, 128)])
            loaded(COUNT, raw_norm, raw_bias)
            pack_small()
        else:
            loaded(chunk, mine.at[:, :, whole(chunk)])
        axis = CHUNKS[chunk][0]
        p = position[axis]
        a, b = halves(chunk)
        far = (p + 2) % SIDE

        def op(i, _):
            send_op[i, a, :] = to_wire(share(axis, far, i)[a, :], ONE)
            send_op[i, b, :] = to_wire(share(axis, far, i)[b, :], ONE)
            return 0

        lax.fori_loop(0, SIDE, op, 0)
        if waiting:
            waiting.pop()
            pl.semaphore_wait(barrier, 4 + PEERS - 1)
        copies(chunk, 0).start()
        copies(chunk, 1).start()

    def send_direct(chunk):
        axis = CHUNKS[chunk][0]
        p = position[axis]
        a, b = halves(chunk)
        right, left = (p + 1) % SIDE, (p + SIDE - 1) % SIDE

        def direct(i, _):
            send_dir[i, a, :] = to_wire(share(axis, right, i)[a, :], ONE)
            send_dir[i, b, :] = to_wire(share(axis, left, i)[b, :], ONE)
            return 0

        lax.fori_loop(0, SIDE, direct, 0)
        copies(chunk, 2).start()
        copies(chunk, 3).start()

    def forward(chunk, number):
        axis = CHUNKS[chunk][0]
        rows = halves(chunk)[number]
        at = (position[axis] + (SIDE - 1, 1)[number]) % SIDE
        copies(chunk, number).wait_recv()

        def body(i, _):
            part = from_wire(recv_op[i, rows, :], ONE) + share(axis, at, i)[rows, :]
            send_fwd[i, rows, :] = to_wire(part, TWO)
            return 0

        lax.fori_loop(0, SIDE, body, 0)
        copies(chunk, 4 + number).start()

    def finish(chunk):
        axis, row, first, second, _ = CHUNKS[chunk]
        p = position[axis]
        all_of(both.at[:, :, whole(chunk)], recv_sem.at[chunk * PER + 2])

        def summed(i, rows):
            return (
                share(axis, p, i)[rows, :]
                + from_wire(recv_dir[i, rows, :], ONE)
                + from_wire(recv_fwd[i, rows, :], TWO)
            )

        paired = {"y": 0, "z": first + second}[axis] if chunk != 1 else 64

        def pairs(t, _):
            for start in range(0, paired, 64):
                rows = pl.ds(row + start, 64)
                low = low_lanes((64, 128))
                upper, lower = summed(2 * t, rows), summed(2 * t + 1, rows)
                first_sum[2 * t, rows, :] = jnp.where(low, upper, turn(lower))
                first_sum[2 * t + 1, rows, :] = jnp.where(low, turn(upper), lower)
            return 0

        if paired:
            lax.fori_loop(0, SIDE // 2, pairs, 0)

        def plain(i, _):
            for start, stop in ((paired, max(first, paired)), (max(first, paired), first + second)):
                if stop > start:
                    rows = pl.ds(row + start, stop - start)
                    first_sum[i, rows, :] = summed(i, rows)
            return 0

        if paired < first + second:
            lax.fori_loop(0, SIDE, plain, 0)

        p = position[other[axis]]
        a, b = halves(chunk)
        far, right, left = (p + 2) % SIDE, (p + 1) % SIDE, (p + SIDE - 1) % SIDE
        send_op2[a, :] = to_wire(first_sum[far, a, :], FOUR)
        copies(chunk, 6).start()
        send_op2[b, :] = to_wire(first_sum[far, b, :], FOUR)
        copies(chunk, 7).start()
        send_dir2[a, :] = to_wire(first_sum[right, a, :], FOUR)
        copies(chunk, 8).start()
        send_dir2[b, :] = to_wire(first_sum[left, b, :], FOUR)
        copies(chunk, 9).start()

    def second_forward(chunk):
        p = position[other[CHUNKS[chunk][0]]]
        a, b = halves(chunk)
        right, left = (p + 1) % SIDE, (p + SIDE - 1) % SIDE
        all_of(recv_op2.at[whole(chunk)], recv_sem.at[chunk * PER + 3])
        for number, rows, at in ((6, a, left), (7, b, right)):
            part = from_wire(recv_op2[rows, :], FOUR) + first_sum[at, rows, :]
            send_fwd2[rows, :] = to_wire(part, EIGHT)
            copies(chunk, 4 + number).start()

    def second_finish(chunk):
        p = position[other[CHUNKS[chunk][0]]]
        all_of(both2.at[:, whole(chunk)], recv_sem.at[chunk * PER + 4])
        for rows in halves(chunk):
            mean[rows, :] = (
                first_sum[p, rows, :]
                + from_wire(recv_dir2[rows, :], FOUR)
                + from_wire(recv_fwd2[rows, :], EIGHT)
            ) * (SIDE * SIDE) ** (-0.5)

    def prepare():
        loaded(COUNT + 2, first_sum.at[0:2, 0:512], mean.at[0:512])
        loaded(COUNT + 4, params[6], params[7], states[6], states[7])
        for number, row, length in ((5, MIXED, 64), (1, DOWN, 256)):
            packed_param[pl.ds(row, length), :] = beside(params[number][...])
            packed_state[pl.ds(row, length), :] = beside(states[number][...])

    def row_squares(row, width, param, top, height):
        got = jnp.zeros((height, 128), jnp.float32)
        own = jnp.zeros((height, 128), jnp.float32)
        for c in range(width):
            m = mean[pl.ds(row + height * c, height), :]
            w = param[pl.ds(top, height), pl.ds(128 * c, 128)]
            got, own = got + m * m, own + w * w
        rest = [jnp.zeros((64 - height, 128), jnp.float32)] if height < 64 else []
        both = jnp.concatenate([got, *rest, own, *rest], axis=0)
        return jnp.sum(both, axis=1, keepdims=True)

    def column_squares(row, length):
        m = mean[pl.ds(row, length), :]
        w = packed_param[pl.ds(row, length), :]
        got = jnp.sum(m * m, axis=0, keepdims=True)
        own = jnp.sum(w * w, axis=0, keepdims=True)
        got, own = got + turn(got), own + turn(own)
        return jnp.where(low_lanes((1, 128)), got, own)

    def norm_copy(group, step):
        return pltpu.make_async_remote_copy(
            src_ref=squares.at[group, 0],
            dst_ref=squares.at[group, step],
            send_sem=send_sem.at[8],
            recv_sem=nrecv_sem.at[group],
            device_id=(replica, (model + step) % PEERS),
            device_id_type=MESH,
        )

    def norm_send(group):
        by_rows, by_columns = [], []
        if group in (0, 2):
            by_rows = [row_squares(UP + 64 * group, 4, params[0], 16 * group, 32)]
        if group == 1:
            by_rows = [row_squares(VALUE, 1, params[4], 0, 64)]
            by_columns = [column_squares(MIXED, 64)]
        if group == 3:
            by_rows = [
                row_squares(QUERY, 1, params[2], 0, 64),
                row_squares(KEY, 1, params[3], 0, 64),
            ]
        if group == 4:
            by_columns = [column_squares(DOWN, 256)]
        tile = jnp.zeros((8, 128), jnp.float32)
        if by_rows:
            lane = lax.broadcasted_iota(jnp.int32, (128, 128), 1)
            block = jnp.zeros((128, 128), jnp.float32)
            for k, column in enumerate(by_rows):
                block = jnp.where(lane == k, column, block)
            tile = block.T[0:8]
        sub = lax.broadcasted_iota(jnp.int32, (8, 128), 0)
        for k, line in enumerate(by_columns):
            tile = jnp.where(sub == len(by_rows) + k, line, tile)
        squares[group, 0] = tile
        for step in range(1, PEERS):
            norm_copy(group, step).start()

    ratios = {}

    def norm_ratios(group):
        all_of(squares.at[group, 1:PEERS], nrecv_sem.at[group])
        total = squares[group, 0]
        for step in range(1, PEERS):
            total = total + squares[group, step]
        low = low_lanes((8, 128))
        back = turn(total)
        got, own = jnp.where(low, total, back), jnp.where(low, back, total)
        ratio = jnp.sqrt(own) * lax.rsqrt(got + 1e-06)
        across = ratio
        down_rows = jnp.concatenate([ratio] * 16, axis=0).T if group != 4 else None
        ratios[group] = across, down_rows

    def stepped(m, param, state):
        state_new = hold_rate * state + (1.0 - hold_rate) * m * m
        return param - learn_rate * m * lax.rsqrt(state_new + 1e-06), state_new

    def updated(rows, m, param, state):
        scaled[rows, :] = m
        gathered[z, y, rows, :] = stepped(m, param, state)[0].astype(jnp.bfloat16)

    def row_update(row, width, ratio, number, top, height):
        for c in range(width):
            rows = pl.ds(row + height * c, height)
            at = (pl.ds(top, height), pl.ds(128 * c, 128))
            updated(rows, mean[rows, :] * ratio, params[number][at], states[number][at])

    def column_update(row, length, ratio):
        rows = pl.ds(row, length)
        updated(rows, mean[rows, :] * ratio, packed_param[rows, :], packed_state[rows, :])

    def update(chunk):
        across, down_rows = ratios[CHUNKS[chunk][4]]
        if chunk in (0, 2):
            row_update(UP + 64 * chunk, 4, down_rows[0:32, 0:1], 0, 16 * chunk, 32)
        if chunk == 1:
            column_update(MIXED, 64, across[1:2])
            row_update(VALUE, 1, down_rows[0:64, 0:1], 4, 0, 64)
            small = pl.ds(SMALL, 16)
            updated(
                small,
                mean[small, :] * 2.0,
                jnp.concatenate([params[6][...], params[7][...]], axis=1),
                jnp.concatenate([states[6][...], states[7][...]], axis=1),
            )
        if chunk == 4:
            row_update(QUERY, 1, down_rows[0:64, 0:1], 2, 0, 64)
            row_update(KEY, 1, down_rows[0:64, 1:2], 3, 0, 64)
        if chunk in (3, 5):
            column_update(CHUNKS[chunk][1], 128, across[0:1])

    def keep():
        def step(number, at, m):
            following[number][at], new[number][at] = stepped(
                m, params[number][at], states[number][at]
            )

        for part in range(2):
            for c in range(4):
                at = (pl.ds(32 * part, 32), pl.ds(128 * c, 128))
                step(0, at, scaled[pl.ds(UP + 128 * part + 32 * c, 32), :])
        everything = (slice(None), slice(None))
        for number, row in ((2, QUERY), (3, KEY), (4, VALUE)):
            step(number, everything, scaled[pl.ds(row, 64), :])
        for number, row, length in ((1, DOWN, 256), (5, MIXED, 64)):
            turned = scaled[pl.ds(row, length), :].T
            step(number, everything, jnp.concatenate([turned[:64], turned[64:]], axis=1))
        line = scaled[pl.ds(SMALL, 1), :]
        step(6, everything, line[:, :64])
        step(7, everything, turn(line)[:, :64])

    def gather_copies(chunk, number):
        name, row, first, second, _ = CHUNKS[chunk]
        a, b = pl.ds(row, first), pl.ds(row + first, second)
        up_way = number % 2 == 0
        step = 1 if up_way else SIDE - 1
        behind = SIDE - 1 if up_way else 1
        p, q = position[name], position[other[name]]
        axis = name
        rows = whole(chunk)
        if number < 4:
            axis = other[name]
            if number >= 2:
                rows, q = (b if up_way else a), (q + behind) % SIDE
        else:
            block = (number - 4) // 2 % 4
            q = (q + (0, SIDE - 1, 1, 2)[block]) % SIDE
            if number >= 12:
                rows, p = (b if up_way else a), (p + behind) % SIDE
        ref = gathered.at[q, p, rows] if name == "y" else gathered.at[p, q, rows]
        arrival = min(number, 2) if number < 4 else min(number - 1, 11)
        return pltpu.make_async_remote_copy(
            src_ref=ref,
            dst_ref=ref,
            send_sem=send_sem.at[6 if number < 4 else 7],
            recv_sem=grecv_sem.at[chunk * PER_GATHER + arrival],
            device_id=place(axis, step),
            device_id_type=MESH,
        )

    def pass_on(chunk, awaited, started):
        for number in awaited:
            gather_copies(chunk, number).wait_recv()
        for number in started:
            gather_copies(chunk, number).start()

    def widen(chunk):
        number, row, start, length = {
            1: (1, MIXED, 0, 64),
            3: (0, DOWN, 0, 128),
            5: (0, DOWN, 128, 128),
        }[chunk]
        out = wides[number]
        half = out.shape[0] // 2
        low = low_lanes((length, 128))
        rows = pl.ds(row + start, length)
        for pair in range(8):
            lanes = pl.ds(128 * pair, 128)
            zz, yy = (2 * pair) // SIDE, (2 * pair) % SIDE
            a = gathered[zz, yy, rows, :].astype(jnp.float32)
            b = gathered[zz, yy + 1, rows, :].astype(jnp.float32)
            out[pl.ds(start, length), lanes] = jnp.where(low, a, turn(b)).astype(jnp.bfloat16)
            out[pl.ds(half + start, length), lanes] = jnp.where(low, turn(a), b).astype(
                jnp.bfloat16
            )

    def small_out():
        sub = lax.broadcasted_iota(jnp.int32, (8, 128), 0)
        low = low_lanes((1, 128))
        lines = [jnp.zeros((8, 128), jnp.float32)] * 2
        for pair in range(8):
            zz, yy = (2 * pair) // SIDE, (2 * pair) % SIDE
            a = gathered[zz, yy, pl.ds(SMALL, 16), :].astype(jnp.float32)[0:1]
            b = gathered[zz, yy + 1, pl.ds(SMALL, 16), :].astype(jnp.float32)[0:1]
            lines[0] = jnp.where(sub == pair, jnp.where(low, a, turn(b)), lines[0])
            lines[1] = jnp.where(sub == pair, jnp.where(low, turn(a), b), lines[1])
        for k in range(2):
            small_halves[k][...] = lines[k].astype(jnp.bfloat16)

    def end(chunk):
        all_of(gathered.at[0, :, whole(chunk)], grecv_sem.at[chunk * PER_GATHER + 11])
        if chunk in (1, 3, 5):
            widen(chunk)
        if chunk == 1:
            small_out()

    def act(name, k):
        if name == "so":
            send(k)
        elif name == "sd":
            send_direct(k)
        elif name in ("fwdA", "fwdB"):
            forward(k, int(name == "fwdB"))
        elif name == "fin":
            finish(k)
        elif name == "Fwd":
            second_forward(k)
        elif name == "Fin":
            second_finish(k)
        elif name == "prepare":
            prepare()
        elif name == "keep":
            keep()
        elif name == "norm":
            norm_send(k)
        elif name == "ratio":
            norm_ratios(k)
        elif name == "upd":
            update(k)
            pass_on(k, (), (0, 1, 4, 5))
        elif name == "xf+":
            pass_on(k, (0,), (2, 6, 7))
        elif name == "xf-":
            pass_on(k, (1,), (3, 8, 9))
        elif name == "far":
            all_of(gathered.at[0, 0, whole(k)], grecv_sem.at[k * PER_GATHER + 2])
            pass_on(k, (), (10, 11))
        elif name == "end":
            end(k)
        else:
            number = 4 + 2 * ("own", "l", "r", "f").index(name[:-2]) + int(name[-1] == "-")
            pass_on(k, (number,), (number + 8,))

    for name, k in ORDER:
        with stage(f"{name}_{k}"):
            act(name, k)

    with stage("sent"):
        for k, ref in enumerate((send_op, send_dir, send_fwd, send_op2, send_dir2, send_fwd2)):
            all_of(ref, send_sem.at[k])
        all_of(gathered.at[0, 0:3], send_sem.at[6])
        all_of(gathered.at[0:3], send_sem.at[7])
        all_of(squares.at[:, 1:PEERS], send_sem.at[8])


def output_kernel(*refs):
    gathered, laid, refs = refs[0], refs[1:21], refs[21:]
    half, rest, sem = refs[:8], refs[8:24], refs[24]
    pairs = []
    for part in range(2):
        for c in range(4):
            pairs.append(
                (
                    gathered.at[:, pl.ds(UP + 128 * part + 32 * c, 32), :],
                    half[0].at[:, pl.ds(32 * part, 32), pl.ds(128 * c, 128)],
                )
            )
    pairs.append((laid[0], half[1]))
    for number, row in ((2, QUERY), (3, KEY), (4, VALUE)):
        pairs.append((gathered.at[:, pl.ds(row, 64), :], half[number]))
    pairs += zip(laid[1:4], half[5:])
    pairs += zip(laid[4:], rest)
    started = [pltpu.make_async_copy(*pair, sem.at[k]) for k, pair in enumerate(pairs)]
    for copy in started:
        copy.start()
    for copy in started:
        copy.wait()


def stay(*arrays):
    return [pltpu.with_memory_space_constraint(a, pltpu.HBM) for a in arrays]


def local(*arrays):
    slopes, params, states = arrays[:8], arrays[8:16], arrays[16:]
    up, down, query, key, value, mixed, norm, bias = slopes

    def shown(group):
        up, down, query, key, value, mixed, norm, bias = group
        return up, down.T, query, key, value, mixed.T, norm[None], bias[None]

    params, states = shown(params), shown(states)
    vmem = pl.BlockSpec(memory_space=pltpu.VMEM)
    anywhere = pl.BlockSpec(memory_space=pl.ANY)
    f32, bf16 = jnp.float32, jnp.bfloat16
    wire = pltpu.VMEM((SIDE, ROWS, 128), bf16)
    wire2 = pltpu.VMEM((ROWS, 128), bf16)
    dma = pltpu.SemaphoreType.DMA
    held = [pltpu.VMEM(a.shape, f32) for a in params]
    gathered, *laid = pl.pallas_call(
        exchange_kernel,
        out_shape=(
            pltpu.VMEM((SIDE, SIDE, ROWS, 128), bf16),
            pltpu.VMEM((512, 1024), bf16),
            pltpu.VMEM((128, 1024), bf16),
            pltpu.VMEM((8, 128), bf16),
            pltpu.VMEM((8, 128), bf16),
            *held,
            *held,
        ),
        in_specs=[pl.BlockSpec(memory_space=pltpu.HBM)] * 24,
        out_specs=(vmem,) * 21,
        scratch_shapes=[
            *held,
            *held,
            pltpu.VMEM((ROWS, 128), f32),
            pltpu.VMEM((SIDE, SIDE, ROWS, 128), f32),
            pltpu.VMEM((1, 1024), f32),
            pltpu.VMEM((1, 1024), f32),
            pltpu.VMEM((ROWS, 128), f32),
            pltpu.VMEM((ROWS, 128), f32),
            *[wire] * 4,
            pltpu.VMEM((2, SIDE, ROWS, 128), bf16),
            pltpu.VMEM((SIDE, ROWS, 128), f32),
            *[wire2] * 4,
            pltpu.VMEM((2, ROWS, 128), bf16),
            pltpu.VMEM((ROWS, 128), f32),
            pltpu.VMEM((GROUPS, PEERS, 8, 128), f32),
            dma((LOADS,)),
            dma((SENDS,)),
            dma((COUNT * PER,)),
            dma((COUNT * PER_GATHER,)),
            dma((GROUPS,)),
        ],
        compiler_params=pltpu.CompilerParams(
            collective_id=0, has_side_effects=True, vmem_limit_bytes=40 * 2**20
        ),
        name="exchange",
    )(
        *stay(
            up.reshape(SIDE, SIDE, 64, 512),
            down.reshape(2, 256, 1024),
            query.reshape(SIDE, SIDE, 64, 128),
            key.reshape(SIDE, SIDE, 64, 128),
            value.reshape(SIDE, SIDE, 64, 128),
            mixed.reshape(2, 64, 1024),
            norm,
            bias,
            *params,
            *states,
        )
    )
    own = [jax.ShapeDtypeStruct(a.shape, f32) for a in params]
    full = [
        jax.ShapeDtypeStruct(s, bf16)
        for s in (
            (16, 64, 512),
            (512, 1024),
            (16, 64, 128),
            (16, 64, 128),
            (16, 64, 128),
            (128, 1024),
            (8, 128),
            (8, 128),
        )
    ]
    out = pl.pallas_call(
        output_kernel,
        out_shape=(*full, *own, *own),
        in_specs=[vmem] * 21,
        out_specs=(anywhere,) * 24,
        scratch_shapes=[dma((8 + 1 + 3 + 3 + 16,))],
        compiler_params=pltpu.CompilerParams(vmem_limit_bytes=8 * 2**20),
        name="outputs",
    )(gathered.reshape(SIDE * SIDE, ROWS, 128), *laid)
    half, following, new = out[:8], out[8:16], out[16:]
    half_up, half_down, half_query, half_key, half_value, half_mixed, half_norm, half_bias = half

    def back(group):
        up, down, query, key, value, mixed, norm, bias = group
        return up, down.T, query, key, value, mixed.T, norm[0], bias[0]

    return (
        half_up.reshape(1024, 512),
        half_down,
        half_query.reshape(1024, 128),
        half_key.reshape(1024, 128),
        half_value.reshape(1024, 128),
        half_mixed,
        half_norm.reshape(1024),
        half_bias.reshape(1024),
        *back(following),
        *back(new),
    )


def solution(mesh):
    def along(split):
        return [
            P(*(("replica", "model") if dim == 0 else ("model", "replica"))[:2])
            if dim < 2
            else P("replica")
            for dim in split
        ]

    shards = along((0, 1, 0, 0, 0, 1, 2, 2))
    slopes = [P("replica", None, "model"), P("replica", "model", None)]
    slopes = [slopes[k] for k in (0, 1, 0, 0, 0, 1)] + [P("replica", None)] * 2
    halves = [P(None, "model"), P("model", None)]
    halves = [halves[k] for k in (0, 1, 0, 0, 0, 1)] + [P()] * 2
    return jax.shard_map(
        local,
        mesh=mesh,
        in_specs=(*slopes, *shards, *shards),
        out_specs=(*halves, *shards, *shards),
        check_vma=False,
    )
```

```python
import contextlib
import math

import jax
import jax.numpy as jnp
from jax import lax
from jax.experimental import pallas as pl
from jax.experimental.pallas import tpu as pltpu
from jax.sharding import PartitionSpec as P

learn_rate = 0.025
hold_rate = 0.7
MESH = pl.DeviceIdType.MESH
SIDE = 4
PEERS = 8

UP, QUERY, KEY, MIXED, VALUE, SMALL, DOWN, ROWS = 0, 256, 320, 384, 448, 512, 528, 784

CHUNKS = (
    ("y", UP, 32, 32),
    ("z", MIXED, 80, 64),
    ("y", UP + 64, 32, 32),
    ("y", UP + 128, 32, 32),
    ("z", DOWN, 32, 32),
    ("y", UP + 192, 32, 32),
    ("z", DOWN + 64, 32, 32),
    ("y", QUERY, 64, 64),
    ("z", DOWN + 128, 32, 32),
    ("z", DOWN + 192, 32, 32),
)
GATHERS = (
    ("y", UP, 64, 64, 0),
    ("z", MIXED, 80, 64, 1),
    ("y", UP + 128, 64, 64, 2),
    ("z", DOWN, 64, 64, 4),
    ("y", QUERY, 64, 64, 3),
    ("z", DOWN + 128, 64, 64, 4),
)
COUNT = len(CHUNKS)
GROUPS = 5
PER = 8
PER_GATHER = 12
LOADS = COUNT + 8
SENDS = 9

ORDER = (
    ("soF", 0), ("sdF", 0), ("soF", 1), ("sdF", 1), ("soO", 2), ("soF", 4), ("soF", 7), ("sdF", 7),
    ("soF", 3), ("soO", 1), ("sdO", 1), ("soO", 7), ("soF", 2), ("sdF", 2), ("fwdBF", 1),
    ("fwdAF", 1), ("soF", 5), ("fwdBF", 7), ("soF", 8), ("sdF", 4), ("fwdAF", 7), ("soF", 9),
    ("sdO", 7), ("soF", 6), ("fwdBO", 2), ("soO", 8), ("soO", 0), ("fwdAO", 1), ("fwdAF", 3),
    ("fwdBO", 1), ("soO", 9), ("fwdBF", 0), ("fwdAF", 0), ("finF", 1), ("fwdAO", 7), ("sdF", 9),
    ("fwdBF", 4), ("fwdAF", 8), ("fwdBO", 7), ("finF", 7), ("soO", 4), ("fwdBF", 2), ("fwdAF", 2),
    ("fwdBF", 9), ("prepare", 0), ("soO", 3), ("fwdAF", 4), ("soO", 6), ("sdF", 8), ("soO", 5),
    ("fwdBF", 6), ("fwdAF", 9), ("sdF", 6), ("fwdAO", 2), ("fwdBF", 3), ("finO", 1), ("Fwd", 1),
    ("sdF", 3), ("fwdBF", 8), ("sdF", 5), ("fwdAF", 6), ("fwdBF", 5), ("finO", 7), ("fwdAF", 5),
    ("fwdAO", 0), ("sdO", 0), ("sdO", 2), ("fwdBO", 0), ("Fwd", 7), ("fwdBO", 8), ("sdO", 9),
    ("fwdBO", 5), ("finF", 0), ("finF", 2), ("fwdAO", 3), ("fwdBO", 4), ("fwdBO", 9), ("fwdAO", 4),
    ("fwdBO", 3), ("fwdAO", 9), ("fwdAO", 6), ("fwdBO", 6), ("sdO", 6), ("finF", 4), ("sdO", 4),
    ("sdO", 8), ("Fin", 1), ("norm", 1), ("finF", 6), ("finF", 9), ("fwdAO", 8), ("finF", 8),
    ("Fin", 7), ("sdO", 3), ("norm", 3), ("fwdAO", 5), ("finF", 3), ("finF", 5), ("sdO", 5),
    ("finO", 2), ("Fwd", 2), ("finO", 0), ("Fwd", 0), ("finO", 9), ("Fwd", 9), ("finO", 6),
    ("Fwd", 6), ("finO", 4), ("Fwd", 4), ("finO", 3), ("finO", 8), ("Fwd", 8), ("finO", 5),
    ("Fwd", 5), ("Fwd", 3), ("ratio", 1), ("upd", 1), ("Fin", 0), ("Fin", 2), ("norm", 0),
    ("Fin", 9), ("ratio", 3), ("upd", 4), ("Fin", 4), ("Fin", 6), ("Fin", 8), ("norm", 4),
    ("Fin", 3), ("Fin", 5), ("norm", 2), ("ownF+", 1), ("xf-", 1), ("xf+", 1), ("ownF+", 4),
    ("ownF-", 4), ("xf+", 4), ("ownF-", 1), ("xf-", 4), ("ratio", 0), ("upd", 0), ("far", 1),
    ("ratio", 4), ("upd", 3), ("ratio", 2), ("upd", 2), ("lF-", 1), ("upd", 5), ("keep", 0),
    ("xf+", 0), ("xf-", 0), ("rF+", 1), ("xf+", 3), ("xf-", 3), ("xf+", 2), ("xf-", 2), ("xf-", 5),
    ("xf+", 5), ("lF+", 0), ("far", 4), ("lF-", 4), ("far", 0), ("far", 3), ("lF+", 1), ("rF+", 0),
    ("rF-", 1), ("far", 2), ("lF-", 0), ("lF+", 4), ("fF-", 1), ("fF+", 1), ("far", 5), ("lF+", 3),
    ("rF+", 4), ("ownF-", 3), ("rF-", 2), ("rF-", 3), ("rF-", 4), ("fF-", 4), ("ownF+", 2),
    ("rF+", 2), ("rF+", 3), ("lF+", 2), ("ownF+", 3), ("lF-", 2), ("rF+", 5), ("lF+", 5),
    ("fF+", 4), ("ownF+", 5), ("rF-", 0), ("ownF-", 5), ("rF-", 5), ("ownF-", 2), ("lF-", 3),
    ("fF+", 3), ("ownF+", 0), ("fF+", 0), ("ownF-", 0), ("lF-", 5), ("fF-", 0), ("fF-", 3),
    ("fF-", 2), ("end", 1), ("fF+", 2), ("fF-", 5), ("fF+", 5), ("end", 3), ("end", 0), ("end", 4),
    ("end", 5), ("end", 2),
)


SPAN, BASE = 251 * math.log(2.0), 125 * math.log(2.0)
ONE, TWO, FOUR, EIGHT = 4.0, 8.0, 16.0, 32.0


def to_wire(x, bound):
    level = jnp.exp(jnp.log(jnp.abs(x)) * (1.0 / 6.0) + math.log(SPAN * bound ** (-1.0 / 6.0)))
    size = jnp.exp(level - BASE)
    return jnp.where(x < 0.0, -size, size).astype(jnp.bfloat16)


def from_wire(c, bound):
    c = c.astype(jnp.float32)
    level = (jnp.log(jnp.abs(c)) + BASE) * (bound ** (1.0 / 6.0) / SPAN)
    square = level * level
    size = square * square * square
    return jnp.where(c < 0.0, -size, size)


def low_lanes(shape):
    return lax.broadcasted_iota(jnp.int32, shape, len(shape) - 1) < 64


def turn(x):
    return pltpu.roll(x, 64, 1)


def beside(x):
    half = x.shape[1] // 2
    return jnp.concatenate([x[:, :half], x[:, half:]], axis=0).T


def stage(name):
    return contextlib.nullcontext()


def exchange_kernel(*refs):
    slopes, given, refs = refs[:8], refs[8:24], refs[24:]
    gathered, wide_down, wide_mixed, small_norm, small_bias, refs = *refs[:5], refs[5:]
    following, new, refs = refs[:8], refs[8:16], refs[16:]
    params, states, refs = refs[:8], refs[8:16], refs[16:]
    exchange(
        slopes,
        given,
        gathered,
        (wide_down, wide_mixed),
        (small_norm, small_bias),
        following,
        new,
        params,
        states,
        *refs,
    )


def exchange(
    slopes,
    given,
    gathered,
    wides,
    small_halves,
    following,
    new,
    params,
    states,
    scaled,
    mine,
    raw_norm,
    raw_bias,
    packed_param,
    packed_state,
    send_op,
    send_dir,
    send_fwd,
    recv_op,
    both,
    first_sum,
    send_op2,
    send_dir2,
    send_fwd2,
    recv_op2,
    both2,
    mean,
    squares,
    load_sem,
    send_sem,
    recv_sem,
    grecv_sem,
    nrecv_sem,
):
    up, down, query, key, value, mixed, norm, bias = slopes
    recv_rest = recv_dir, recv_fwd = both.at[0], both.at[1]
    recv_rest2 = recv_dir2, recv_fwd2 = both2.at[0], both2.at[1]
    replica = lax.axis_index("replica")
    model = lax.axis_index("model")
    z, y = replica // SIDE, replica % SIDE

    def place(axis, step):
        if axis == "y":
            return (z * SIDE + (y + step) % SIDE, model)
        return (((z + step) % SIDE) * SIDE + y, model)

    position = {"y": y, "z": z}
    other = {"y": "z", "z": "y"}

    def all_of(ref, sem):
        pltpu.make_async_copy(ref, ref, sem).wait()

    def load(number, pairs):
        for src, dst in pairs:
            pltpu.make_async_copy(src, dst, load_sem.at[number]).start()

    def loaded(number, *refs):
        for k, ref in enumerate(refs):
            all_of(ref, load_sem.at[number + k])

    def whole(chunk, table=CHUNKS):
        _, row, first, second, *_ = table[chunk]
        return pl.ds(row, first + second)

    def up_part(part, columns):
        return [
            (
                up.at[:, :, pl.ds(32 * part, 32), pl.ds(128 * c, 128)],
                mine.at[:, :, pl.ds(UP + 128 * part + 32 * c, 32), :],
            )
            for c in columns
        ]

    def columns(array, row, start, length):
        return [
            (
                array.at[:, pl.ds(start, length), pl.ds(128 * k, 128)],
                mine.at[k // 2, pl.ds(2 * (k % 2), 2), pl.ds(row + start, length), :],
            )
            for k in range(8)
        ]

    load(0, up_part(0, (0, 1)))
    load(
        1,
        [
            *columns(mixed, MIXED, 0, 64),
            (value, mine.at[:, :, pl.ds(VALUE, 64), :]),
        ],
    )
    load(COUNT, [(norm, raw_norm)])
    load(COUNT + 1, [(bias, raw_bias)])
    load(2, up_part(0, (2, 3)))
    load(3, up_part(1, (0, 1)))
    load(4, columns(down, DOWN, 0, 64))
    load(5, up_part(1, (2, 3)))
    load(6, columns(down, DOWN, 64, 64))
    load(7, [(query, mine.at[:, :, pl.ds(QUERY, 64), :]), (key, mine.at[:, :, pl.ds(KEY, 64), :])])
    load(8, columns(down, DOWN, 128, 64))
    load(9, columns(down, DOWN, 192, 64))
    held = [*zip(given, (*params, *states))]
    load(COUNT + 2, [held[k] for k in (0, 1, 8, 9)])
    load(COUNT + 3, [held[k] for k in (2, 3, 4, 5, 10, 11, 12, 13)])
    for k, pair in enumerate((held[6], held[7], held[14], held[15])):
        load(COUNT + 4 + k, [pair])

    barrier = pltpu.get_barrier_semaphore()
    for axis in ("y", "z"):
        for step in (1, SIDE - 1):
            pl.semaphore_signal(barrier, 1, device_id=place(axis, step), device_id_type=MESH)
    for step in range(1, PEERS):
        pl.semaphore_signal(
            barrier, 1, device_id=(replica, (model + step) % PEERS), device_id_type=MESH
        )
    waiting = [True]

    def pack_small():
        low = low_lanes((1, 128))
        for pair in range(8):
            lanes = pl.ds(128 * pair, 128)
            zz, yy = (2 * pair) // SIDE, (2 * pair) % SIDE
            a = raw_norm[:, lanes] * 0.5
            b = raw_bias[:, lanes] * 0.5
            mine[zz, yy, pl.ds(SMALL, 16), :] = jnp.broadcast_to(
                jnp.where(low, a, turn(b)), (16, 128)
            )
            mine[zz, yy + 1, pl.ds(SMALL, 16), :] = jnp.broadcast_to(
                jnp.where(low, turn(a), b), (16, 128)
            )

    def halves(chunk):
        _, row, first, second = CHUNKS[chunk]
        return pl.ds(row, first), pl.ds(row + first, second)

    def pair_of(chunk, part):
        own = position[other[CHUNKS[chunk][0]]] // 2
        return 2 * own if part else 2 - 2 * own

    def share(axis, at, b):
        if axis == "y":
            return mine.at[b, at]
        return mine.at[at, b]

    def copies(chunk, number, part=0):
        axis = CHUNKS[chunk][0]
        a, b = halves(chunk)
        second = number >= 6
        if second:
            axis = other[axis]
            sources, targets = (send_op2, send_dir2, send_fwd2), (recv_op2, *recv_rest2)
        else:
            sources, targets = (send_op, send_dir, send_fwd), (recv_op, *recv_rest)
        kind, half = divmod(number % 6, 2)
        rows = b if half else a
        at = (rows, slice(None))
        if not second:
            at = (pl.ds(pair_of(chunk, part), 2), *at)
        step = (SIDE - 1, 1)[half] if kind != 1 else (1, SIDE - 1)[half]
        if second:
            arrival = 6 if kind == 0 else 7
        else:
            arrival = 3 * part + (half if kind == 0 else 2)
        return pltpu.make_async_remote_copy(
            src_ref=sources[kind].at[at],
            dst_ref=targets[kind].at[at],
            send_sem=send_sem.at[3 * second + kind],
            recv_sem=recv_sem.at[chunk * PER + arrival],
            device_id=place(axis, step),
            device_id_type=MESH,
        )

    ready = set()

    def send(chunk, part):
        if chunk not in ready:
            ready.add(chunk)
            if chunk == 1:
                loaded(chunk, mine.at[:, :, pl.ds(MIXED, 128)])
                loaded(COUNT, raw_norm, raw_bias)
                pack_small()
            else:
                loaded(chunk, mine.at[:, :, whole(chunk)])
        axis = CHUNKS[chunk][0]
        far = (position[axis] + 2) % SIDE
        pair, rows = pair_of(chunk, part), whole(chunk)

        def op(i, _):
            send_op[pair + i, rows, :] = to_wire(share(axis, far, pair + i)[rows, :], ONE)
            return 0

        lax.fori_loop(0, 2, op, 0)
        if waiting:
            waiting.pop()
            pl.semaphore_wait(barrier, 4 + PEERS - 1)
        copies(chunk, 0, part).start()
        copies(chunk, 1, part).start()

    def send_direct(chunk, part):
        axis = CHUNKS[chunk][0]
        p = position[axis]
        a, b = halves(chunk)
        right, left = (p + 1) % SIDE, (p + SIDE - 1) % SIDE
        pair = pair_of(chunk, part)

        def direct(i, _):
            send_dir[pair + i, a, :] = to_wire(share(axis, right, pair + i)[a, :], ONE)
            send_dir[pair + i, b, :] = to_wire(share(axis, left, pair + i)[b, :], ONE)
            return 0

        lax.fori_loop(0, 2, direct, 0)
        copies(chunk, 2, part).start()
        copies(chunk, 3, part).start()

    def forward(chunk, part, number):
        axis = CHUNKS[chunk][0]
        rows = halves(chunk)[number]
        at = (position[axis] + (SIDE - 1, 1)[number]) % SIDE
        pair = pair_of(chunk, part)
        copies(chunk, number, part).wait_recv()

        def body(i, _):
            term = from_wire(recv_op[pair + i, rows, :], ONE) + share(axis, at, pair + i)[rows, :]
            send_fwd[pair + i, rows, :] = to_wire(term, TWO)
            return 0

        lax.fori_loop(0, 2, body, 0)
        copies(chunk, 4 + number, part).start()

    def finish(chunk, part):
        axis, row, first, second = CHUNKS[chunk]
        length = first + second
        p = position[axis]
        pair = pair_of(chunk, part)
        all_of(
            both.at[:, pl.ds(pair, 2), whole(chunk)], recv_sem.at[chunk * PER + 3 * part + 2]
        )

        def summed(i, rows):
            return (
                share(axis, p, i)[rows, :]
                + from_wire(recv_dir[i, rows, :], ONE)
                + from_wire(recv_fwd[i, rows, :], TWO)
            )

        paired = 64 if axis == "z" else 0
        if paired:
            rows = pl.ds(row, 64)
            low = low_lanes((64, 128))
            upper, lower = summed(pair, rows), summed(pair + 1, rows)
            first_sum[pair, rows, :] = jnp.where(low, upper, turn(lower))
            first_sum[pair + 1, rows, :] = jnp.where(low, turn(upper), lower)
        if paired < length:

            def plain(i, _):
                rows = pl.ds(row + paired, length - paired)
                first_sum[pair + i, rows, :] = summed(pair + i, rows)
                return 0

            lax.fori_loop(0, 2, plain, 0)

        p = position[other[axis]]
        a, b = halves(chunk)
        far, right, left = (p + 2) % SIDE, (p + 1) % SIDE, (p + SIDE - 1) % SIDE
        if part == 0:
            rows = whole(chunk)
            send_op2[rows, :] = to_wire(first_sum[far, rows, :], FOUR)
            copies(chunk, 6).start()
            copies(chunk, 7).start()
        else:
            send_dir2[a, :] = to_wire(first_sum[right, a, :], FOUR)
            copies(chunk, 8).start()
            send_dir2[b, :] = to_wire(first_sum[left, b, :], FOUR)
            copies(chunk, 9).start()

    def second_forward(chunk):
        p = position[other[CHUNKS[chunk][0]]]
        a, b = halves(chunk)
        right, left = (p + 1) % SIDE, (p + SIDE - 1) % SIDE
        all_of(recv_op2.at[whole(chunk)], recv_sem.at[chunk * PER + 6])
        for number, rows, at in ((6, a, left), (7, b, right)):
            part = from_wire(recv_op2[rows, :], FOUR) + first_sum[at, rows, :]
            send_fwd2[rows, :] = to_wire(part, EIGHT)
            copies(chunk, 4 + number).start()

    def second_finish(chunk):
        p = position[other[CHUNKS[chunk][0]]]
        all_of(both2.at[:, whole(chunk)], recv_sem.at[chunk * PER + 7])
        for rows in halves(chunk):
            mean[rows, :] = (
                first_sum[p, rows, :]
                + from_wire(recv_dir2[rows, :], FOUR)
                + from_wire(recv_fwd2[rows, :], EIGHT)
            ) * (SIDE * SIDE) ** (-0.5)

    def prepare():
        loaded(COUNT + 2, first_sum.at[0:2, 0:512], mean.at[0:512])
        loaded(COUNT + 4, params[6], params[7], states[6], states[7])
        for number, row, length in ((5, MIXED, 64), (1, DOWN, 256)):
            packed_param[pl.ds(row, length), :] = beside(params[number][...])
            packed_state[pl.ds(row, length), :] = beside(states[number][...])

    def row_squares(row, width, param, top, height):
        got = jnp.zeros((height, 128), jnp.float32)
        own = jnp.zeros((height, 128), jnp.float32)
        for c in range(width):
            m = mean[pl.ds(row + height * c, height), :]
            w = param[pl.ds(top, height), pl.ds(128 * c, 128)]
            got, own = got + m * m, own + w * w
        rest = [jnp.zeros((64 - height, 128), jnp.float32)] if height < 64 else []
        both = jnp.concatenate([got, *rest, own, *rest], axis=0)
        return jnp.sum(both, axis=1, keepdims=True)

    def column_squares(row, length):
        m = mean[pl.ds(row, length), :]
        w = packed_param[pl.ds(row, length), :]
        got = jnp.sum(m * m, axis=0, keepdims=True)
        own = jnp.sum(w * w, axis=0, keepdims=True)
        got, own = got + turn(got), own + turn(own)
        return jnp.where(low_lanes((1, 128)), got, own)

    def norm_copy(group, step):
        return pltpu.make_async_remote_copy(
            src_ref=squares.at[group, 0],
            dst_ref=squares.at[group, step],
            send_sem=send_sem.at[8],
            recv_sem=nrecv_sem.at[group],
            device_id=(replica, (model + step) % PEERS),
            device_id_type=MESH,
        )

    def norm_send(group):
        by_rows, by_columns = [], []
        if group in (0, 2):
            by_rows = [row_squares(UP + 64 * group, 4, params[0], 16 * group, 32)]
        if group == 1:
            by_rows = [row_squares(VALUE, 1, params[4], 0, 64)]
            by_columns = [column_squares(MIXED, 64)]
        if group == 3:
            by_rows = [
                row_squares(QUERY, 1, params[2], 0, 64),
                row_squares(KEY, 1, params[3], 0, 64),
            ]
        if group == 4:
            by_columns = [column_squares(DOWN, 256)]
        tile = jnp.zeros((8, 128), jnp.float32)
        if by_rows:
            lane = lax.broadcasted_iota(jnp.int32, (128, 128), 1)
            block = jnp.zeros((128, 128), jnp.float32)
            for k, column in enumerate(by_rows):
                block = jnp.where(lane == k, column, block)
            tile = block.T[0:8]
        sub = lax.broadcasted_iota(jnp.int32, (8, 128), 0)
        for k, line in enumerate(by_columns):
            tile = jnp.where(sub == len(by_rows) + k, line, tile)
        squares[group, 0] = tile
        for step in range(1, PEERS):
            norm_copy(group, step).start()

    ratios = {}

    def norm_ratios(group):
        all_of(squares.at[group, 1:PEERS], nrecv_sem.at[group])
        total = squares[group, 0]
        for step in range(1, PEERS):
            total = total + squares[group, step]
        low = low_lanes((8, 128))
        back = turn(total)
        got, own = jnp.where(low, total, back), jnp.where(low, back, total)
        ratio = jnp.sqrt(own) * lax.rsqrt(got + 1e-06)
        across = ratio
        down_rows = jnp.concatenate([ratio] * 16, axis=0).T if group != 4 else None
        ratios[group] = across, down_rows

    def stepped(m, param, state):
        state_new = hold_rate * state + (1.0 - hold_rate) * m * m
        return param - learn_rate * m * lax.rsqrt(state_new + 1e-06), state_new

    def updated(rows, m, param, state):
        scaled[rows, :] = m
        gathered[z, y, rows, :] = stepped(m, param, state)[0].astype(jnp.bfloat16)

    def row_update(row, width, ratio, number, top, height):
        for c in range(width):
            rows = pl.ds(row + height * c, height)
            at = (pl.ds(top, height), pl.ds(128 * c, 128))
            updated(rows, mean[rows, :] * ratio, params[number][at], states[number][at])

    def column_update(row, length, ratio):
        rows = pl.ds(row, length)
        updated(rows, mean[rows, :] * ratio, packed_param[rows, :], packed_state[rows, :])

    def update(chunk):
        across, down_rows = ratios[GATHERS[chunk][4]]
        if chunk in (0, 2):
            row_update(UP + 64 * chunk, 4, down_rows[0:32, 0:1], 0, 16 * chunk, 32)
        if chunk == 1:
            column_update(MIXED, 64, across[1:2])
            row_update(VALUE, 1, down_rows[0:64, 0:1], 4, 0, 64)
            small = pl.ds(SMALL, 16)
            updated(
                small,
                mean[small, :] * 2.0,
                jnp.concatenate([params[6][...], params[7][...]], axis=1),
                jnp.concatenate([states[6][...], states[7][...]], axis=1),
            )
        if chunk == 4:
            row_update(QUERY, 1, down_rows[0:64, 0:1], 2, 0, 64)
            row_update(KEY, 1, down_rows[0:64, 1:2], 3, 0, 64)
        if chunk in (3, 5):
            column_update(GATHERS[chunk][1], 128, across[0:1])

    def keep():
        def step(number, at, m):
            following[number][at], new[number][at] = stepped(
                m, params[number][at], states[number][at]
            )

        for part in range(2):
            for c in range(4):
                at = (pl.ds(32 * part, 32), pl.ds(128 * c, 128))
                step(0, at, scaled[pl.ds(UP + 128 * part + 32 * c, 32), :])
        everything = (slice(None), slice(None))
        for number, row in ((2, QUERY), (3, KEY), (4, VALUE)):
            step(number, everything, scaled[pl.ds(row, 64), :])
        for number, row, length in ((1, DOWN, 256), (5, MIXED, 64)):
            turned = scaled[pl.ds(row, length), :].T
            step(number, everything, jnp.concatenate([turned[:64], turned[64:]], axis=1))
        line = scaled[pl.ds(SMALL, 1), :]
        step(6, everything, line[:, :64])
        step(7, everything, turn(line)[:, :64])

    def gather_copies(chunk, number):
        name, row, first, second, _ = GATHERS[chunk]
        a, b = pl.ds(row, first), pl.ds(row + first, second)
        up_way = number % 2 == 0
        step = 1 if up_way else SIDE - 1
        behind = SIDE - 1 if up_way else 1
        p, q = position[name], position[other[name]]
        axis = name
        rows = whole(chunk, GATHERS)
        if number < 4:
            axis = other[name]
            if number >= 2:
                rows, q = (b if up_way else a), (q + behind) % SIDE
        else:
            block = (number - 4) // 2 % 4
            q = (q + (0, SIDE - 1, 1, 2)[block]) % SIDE
            if number >= 12:
                rows, p = (b if up_way else a), (p + behind) % SIDE
        ref = gathered.at[q, p, rows] if name == "y" else gathered.at[p, q, rows]
        arrival = min(number, 2) if number < 4 else min(number - 1, 11)
        return pltpu.make_async_remote_copy(
            src_ref=ref,
            dst_ref=ref,
            send_sem=send_sem.at[6 if number < 4 else 7],
            recv_sem=grecv_sem.at[chunk * PER_GATHER + arrival],
            device_id=place(axis, step),
            device_id_type=MESH,
        )

    def pass_on(chunk, awaited, started):
        for number in awaited:
            gather_copies(chunk, number).wait_recv()
        for number in started:
            gather_copies(chunk, number).start()

    def widen(chunk):
        number, row, start, length = {
            1: (1, MIXED, 0, 64),
            3: (0, DOWN, 0, 128),
            5: (0, DOWN, 128, 128),
        }[chunk]
        out = wides[number]
        half = out.shape[0] // 2
        low = low_lanes((length, 128))
        rows = pl.ds(row + start, length)
        for pair in range(8):
            lanes = pl.ds(128 * pair, 128)
            zz, yy = (2 * pair) // SIDE, (2 * pair) % SIDE
            a = gathered[zz, yy, rows, :].astype(jnp.float32)
            b = gathered[zz, yy + 1, rows, :].astype(jnp.float32)
            out[pl.ds(start, length), lanes] = jnp.where(low, a, turn(b)).astype(jnp.bfloat16)
            out[pl.ds(half + start, length), lanes] = jnp.where(low, turn(a), b).astype(
                jnp.bfloat16
            )

    def small_out():
        sub = lax.broadcasted_iota(jnp.int32, (8, 128), 0)
        low = low_lanes((1, 128))
        lines = [jnp.zeros((8, 128), jnp.float32)] * 2
        for pair in range(8):
            zz, yy = (2 * pair) // SIDE, (2 * pair) % SIDE
            a = gathered[zz, yy, pl.ds(SMALL, 16), :].astype(jnp.float32)[0:1]
            b = gathered[zz, yy + 1, pl.ds(SMALL, 16), :].astype(jnp.float32)[0:1]
            lines[0] = jnp.where(sub == pair, jnp.where(low, a, turn(b)), lines[0])
            lines[1] = jnp.where(sub == pair, jnp.where(low, turn(a), b), lines[1])
        for k in range(2):
            small_halves[k][...] = lines[k].astype(jnp.bfloat16)

    def end(chunk):
        all_of(gathered.at[0, :, whole(chunk, GATHERS)], grecv_sem.at[chunk * PER_GATHER + 11])
        if chunk in (1, 3, 5):
            widen(chunk)
        if chunk == 1:
            small_out()

    def act(name, k):
        part = int(name.endswith("O"))
        if name in ("soF", "soO"):
            send(k, part)
        elif name in ("sdF", "sdO"):
            send_direct(k, part)
        elif name[:4] in ("fwdA", "fwdB"):
            forward(k, part, int(name[3] == "B"))
        elif name in ("finF", "finO"):
            finish(k, part)
        elif name == "Fwd":
            second_forward(k)
        elif name == "Fin":
            second_finish(k)
        elif name == "prepare":
            prepare()
        elif name == "keep":
            keep()
        elif name == "norm":
            norm_send(k)
        elif name == "ratio":
            norm_ratios(k)
        elif name == "upd":
            update(k)
            pass_on(k, (), (0, 1, 4, 5))
        elif name == "xf+":
            pass_on(k, (0,), (2, 6, 7))
        elif name == "xf-":
            pass_on(k, (1,), (3, 8, 9))
        elif name == "far":
            all_of(gathered.at[0, 0, whole(k, GATHERS)], grecv_sem.at[k * PER_GATHER + 2])
            pass_on(k, (), (10, 11))
        elif name == "end":
            end(k)
        else:
            number = 4 + 2 * ("own", "l", "r", "f").index(name[:-2]) + int(name[-1] == "-")
            pass_on(k, (number,), (number + 8,))

    for name, k in ORDER:
        with stage(f"{name}_{k}"):
            act(name, k)

    with stage("sent"):
        for k, ref in enumerate((send_op, send_dir, send_fwd, send_op2, send_dir2, send_fwd2)):
            all_of(ref, send_sem.at[k])
        all_of(gathered.at[0, 0:3], send_sem.at[6])
        all_of(gathered.at[0:3], send_sem.at[7])
        all_of(squares.at[:, 1:PEERS], send_sem.at[8])


def output_kernel(*refs):
    gathered, laid, refs = refs[0], refs[1:21], refs[21:]
    half, rest, sem = refs[:8], refs[8:24], refs[24]
    pairs = []
    for part in range(2):
        for c in range(4):
            pairs.append(
                (
                    gathered.at[:, pl.ds(UP + 128 * part + 32 * c, 32), :],
                    half[0].at[:, pl.ds(32 * part, 32), pl.ds(128 * c, 128)],
                )
            )
    pairs.append((laid[0], half[1]))
    for number, row in ((2, QUERY), (3, KEY), (4, VALUE)):
        pairs.append((gathered.at[:, pl.ds(row, 64), :], half[number]))
    pairs += zip(laid[1:4], half[5:])
    pairs += zip(laid[4:], rest)
    started = [pltpu.make_async_copy(*pair, sem.at[k]) for k, pair in enumerate(pairs)]
    for copy in started:
        copy.start()
    for copy in started:
        copy.wait()


def stay(*arrays):
    return [pltpu.with_memory_space_constraint(a, pltpu.HBM) for a in arrays]


def local(*arrays):
    slopes, params, states = arrays[:8], arrays[8:16], arrays[16:]
    up, down, query, key, value, mixed, norm, bias = slopes

    def shown(group):
        up, down, query, key, value, mixed, norm, bias = group
        return up, down.T, query, key, value, mixed.T, norm[None], bias[None]

    params, states = shown(params), shown(states)
    vmem = pl.BlockSpec(memory_space=pltpu.VMEM)
    anywhere = pl.BlockSpec(memory_space=pl.ANY)
    f32, bf16 = jnp.float32, jnp.bfloat16
    wire = pltpu.VMEM((SIDE, ROWS, 128), bf16)
    wire2 = pltpu.VMEM((ROWS, 128), bf16)
    dma = pltpu.SemaphoreType.DMA
    held = [pltpu.VMEM(a.shape, f32) for a in params]
    gathered, *laid = pl.pallas_call(
        exchange_kernel,
        out_shape=(
            pltpu.VMEM((SIDE, SIDE, ROWS, 128), bf16),
            pltpu.VMEM((512, 1024), bf16),
            pltpu.VMEM((128, 1024), bf16),
            pltpu.VMEM((8, 128), bf16),
            pltpu.VMEM((8, 128), bf16),
            *held,
            *held,
        ),
        in_specs=[pl.BlockSpec(memory_space=pltpu.HBM)] * 24,
        out_specs=(vmem,) * 21,
        scratch_shapes=[
            *held,
            *held,
            pltpu.VMEM((ROWS, 128), f32),
            pltpu.VMEM((SIDE, SIDE, ROWS, 128), f32),
            pltpu.VMEM((1, 1024), f32),
            pltpu.VMEM((1, 1024), f32),
            pltpu.VMEM((ROWS, 128), f32),
            pltpu.VMEM((ROWS, 128), f32),
            *[wire] * 4,
            pltpu.VMEM((2, SIDE, ROWS, 128), bf16),
            pltpu.VMEM((SIDE, ROWS, 128), f32),
            *[wire2] * 4,
            pltpu.VMEM((2, ROWS, 128), bf16),
            pltpu.VMEM((ROWS, 128), f32),
            pltpu.VMEM((GROUPS, PEERS, 8, 128), f32),
            dma((LOADS,)),
            dma((SENDS,)),
            dma((COUNT * PER,)),
            dma((len(GATHERS) * PER_GATHER,)),
            dma((GROUPS,)),
        ],
        compiler_params=pltpu.CompilerParams(
            collective_id=0, has_side_effects=True, vmem_limit_bytes=40 * 2**20
        ),
        name="exchange",
    )(
        *stay(
            up.reshape(SIDE, SIDE, 64, 512),
            down.reshape(2, 256, 1024),
            query.reshape(SIDE, SIDE, 64, 128),
            key.reshape(SIDE, SIDE, 64, 128),
            value.reshape(SIDE, SIDE, 64, 128),
            mixed.reshape(2, 64, 1024),
            norm,
            bias,
            *params,
            *states,
        )
    )
    own = [jax.ShapeDtypeStruct(a.shape, f32) for a in params]
    full = [
        jax.ShapeDtypeStruct(s, bf16)
        for s in (
            (16, 64, 512),
            (512, 1024),
            (16, 64, 128),
            (16, 64, 128),
            (16, 64, 128),
            (128, 1024),
            (8, 128),
            (8, 128),
        )
    ]
    out = pl.pallas_call(
        output_kernel,
        out_shape=(*full, *own, *own),
        in_specs=[vmem] * 21,
        out_specs=(anywhere,) * 24,
        scratch_shapes=[dma((8 + 1 + 3 + 3 + 16,))],
        compiler_params=pltpu.CompilerParams(vmem_limit_bytes=8 * 2**20),
        name="outputs",
    )(gathered.reshape(SIDE * SIDE, ROWS, 128), *laid)
    half, following, new = out[:8], out[8:16], out[16:]
    half_up, half_down, half_query, half_key, half_value, half_mixed, half_norm, half_bias = half

    def back(group):
        up, down, query, key, value, mixed, norm, bias = group
        return up, down.T, query, key, value, mixed.T, norm[0], bias[0]

    return (
        half_up.reshape(1024, 512),
        half_down,
        half_query.reshape(1024, 128),
        half_key.reshape(1024, 128),
        half_value.reshape(1024, 128),
        half_mixed,
        half_norm.reshape(1024),
        half_bias.reshape(1024),
        *back(following),
        *back(new),
    )


def solution(mesh):
    def along(split):
        return [
            P(*(("replica", "model") if dim == 0 else ("model", "replica"))[:2])
            if dim < 2
            else P("replica")
            for dim in split
        ]

    shards = along((0, 1, 0, 0, 0, 1, 2, 2))
    slopes = [P("replica", None, "model"), P("replica", "model", None)]
    slopes = [slopes[k] for k in (0, 1, 0, 0, 0, 1)] + [P("replica", None)] * 2
    halves = [P(None, "model"), P("model", None)]
    halves = [halves[k] for k in (0, 1, 0, 0, 0, 1)] + [P()] * 2
    return jax.shard_map(
        local,
        mesh=mesh,
        in_specs=(*slopes, *shards, *shards),
        out_specs=(*halves, *shards, *shards),
        check_vma=False,
    )
```

```python
import contextlib
import math

import jax
import jax.numpy as jnp
from jax import lax
from jax.experimental import pallas as pl
from jax.experimental.pallas import tpu as pltpu
from jax.sharding import PartitionSpec as P

learn_rate = 0.025
hold_rate = 0.7
MESH = pl.DeviceIdType.MESH
SIDE = 4
PEERS = 8

UP, QUERY, KEY, MIXED, VALUE, SMALL, DOWN, ROWS = 0, 256, 320, 384, 448, 512, 528, 784

CHUNKS = (
    ("y", UP, 32, 32),
    ("z", MIXED, 80, 64),
    ("y", UP + 64, 32, 32),
    ("y", UP + 128, 32, 32),
    ("z", DOWN, 32, 32),
    ("y", UP + 192, 32, 32),
    ("z", DOWN + 64, 32, 32),
    ("y", QUERY, 64, 64),
    ("z", DOWN + 128, 32, 32),
    ("z", DOWN + 192, 32, 32),
)
GATHERS = (
    ("y", UP, 64, 64, 0),
    ("z", MIXED, 80, 64, 1),
    ("y", UP + 128, 64, 64, 2),
    ("z", DOWN, 64, 64, 4),
    ("y", QUERY, 64, 64, 3),
    ("z", DOWN + 128, 64, 64, 4),
)
COUNT = len(CHUNKS)
GROUPS = 5
PER = 6
PER_GATHER = 7
LOADS = COUNT + 8
SENDS = 9

ORDER = (
    ("soF", 0), ("soF", 1), ("soO", 0), ("sdF", 0), ("sdF", 1), ("soF", 4), ("soF", 2), ("soF", 7),
    ("sdF", 7), ("soO", 1), ("soO", 3), ("soO", 5), ("sdO", 1), ("soF", 3), ("fwdF", 1),
    ("soF", 9), ("soF", 8), ("soO", 7), ("sdF", 4), ("fwdF", 0), ("soO", 6), ("fwdF", 7),
    ("fwdO", 1), ("fwdF", 2), ("soF", 6), ("soF", 5), ("sdO", 7), ("sdF", 8), ("fwdF", 4),
    ("finF", 1), ("fwdO", 7), ("fwdF", 8), ("soO", 2), ("sdO", 2), ("soO", 8), ("finF", 7),
    ("soO", 4), ("sdF", 2), ("fwdF", 9), ("sdF", 9), ("prepare", 0), ("finF", 0), ("sdF", 5),
    ("finO", 1), ("Fwd", 1), ("sdO", 8), ("fwdF", 6), ("sdO", 0), ("fwdF", 5), ("finF", 8),
    ("soO", 9), ("sdF", 3), ("finO", 7), ("Fwd", 7), ("fwdO", 2), ("sdF", 6), ("fwdO", 0),
    ("fwdO", 8), ("fwdO", 4), ("fwdF", 3), ("sdO", 3), ("finF", 2), ("sdO", 9), ("fwdO", 3),
    ("sdO", 4), ("Fin", 1), ("norm", 1), ("fwdO", 9), ("finF", 9), ("sdO", 6), ("fwdO", 6),
    ("finF", 4), ("Fin", 7), ("norm", 3), ("finF", 5), ("finF", 6), ("finO", 0), ("Fwd", 0),
    ("sdO", 5), ("fwdO", 5), ("finF", 3), ("finO", 2), ("Fwd", 2), ("finO", 8), ("Fwd", 8),
    ("finO", 4), ("Fwd", 4), ("finO", 9), ("Fwd", 9), ("finO", 6), ("Fwd", 6), ("finO", 3),
    ("Fin", 0), ("finO", 5), ("Fwd", 5), ("Fwd", 3), ("Fin", 8), ("Fin", 2), ("norm", 0),
    ("ratio", 1), ("upd", 1), ("Fin", 9), ("Fin", 4), ("Fin", 6), ("norm", 4), ("ratio", 3),
    ("upd", 4), ("Fin", 5), ("Fin", 3), ("norm", 2), ("xf", 1), ("ownF", 1), ("ownF", 4),
    ("xf", 4), ("ratio", 0), ("upd", 0), ("far", 1), ("ratio", 4), ("upd", 3), ("upd", 5),
    ("ratio", 2), ("upd", 2), ("keep", 0), ("lF", 1), ("xf", 0), ("xf", 3), ("xf", 5), ("ownF", 0),
    ("xf", 2), ("rF", 4), ("far", 0), ("lF", 3), ("far", 4), ("far", 5), ("rF", 0), ("far", 3),
    ("lF", 4), ("rF", 1), ("rF", 5), ("ownF", 5), ("far", 2), ("rF", 3), ("lF", 2), ("lF", 0),
    ("lF", 5), ("fF", 5), ("fF", 0), ("ownF", 2), ("ownF", 3), ("fF", 4), ("fF", 3), ("rF", 2),
    ("fF", 1), ("fF", 2), ("end", 5), ("end", 0), ("end", 3), ("end", 4), ("end", 1), ("end", 2),
)


SPAN, BASE = 251 * math.log(2.0), 125 * math.log(2.0)
ONE, TWO, FOUR, EIGHT = 4.0, 8.0, 16.0, 32.0


def to_wire(x, bound):
    level = jnp.exp(jnp.log(jnp.abs(x)) * (1.0 / 6.0) + math.log(SPAN * bound ** (-1.0 / 6.0)))
    size = jnp.exp(level - BASE)
    return jnp.where(x < 0.0, -size, size).astype(jnp.bfloat16)


def from_wire(c, bound):
    c = c.astype(jnp.float32)
    level = (jnp.log(jnp.abs(c)) + BASE) * (bound ** (1.0 / 6.0) / SPAN)
    square = level * level
    size = square * square * square
    return jnp.where(c < 0.0, -size, size)


def low_lanes(shape):
    return lax.broadcasted_iota(jnp.int32, shape, len(shape) - 1) < 64


def turn(x):
    return pltpu.roll(x, 64, 1)


def beside(x):
    half = x.shape[1] // 2
    return jnp.concatenate([x[:, :half], x[:, half:]], axis=0).T


def stage(name):
    return contextlib.nullcontext()


def exchange_kernel(*refs):
    slopes, given, refs = refs[:8], refs[8:24], refs[24:]
    gathered, wide_down, wide_mixed, small_norm, small_bias, refs = *refs[:5], refs[5:]
    following, new, refs = refs[:8], refs[8:16], refs[16:]
    params, states, refs = refs[:8], refs[8:16], refs[16:]
    exchange(
        slopes,
        given,
        gathered,
        (wide_down, wide_mixed),
        (small_norm, small_bias),
        following,
        new,
        params,
        states,
        *refs,
    )


def exchange(
    slopes,
    given,
    gathered,
    wides,
    small_halves,
    following,
    new,
    params,
    states,
    scaled,
    mine,
    raw_norm,
    raw_bias,
    packed_param,
    packed_state,
    send_op,
    send_dir,
    send_fwd,
    recv_op,
    both,
    first_sum,
    send_op2,
    send_dir2,
    send_fwd2,
    recv_op2,
    both2,
    mean,
    squares,
    load_sem,
    send_sem,
    recv_sem,
    grecv_sem,
    nrecv_sem,
):
    up, down, query, key, value, mixed, norm, bias = slopes
    recv_rest = recv_dir, recv_fwd = both.at[0], both.at[1]
    recv_rest2 = recv_dir2, recv_fwd2 = both2.at[0], both2.at[1]
    replica = lax.axis_index("replica")
    model = lax.axis_index("model")
    z, y = replica // SIDE, replica % SIDE

    def place(axis, step):
        if axis == "y":
            return (z * SIDE + (y + step) % SIDE, model)
        return (((z + step) % SIDE) * SIDE + y, model)

    position = {"y": y, "z": z}
    other = {"y": "z", "z": "y"}

    def all_of(ref, sem):
        pltpu.make_async_copy(ref, ref, sem).wait()

    def load(number, pairs):
        for src, dst in pairs:
            pltpu.make_async_copy(src, dst, load_sem.at[number]).start()

    def loaded(number, *refs):
        for k, ref in enumerate(refs):
            all_of(ref, load_sem.at[number + k])

    def whole(chunk, table=CHUNKS):
        _, row, first, second, *_ = table[chunk]
        return pl.ds(row, first + second)

    def up_part(part, columns):
        return [
            (
                up.at[:, :, pl.ds(32 * part, 32), pl.ds(128 * c, 128)],
                mine.at[:, :, pl.ds(UP + 128 * part + 32 * c, 32), :],
            )
            for c in columns
        ]

    def columns(array, row, start, length):
        return [
            (
                array.at[:, pl.ds(start, length), pl.ds(128 * k, 128)],
                mine.at[k // 2, pl.ds(2 * (k % 2), 2), pl.ds(row + start, length), :],
            )
            for k in range(8)
        ]

    load(0, up_part(0, (0, 1)))
    load(
        1,
        [
            *columns(mixed, MIXED, 0, 64),
            (value, mine.at[:, :, pl.ds(VALUE, 64), :]),
        ],
    )
    load(COUNT, [(norm, raw_norm)])
    load(COUNT + 1, [(bias, raw_bias)])
    barrier = pltpu.get_barrier_semaphore()
    for axis in ("y", "z"):
        for step in (1, SIDE - 1):
            pl.semaphore_signal(barrier, 1, device_id=place(axis, step), device_id_type=MESH)
    for step in range(1, PEERS):
        pl.semaphore_signal(
            barrier, 1, device_id=(replica, (model + step) % PEERS), device_id_type=MESH
        )
    waiting = [True]

    def load_rest():
        load(2, up_part(0, (2, 3)))
        load(3, up_part(1, (0, 1)))
        load(4, columns(down, DOWN, 0, 64))
        load(5, up_part(1, (2, 3)))
        load(6, columns(down, DOWN, 64, 64))
        load(7, [(query, mine.at[:, :, pl.ds(QUERY, 64), :]), (key, mine.at[:, :, pl.ds(KEY, 64), :])])
        load(8, columns(down, DOWN, 128, 64))
        load(9, columns(down, DOWN, 192, 64))
        held = [*zip(given, (*params, *states))]
        load(COUNT + 2, [held[k] for k in (0, 1, 8, 9)])
        load(COUNT + 3, [held[k] for k in (2, 3, 4, 5, 10, 11, 12, 13)])
        for k, pair in enumerate((held[6], held[7], held[14], held[15])):
            load(COUNT + 4 + k, [pair])

    def pack_small():
        low = low_lanes((1, 128))
        for pair in range(8):
            lanes = pl.ds(128 * pair, 128)
            zz, yy = (2 * pair) // SIDE, (2 * pair) % SIDE
            a = raw_norm[:, lanes] * 0.5
            b = raw_bias[:, lanes] * 0.5
            mine[zz, yy, pl.ds(SMALL, 16), :] = jnp.broadcast_to(
                jnp.where(low, a, turn(b)), (16, 128)
            )
            mine[zz, yy + 1, pl.ds(SMALL, 16), :] = jnp.broadcast_to(
                jnp.where(low, turn(a), b), (16, 128)
            )

    def halves(chunk):
        _, row, first, second = CHUNKS[chunk]
        return pl.ds(row, first), pl.ds(row + first, second)

    def pair_of(chunk, part):
        own = position[other[CHUNKS[chunk][0]]] // 2
        return 2 * own if part else 2 - 2 * own

    def share(axis, at, b):
        if axis == "y":
            return mine.at[b, at]
        return mine.at[at, b]

    def copies(chunk, number, part=0):
        axis = CHUNKS[chunk][0]
        a, b = halves(chunk)
        second = number >= 6
        if second:
            axis = other[axis]
            sources, targets = (send_op2, send_dir2, send_fwd2), (recv_op2, *recv_rest2)
        else:
            sources, targets = (send_op, send_dir, send_fwd), (recv_op, *recv_rest)
        kind, half = divmod(number % 6, 2)
        rows = b if half else a
        at = (rows, slice(None))
        if not second:
            at = (pl.ds(pair_of(chunk, part), 2), *at)
        step = (SIDE - 1, 1)[half] if kind != 1 else (1, SIDE - 1)[half]
        if second:
            arrival = 4 if kind == 0 else 5
        else:
            arrival = 2 * part + (kind > 0)
        return pltpu.make_async_remote_copy(
            src_ref=sources[kind].at[at],
            dst_ref=targets[kind].at[at],
            send_sem=send_sem.at[3 * second + kind],
            recv_sem=recv_sem.at[chunk * PER + arrival],
            device_id=place(axis, step),
            device_id_type=MESH,
        )

    ready = set()

    def send(chunk, part):
        if chunk not in ready:
            ready.add(chunk)
            if chunk == 1:
                loaded(chunk, mine.at[:, :, pl.ds(MIXED, 128)])
                loaded(COUNT, raw_norm, raw_bias)
                pack_small()
            else:
                loaded(chunk, mine.at[:, :, whole(chunk)])
        axis = CHUNKS[chunk][0]
        far = (position[axis] + 2) % SIDE
        pair, rows = pair_of(chunk, part), whole(chunk)

        def op(i, _):
            send_op[pair + i, rows, :] = to_wire(share(axis, far, pair + i)[rows, :], ONE)
            return 0

        lax.fori_loop(0, 2, op, 0)
        if waiting:
            waiting.pop()
            load_rest()
            pl.semaphore_wait(barrier, 4 + PEERS - 1)
        copies(chunk, 0, part).start()
        copies(chunk, 1, part).start()

    def send_direct(chunk, part):
        axis = CHUNKS[chunk][0]
        p = position[axis]
        a, b = halves(chunk)
        right, left = (p + 1) % SIDE, (p + SIDE - 1) % SIDE
        pair = pair_of(chunk, part)

        def direct(i, _):
            send_dir[pair + i, a, :] = to_wire(share(axis, right, pair + i)[a, :], ONE)
            send_dir[pair + i, b, :] = to_wire(share(axis, left, pair + i)[b, :], ONE)
            return 0

        lax.fori_loop(0, 2, direct, 0)
        copies(chunk, 2, part).start()
        copies(chunk, 3, part).start()

    def forward(chunk, part):
        axis = CHUNKS[chunk][0]
        a, b = halves(chunk)
        right, left = (position[axis] + 1) % SIDE, (position[axis] + SIDE - 1) % SIDE
        pair = pair_of(chunk, part)
        all_of(recv_op.at[pl.ds(pair, 2), whole(chunk)], recv_sem.at[chunk * PER + 2 * part])
        for number, rows, at in ((4, a, left), (5, b, right)):

            def body(i, _):
                own = share(axis, at, pair + i)[rows, :]
                term = from_wire(recv_op[pair + i, rows, :], ONE) + own
                send_fwd[pair + i, rows, :] = to_wire(term, TWO)
                return 0

            lax.fori_loop(0, 2, body, 0)
            copies(chunk, number, part).start()

    def finish(chunk, part):
        axis, row, first, second = CHUNKS[chunk]
        length = first + second
        p = position[axis]
        pair = pair_of(chunk, part)
        all_of(
            both.at[:, pl.ds(pair, 2), whole(chunk)], recv_sem.at[chunk * PER + 2 * part + 1]
        )

        def summed(i, rows):
            return (
                share(axis, p, i)[rows, :]
                + from_wire(recv_dir[i, rows, :], ONE)
                + from_wire(recv_fwd[i, rows, :], TWO)
            )

        paired = 64 if axis == "z" else 0
        if paired:
            rows = pl.ds(row, 64)
            low = low_lanes((64, 128))
            upper, lower = summed(pair, rows), summed(pair + 1, rows)
            first_sum[pair, rows, :] = jnp.where(low, upper, turn(lower))
            first_sum[pair + 1, rows, :] = jnp.where(low, turn(upper), lower)
        if paired < length:

            def plain(i, _):
                rows = pl.ds(row + paired, length - paired)
                first_sum[pair + i, rows, :] = summed(pair + i, rows)
                return 0

            lax.fori_loop(0, 2, plain, 0)

        p = position[other[axis]]
        a, b = halves(chunk)
        far, right, left = (p + 2) % SIDE, (p + 1) % SIDE, (p + SIDE - 1) % SIDE
        if part == 0:
            rows = whole(chunk)
            send_op2[rows, :] = to_wire(first_sum[far, rows, :], FOUR)
            copies(chunk, 6).start()
            copies(chunk, 7).start()
        else:
            send_dir2[a, :] = to_wire(first_sum[right, a, :], FOUR)
            copies(chunk, 8).start()
            send_dir2[b, :] = to_wire(first_sum[left, b, :], FOUR)
            copies(chunk, 9).start()

    def second_forward(chunk):
        p = position[other[CHUNKS[chunk][0]]]
        a, b = halves(chunk)
        right, left = (p + 1) % SIDE, (p + SIDE - 1) % SIDE
        all_of(recv_op2.at[whole(chunk)], recv_sem.at[chunk * PER + 4])
        for number, rows, at in ((6, a, left), (7, b, right)):
            part = from_wire(recv_op2[rows, :], FOUR) + first_sum[at, rows, :]
            send_fwd2[rows, :] = to_wire(part, EIGHT)
            copies(chunk, 4 + number).start()

    def second_finish(chunk):
        p = position[other[CHUNKS[chunk][0]]]
        all_of(both2.at[:, whole(chunk)], recv_sem.at[chunk * PER + 5])
        for rows in halves(chunk):
            mean[rows, :] = (
                first_sum[p, rows, :]
                + from_wire(recv_dir2[rows, :], FOUR)
                + from_wire(recv_fwd2[rows, :], EIGHT)
            ) * (SIDE * SIDE) ** (-0.5)

    def prepare():
        loaded(COUNT + 2, first_sum.at[0:2, 0:512], mean.at[0:512])
        loaded(COUNT + 4, params[6], params[7], states[6], states[7])
        for number, row, length in ((5, MIXED, 64), (1, DOWN, 256)):
            packed_param[pl.ds(row, length), :] = beside(params[number][...])
            packed_state[pl.ds(row, length), :] = beside(states[number][...])

    def row_squares(row, width, param, top, height):
        got = jnp.zeros((height, 128), jnp.float32)
        own = jnp.zeros((height, 128), jnp.float32)
        for c in range(width):
            m = mean[pl.ds(row + height * c, height), :]
            w = param[pl.ds(top, height), pl.ds(128 * c, 128)]
            got, own = got + m * m, own + w * w
        rest = [jnp.zeros((64 - height, 128), jnp.float32)] if height < 64 else []
        both = jnp.concatenate([got, *rest, own, *rest], axis=0)
        return jnp.sum(both, axis=1, keepdims=True)

    def column_squares(row, length):
        m = mean[pl.ds(row, length), :]
        w = packed_param[pl.ds(row, length), :]
        got = jnp.sum(m * m, axis=0, keepdims=True)
        own = jnp.sum(w * w, axis=0, keepdims=True)
        got, own = got + turn(got), own + turn(own)
        return jnp.where(low_lanes((1, 128)), got, own)

    def norm_copy(group, step):
        return pltpu.make_async_remote_copy(
            src_ref=squares.at[group, 0],
            dst_ref=squares.at[group, step],
            send_sem=send_sem.at[8],
            recv_sem=nrecv_sem.at[group],
            device_id=(replica, (model + step) % PEERS),
            device_id_type=MESH,
        )

    def norm_send(group):
        by_rows, by_columns = [], []
        if group in (0, 2):
            by_rows = [row_squares(UP + 64 * group, 4, params[0], 16 * group, 32)]
        if group == 1:
            by_rows = [row_squares(VALUE, 1, params[4], 0, 64)]
            by_columns = [column_squares(MIXED, 64)]
        if group == 3:
            by_rows = [
                row_squares(QUERY, 1, params[2], 0, 64),
                row_squares(KEY, 1, params[3], 0, 64),
            ]
        if group == 4:
            by_columns = [column_squares(DOWN, 256)]
        tile = jnp.zeros((8, 128), jnp.float32)
        if by_rows:
            lane = lax.broadcasted_iota(jnp.int32, (128, 128), 1)
            block = jnp.zeros((128, 128), jnp.float32)
            for k, column in enumerate(by_rows):
                block = jnp.where(lane == k, column, block)
            tile = block.T[0:8]
        sub = lax.broadcasted_iota(jnp.int32, (8, 128), 0)
        for k, line in enumerate(by_columns):
            tile = jnp.where(sub == len(by_rows) + k, line, tile)
        squares[group, 0] = tile
        for step in range(1, PEERS):
            norm_copy(group, step).start()

    ratios = {}

    def norm_ratios(group):
        all_of(squares.at[group, 1:PEERS], nrecv_sem.at[group])
        total = squares[group, 0]
        for step in range(1, PEERS):
            total = total + squares[group, step]
        low = low_lanes((8, 128))
        back = turn(total)
        got, own = jnp.where(low, total, back), jnp.where(low, back, total)
        ratio = jnp.sqrt(own) * lax.rsqrt(got + 1e-06)
        across = ratio
        down_rows = jnp.concatenate([ratio] * 16, axis=0).T if group != 4 else None
        ratios[group] = across, down_rows

    def stepped(m, param, state):
        state_new = hold_rate * state + (1.0 - hold_rate) * m * m
        return param - learn_rate * m * lax.rsqrt(state_new + 1e-06), state_new

    def updated(rows, m, param, state):
        scaled[rows, :] = m
        gathered[z, y, rows, :] = stepped(m, param, state)[0].astype(jnp.bfloat16)

    def row_update(row, width, ratio, number, top, height):
        for c in range(width):
            rows = pl.ds(row + height * c, height)
            at = (pl.ds(top, height), pl.ds(128 * c, 128))
            updated(rows, mean[rows, :] * ratio, params[number][at], states[number][at])

    def column_update(row, length, ratio):
        rows = pl.ds(row, length)
        updated(rows, mean[rows, :] * ratio, packed_param[rows, :], packed_state[rows, :])

    def update(chunk):
        across, down_rows = ratios[GATHERS[chunk][4]]
        if chunk in (0, 2):
            row_update(UP + 64 * chunk, 4, down_rows[0:32, 0:1], 0, 16 * chunk, 32)
        if chunk == 1:
            column_update(MIXED, 64, across[1:2])
            row_update(VALUE, 1, down_rows[0:64, 0:1], 4, 0, 64)
            small = pl.ds(SMALL, 16)
            updated(
                small,
                mean[small, :] * 2.0,
                jnp.concatenate([params[6][...], params[7][...]], axis=1),
                jnp.concatenate([states[6][...], states[7][...]], axis=1),
            )
        if chunk == 4:
            row_update(QUERY, 1, down_rows[0:64, 0:1], 2, 0, 64)
            row_update(KEY, 1, down_rows[0:64, 1:2], 3, 0, 64)
        if chunk in (3, 5):
            column_update(GATHERS[chunk][1], 128, across[0:1])

    def keep():
        def step(number, at, m):
            following[number][at], new[number][at] = stepped(
                m, params[number][at], states[number][at]
            )

        for part in range(2):
            for c in range(4):
                at = (pl.ds(32 * part, 32), pl.ds(128 * c, 128))
                step(0, at, scaled[pl.ds(UP + 128 * part + 32 * c, 32), :])
        everything = (slice(None), slice(None))
        for number, row in ((2, QUERY), (3, KEY), (4, VALUE)):
            step(number, everything, scaled[pl.ds(row, 64), :])
        for number, row, length in ((1, DOWN, 256), (5, MIXED, 64)):
            turned = scaled[pl.ds(row, length), :].T
            step(number, everything, jnp.concatenate([turned[:64], turned[64:]], axis=1))
        line = scaled[pl.ds(SMALL, 1), :]
        step(6, everything, line[:, :64])
        step(7, everything, turn(line)[:, :64])

    def gather_copies(chunk, number):
        name, row, first, second, _ = GATHERS[chunk]
        a, b = pl.ds(row, first), pl.ds(row + first, second)
        up_way = number % 2 == 0
        step = 1 if up_way else SIDE - 1
        behind = SIDE - 1 if up_way else 1
        p, q = position[name], position[other[name]]
        axis = name
        rows = whole(chunk, GATHERS)
        if number < 4:
            axis = other[name]
            if number >= 2:
                rows, q = (b if up_way else a), (q + behind) % SIDE
        else:
            block = (number - 4) // 2 % 4
            q = (q + (0, SIDE - 1, 1, 2)[block]) % SIDE
            if number >= 12:
                rows, p = (b if up_way else a), (p + behind) % SIDE
        ref = gathered.at[q, p, rows] if name == "y" else gathered.at[p, q, rows]
        arrival = min(number // 2, 6)
        return pltpu.make_async_remote_copy(
            src_ref=ref,
            dst_ref=ref,
            send_sem=send_sem.at[6 if number < 4 else 7],
            recv_sem=grecv_sem.at[chunk * PER_GATHER + arrival],
            device_id=place(axis, step),
            device_id_type=MESH,
        )

    def pass_on(chunk, arrival, started):
        rows = whole(chunk, GATHERS)
        if arrival is not None:
            ref = gathered.at[0, 0:2, rows]
            if arrival == 1:
                ref = gathered.at[0, 0, rows]
            if arrival == 6:
                ref = gathered.at[0, :, rows]
            all_of(ref, grecv_sem.at[chunk * PER_GATHER + arrival])
        for number in started:
            gather_copies(chunk, number).start()

    def widen(chunk):
        number, row, start, length = {
            1: (1, MIXED, 0, 64),
            3: (0, DOWN, 0, 128),
            5: (0, DOWN, 128, 128),
        }[chunk]
        out = wides[number]
        half = out.shape[0] // 2
        low = low_lanes((length, 128))
        rows = pl.ds(row + start, length)
        for pair in range(8):
            lanes = pl.ds(128 * pair, 128)
            zz, yy = (2 * pair) // SIDE, (2 * pair) % SIDE
            a = gathered[zz, yy, rows, :].astype(jnp.float32)
            b = gathered[zz, yy + 1, rows, :].astype(jnp.float32)
            out[pl.ds(start, length), lanes] = jnp.where(low, a, turn(b)).astype(jnp.bfloat16)
            out[pl.ds(half + start, length), lanes] = jnp.where(low, turn(a), b).astype(
                jnp.bfloat16
            )

    def small_out():
        sub = lax.broadcasted_iota(jnp.int32, (8, 128), 0)
        low = low_lanes((1, 128))
        lines = [jnp.zeros((8, 128), jnp.float32)] * 2
        for pair in range(8):
            zz, yy = (2 * pair) // SIDE, (2 * pair) % SIDE
            a = gathered[zz, yy, pl.ds(SMALL, 16), :].astype(jnp.float32)[0:1]
            b = gathered[zz, yy + 1, pl.ds(SMALL, 16), :].astype(jnp.float32)[0:1]
            lines[0] = jnp.where(sub == pair, jnp.where(low, a, turn(b)), lines[0])
            lines[1] = jnp.where(sub == pair, jnp.where(low, turn(a), b), lines[1])
        for k in range(2):
            small_halves[k][...] = lines[k].astype(jnp.bfloat16)

    def end(chunk):
        pass_on(chunk, 6, ())
        if chunk in (1, 3, 5):
            widen(chunk)
        if chunk == 1:
            small_out()

    def act(name, k):
        part = int(name.endswith("O"))
        if name in ("soF", "soO"):
            send(k, part)
        elif name in ("sdF", "sdO"):
            send_direct(k, part)
        elif name in ("fwdF", "fwdO"):
            forward(k, part)
        elif name in ("finF", "finO"):
            finish(k, part)
        elif name == "Fwd":
            second_forward(k)
        elif name == "Fin":
            second_finish(k)
        elif name == "prepare":
            prepare()
        elif name == "keep":
            keep()
        elif name == "norm":
            norm_send(k)
        elif name == "ratio":
            norm_ratios(k)
        elif name == "upd":
            update(k)
            pass_on(k, None, (0, 1, 4, 5))
        elif name == "xf":
            pass_on(k, 0, (2, 3, 6, 7, 8, 9))
        elif name == "far":
            pass_on(k, 1, (10, 11))
        elif name == "end":
            end(k)
        else:
            block = ("own", "l", "r", "f").index(name[:-1])
            pass_on(k, 2 + block, (12 + 2 * block, 13 + 2 * block))

    for name, k in ORDER:
        with stage(f"{name}_{k}"):
            act(name, k)

    with stage("sent"):
        for k, ref in enumerate((send_op, send_dir, send_fwd, send_op2, send_dir2, send_fwd2)):
            all_of(ref, send_sem.at[k])
        all_of(gathered.at[0, 0:3], send_sem.at[6])
        all_of(gathered.at[0:3], send_sem.at[7])
        all_of(squares.at[:, 1:PEERS], send_sem.at[8])


def output_kernel(*refs):
    gathered, laid, refs = refs[0], refs[1:21], refs[21:]
    half, rest, sem = refs[:8], refs[8:24], refs[24]
    pairs = []
    for part in range(2):
        for c in range(4):
            pairs.append(
                (
                    gathered.at[:, pl.ds(UP + 128 * part + 32 * c, 32), :],
                    half[0].at[:, pl.ds(32 * part, 32), pl.ds(128 * c, 128)],
                )
            )
    pairs.append((laid[0], half[1]))
    for number, row in ((2, QUERY), (3, KEY), (4, VALUE)):
        pairs.append((gathered.at[:, pl.ds(row, 64), :], half[number]))
    pairs += zip(laid[1:4], half[5:])
    pairs += zip(laid[4:], rest)
    started = [pltpu.make_async_copy(*pair, sem.at[k]) for k, pair in enumerate(pairs)]
    for copy in started:
        copy.start()
    for copy in started:
        copy.wait()


def stay(*arrays):
    return [pltpu.with_memory_space_constraint(a, pltpu.HBM) for a in arrays]


def local(*arrays):
    slopes, params, states = arrays[:8], arrays[8:16], arrays[16:]
    up, down, query, key, value, mixed, norm, bias = slopes

    def shown(group):
        up, down, query, key, value, mixed, norm, bias = group
        return up, down.T, query, key, value, mixed.T, norm[None], bias[None]

    params, states = shown(params), shown(states)
    vmem = pl.BlockSpec(memory_space=pltpu.VMEM)
    anywhere = pl.BlockSpec(memory_space=pl.ANY)
    f32, bf16 = jnp.float32, jnp.bfloat16
    wire = pltpu.VMEM((SIDE, ROWS, 128), bf16)
    wire2 = pltpu.VMEM((ROWS, 128), bf16)
    dma = pltpu.SemaphoreType.DMA
    held = [pltpu.VMEM(a.shape, f32) for a in params]
    gathered, *laid = pl.pallas_call(
        exchange_kernel,
        out_shape=(
            pltpu.VMEM((SIDE, SIDE, ROWS, 128), bf16),
            pltpu.VMEM((512, 1024), bf16),
            pltpu.VMEM((128, 1024), bf16),
            pltpu.VMEM((8, 128), bf16),
            pltpu.VMEM((8, 128), bf16),
            *held,
            *held,
        ),
        in_specs=[pl.BlockSpec(memory_space=pltpu.HBM)] * 24,
        out_specs=(vmem,) * 21,
        scratch_shapes=[
            *held,
            *held,
            pltpu.VMEM((ROWS, 128), f32),
            pltpu.VMEM((SIDE, SIDE, ROWS, 128), f32),
            pltpu.VMEM((1, 1024), f32),
            pltpu.VMEM((1, 1024), f32),
            pltpu.VMEM((ROWS, 128), f32),
            pltpu.VMEM((ROWS, 128), f32),
            *[wire] * 4,
            pltpu.VMEM((2, SIDE, ROWS, 128), bf16),
            pltpu.VMEM((SIDE, ROWS, 128), f32),
            *[wire2] * 4,
            pltpu.VMEM((2, ROWS, 128), bf16),
            pltpu.VMEM((ROWS, 128), f32),
            pltpu.VMEM((GROUPS, PEERS, 8, 128), f32),
            dma((LOADS,)),
            dma((SENDS,)),
            dma((COUNT * PER,)),
            dma((len(GATHERS) * PER_GATHER,)),
            dma((GROUPS,)),
        ],
        compiler_params=pltpu.CompilerParams(
            collective_id=0, has_side_effects=True, vmem_limit_bytes=40 * 2**20
        ),
        name="exchange",
    )(
        *stay(
            up.reshape(SIDE, SIDE, 64, 512),
            down.reshape(2, 256, 1024),
            query.reshape(SIDE, SIDE, 64, 128),
            key.reshape(SIDE, SIDE, 64, 128),
            value.reshape(SIDE, SIDE, 64, 128),
            mixed.reshape(2, 64, 1024),
            norm,
            bias,
            *params,
            *states,
        )
    )
    own = [jax.ShapeDtypeStruct(a.shape, f32) for a in params]
    full = [
        jax.ShapeDtypeStruct(s, bf16)
        for s in (
            (16, 64, 512),
            (512, 1024),
            (16, 64, 128),
            (16, 64, 128),
            (16, 64, 128),
            (128, 1024),
            (8, 128),
            (8, 128),
        )
    ]
    out = pl.pallas_call(
        output_kernel,
        out_shape=(*full, *own, *own),
        in_specs=[vmem] * 21,
        out_specs=(anywhere,) * 24,
        scratch_shapes=[dma((8 + 1 + 3 + 3 + 16,))],
        compiler_params=pltpu.CompilerParams(vmem_limit_bytes=8 * 2**20),
        name="outputs",
    )(gathered.reshape(SIDE * SIDE, ROWS, 128), *laid)
    half, following, new = out[:8], out[8:16], out[16:]
    half_up, half_down, half_query, half_key, half_value, half_mixed, half_norm, half_bias = half

    def back(group):
        up, down, query, key, value, mixed, norm, bias = group
        return up, down.T, query, key, value, mixed.T, norm[0], bias[0]

    return (
        half_up.reshape(1024, 512),
        half_down,
        half_query.reshape(1024, 128),
        half_key.reshape(1024, 128),
        half_value.reshape(1024, 128),
        half_mixed,
        half_norm.reshape(1024),
        half_bias.reshape(1024),
        *back(following),
        *back(new),
    )


def solution(mesh):
    def along(split):
        return [
            P(*(("replica", "model") if dim == 0 else ("model", "replica"))[:2])
            if dim < 2
            else P("replica")
            for dim in split
        ]

    shards = along((0, 1, 0, 0, 0, 1, 2, 2))
    slopes = [P("replica", None, "model"), P("replica", "model", None)]
    slopes = [slopes[k] for k in (0, 1, 0, 0, 0, 1)] + [P("replica", None)] * 2
    halves = [P(None, "model"), P("model", None)]
    halves = [halves[k] for k in (0, 1, 0, 0, 0, 1)] + [P()] * 2
    return jax.shard_map(
        local,
        mesh=mesh,
        in_specs=(*slopes, *shards, *shards),
        out_specs=(*halves, *shards, *shards),
        check_vma=False,
    )
```

```python
import contextlib
import math

import jax
import jax.numpy as jnp
from jax import lax
from jax.experimental import pallas as pl
from jax.experimental.pallas import tpu as pltpu
from jax.sharding import PartitionSpec as P

learn_rate = 0.025
hold_rate = 0.7
MESH = pl.DeviceIdType.MESH
SIDE = 4
PEERS = 8

UP, QUERY, KEY, MIXED, VALUE, SMALL, DOWN, ROWS = 0, 256, 320, 384, 448, 512, 528, 784

CHUNKS = (
    ("y", UP, 32, 32),
    ("z", MIXED, 80, 64),
    ("y", UP + 64, 32, 32),
    ("y", UP + 128, 32, 32),
    ("z", DOWN, 32, 32),
    ("y", UP + 192, 32, 32),
    ("z", DOWN + 64, 32, 32),
    ("y", QUERY, 64, 64),
    ("z", DOWN + 128, 32, 32),
    ("z", DOWN + 192, 32, 32),
)
GATHERS = (
    ("y", UP, 64, 64, 0),
    ("z", MIXED, 80, 64, 1),
    ("y", UP + 128, 64, 64, 2),
    ("z", DOWN, 64, 64, 4),
    ("y", QUERY, 64, 64, 3),
    ("z", DOWN + 128, 64, 64, 4),
)
COUNT = len(CHUNKS)
GROUPS = 5
PER = 6
PER_GATHER = 7
LOADS = COUNT + 8
SENDS = 9

ORDER = (
    ("soO", 0), ("soF", 0), ("soF", 1), ("soF", 2), ("soF", 6), ("soF", 3), ("sdF", 2), ("soO", 1),
    ("sdO", 1), ("sdF", 1), ("soO", 2), ("sdO", 2), ("soF", 7), ("soO", 5), ("soO", 3), ("sdF", 0),
    ("fwdF", 1), ("soF", 5), ("soF", 4), ("fwdF", 2), ("soO", 6), ("fwdF", 0), ("fwdO", 0),
    ("soO", 7), ("fwdO", 2), ("sdF", 5), ("soO", 4), ("fwdO", 1), ("soO", 9), ("soF", 8),
    ("sdF", 6), ("finF", 1), ("sdO", 0), ("fwdF", 6), ("sdF", 7), ("finF", 2), ("sdF", 3),
    ("fwdF", 3), ("finF", 0), ("fwdF", 5), ("soF", 9), ("sdF", 9), ("soO", 8), ("fwdF", 4),
    ("finO", 2), ("sdO", 9), ("finO", 1), ("Fwd", 1), ("sdF", 8), ("fwdF", 7), ("fwdF", 8),
    ("Fwd", 2), ("finO", 0), ("Fwd", 0), ("prepare", 0), ("sdO", 5), ("fwdO", 3), ("sdO", 3),
    ("sdF", 4), ("fwdF", 9), ("fwdO", 9), ("finF", 3), ("fwdO", 5), ("fwdO", 6), ("sdO", 7),
    ("finF", 5), ("sdO", 6), ("fwdO", 7), ("fwdO", 4), ("Fin", 1), ("norm", 1), ("finF", 6),
    ("finF", 7), ("sdO", 4), ("sdO", 8), ("Fin", 0), ("Fin", 2), ("norm", 0), ("finF", 4),
    ("finF", 9), ("fwdO", 8), ("finF", 8), ("finO", 3), ("Fwd", 3), ("finO", 5), ("Fwd", 5),
    ("finO", 6), ("finO", 9), ("finO", 7), ("Fwd", 7), ("Fwd", 6), ("finO", 4), ("Fwd", 4),
    ("Fwd", 9), ("finO", 8), ("Fwd", 8), ("ratio", 1), ("upd", 1), ("Fin", 3), ("Fin", 5),
    ("norm", 2), ("ratio", 0), ("upd", 0), ("Fin", 7), ("norm", 3), ("Fin", 6), ("Fin", 4),
    ("Fin", 9), ("Fin", 8), ("norm", 4), ("ownF", 1), ("xf", 1), ("xf", 0), ("ratio", 2),
    ("upd", 2), ("ownF", 0), ("far", 1), ("ratio", 3), ("upd", 4), ("lF", 1), ("ratio", 4),
    ("upd", 5), ("rF", 1), ("upd", 3), ("xf", 2), ("xf", 4), ("xf", 5), ("lF", 0), ("xf", 3),
    ("far", 2), ("far", 4), ("far", 0), ("rF", 0), ("ownF", 5), ("rF", 2), ("lF", 5), ("lF", 2),
    ("rF", 4), ("far", 5), ("keep", 0), ("far", 3), ("lF", 3), ("ownF", 2), ("fF", 1), ("fF", 2),
    ("rF", 3), ("fF", 4), ("rF", 5), ("fF", 0), ("fF", 5), ("ownF", 3), ("ownF", 4), ("lF", 4),
    ("fF", 3), ("end", 2), ("end", 5), ("end", 0), ("end", 1), ("end", 3), ("end", 4),
)


SPAN, BASE = 251 * math.log(2.0), 125 * math.log(2.0)
ONE, TWO, FOUR, EIGHT = 4.0, 8.0, 16.0, 32.0


def to_wire(x, bound):
    level = jnp.exp(jnp.log(jnp.abs(x)) * (1.0 / 6.0) + math.log(SPAN * bound ** (-1.0 / 6.0)))
    size = jnp.exp(level - BASE)
    return jnp.where(x < 0.0, -size, size).astype(jnp.bfloat16)


def from_wire(c, bound):
    c = c.astype(jnp.float32)
    level = (jnp.log(jnp.abs(c)) + BASE) * (bound ** (1.0 / 6.0) / SPAN)
    square = level * level
    size = square * square * square
    return jnp.where(c < 0.0, -size, size)


def low_lanes(shape):
    return lax.broadcasted_iota(jnp.int32, shape, len(shape) - 1) < 64


def turn(x):
    return pltpu.roll(x, 64, 1)


def beside(x):
    half = x.shape[1] // 2
    return jnp.concatenate([x[:, :half], x[:, half:]], axis=0).T


def stage(name):
    return contextlib.nullcontext()


def exchange_kernel(*refs):
    slopes, given, refs = refs[:8], refs[8:24], refs[24:]
    gathered, wide_down, wide_mixed, small_norm, small_bias, refs = *refs[:5], refs[5:]
    following, new, refs = refs[:8], refs[8:16], refs[16:]
    params, states, refs = refs[:8], refs[8:16], refs[16:]
    exchange(
        slopes,
        given,
        gathered,
        (wide_down, wide_mixed),
        (small_norm, small_bias),
        following,
        new,
        params,
        states,
        *refs,
    )


def exchange(
    slopes,
    given,
    gathered,
    wides,
    small_halves,
    following,
    new,
    params,
    states,
    scaled,
    mine,
    raw_norm,
    raw_bias,
    packed_param,
    packed_state,
    send_op,
    send_dir,
    send_fwd,
    recv_op,
    both,
    first_sum,
    send_op2,
    send_dir2,
    send_fwd2,
    recv_op2,
    both2,
    mean,
    squares,
    load_sem,
    send_sem,
    recv_sem,
    grecv_sem,
    nrecv_sem,
):
    up, down, query, key, value, mixed, norm, bias = slopes
    recv_rest = recv_dir, recv_fwd = both.at[0], both.at[1]
    recv_rest2 = recv_dir2, recv_fwd2 = both2.at[0], both2.at[1]
    replica = lax.axis_index("replica")
    model = lax.axis_index("model")
    z, y = replica // SIDE, replica % SIDE

    def place(axis, step):
        if axis == "y":
            return (z * SIDE + (y + step) % SIDE, model)
        return (((z + step) % SIDE) * SIDE + y, model)

    position = {"y": y, "z": z}
    other = {"y": "z", "z": "y"}

    def all_of(ref, sem):
        pltpu.make_async_copy(ref, ref, sem).wait()

    def load(number, pairs):
        for src, dst in pairs:
            pltpu.make_async_copy(src, dst, load_sem.at[number]).start()

    def loaded(number, *refs):
        for k, ref in enumerate(refs):
            all_of(ref, load_sem.at[number + k])

    def whole(chunk, table=CHUNKS):
        _, row, first, second, *_ = table[chunk]
        return pl.ds(row, first + second)

    def up_part(part, columns):
        return [
            (
                up.at[:, :, pl.ds(32 * part, 32), pl.ds(128 * c, 128)],
                mine.at[:, :, pl.ds(UP + 128 * part + 32 * c, 32), :],
            )
            for c in columns
        ]

    def columns(array, row, start, length):
        return [
            (
                array.at[:, pl.ds(start, length), pl.ds(128 * k, 128)],
                mine.at[k // 2, pl.ds(2 * (k % 2), 2), pl.ds(row + start, length), :],
            )
            for k in range(8)
        ]

    load(0, up_part(0, (0, 1)))
    load(
        1,
        [
            *columns(mixed, MIXED, 0, 64),
            (value, mine.at[:, :, pl.ds(VALUE, 64), :]),
        ],
    )
    load(COUNT, [(norm, raw_norm)])
    load(COUNT + 1, [(bias, raw_bias)])
    barrier = pltpu.get_barrier_semaphore()
    for axis in ("y", "z"):
        for step in (1, SIDE - 1):
            pl.semaphore_signal(barrier, 1, device_id=place(axis, step), device_id_type=MESH)
    for step in range(1, PEERS):
        pl.semaphore_signal(
            barrier, 1, device_id=(replica, (model + step) % PEERS), device_id_type=MESH
        )
    waiting = [True]

    def load_rest():
        load(2, up_part(0, (2, 3)))
        load(3, up_part(1, (0, 1)))
        load(4, columns(down, DOWN, 0, 64))
        load(5, up_part(1, (2, 3)))
        load(6, columns(down, DOWN, 64, 64))
        load(7, [(query, mine.at[:, :, pl.ds(QUERY, 64), :]), (key, mine.at[:, :, pl.ds(KEY, 64), :])])
        load(8, columns(down, DOWN, 128, 64))
        load(9, columns(down, DOWN, 192, 64))
        held = [*zip(given, (*params, *states))]
        load(COUNT + 2, [held[k] for k in (0, 1, 8, 9)])
        load(COUNT + 3, [held[k] for k in (2, 3, 4, 5, 10, 11, 12, 13)])
        for k, pair in enumerate((held[6], held[7], held[14], held[15])):
            load(COUNT + 4 + k, [pair])

    def pack_small():
        low = low_lanes((1, 128))
        for pair in range(8):
            lanes = pl.ds(128 * pair, 128)
            zz, yy = (2 * pair) // SIDE, (2 * pair) % SIDE
            a = raw_norm[:, lanes] * 0.5
            b = raw_bias[:, lanes] * 0.5
            mine[zz, yy, pl.ds(SMALL, 16), :] = jnp.broadcast_to(
                jnp.where(low, a, turn(b)), (16, 128)
            )
            mine[zz, yy + 1, pl.ds(SMALL, 16), :] = jnp.broadcast_to(
                jnp.where(low, turn(a), b), (16, 128)
            )

    def halves(chunk):
        _, row, first, second = CHUNKS[chunk]
        return pl.ds(row, first), pl.ds(row + first, second)

    def pair_of(chunk, part):
        own = position[other[CHUNKS[chunk][0]]] // 2
        return 2 * own if part else 2 - 2 * own

    def share(axis, at, b):
        if axis == "y":
            return mine.at[b, at]
        return mine.at[at, b]

    def copies(chunk, number, part=0):
        axis = CHUNKS[chunk][0]
        a, b = halves(chunk)
        second = number >= 6
        if second:
            axis = other[axis]
            sources, targets = (send_op2, send_dir2, send_fwd2), (recv_op2, *recv_rest2)
        else:
            sources, targets = (send_op, send_dir, send_fwd), (recv_op, *recv_rest)
        kind, half = divmod(number % 6, 2)
        rows = b if half else a
        at = (rows, slice(None))
        if not second:
            at = (pl.ds(pair_of(chunk, part), 2), *at)
        step = (SIDE - 1, 1)[half] if kind != 1 else (1, SIDE - 1)[half]
        if second:
            arrival = 4 if kind == 0 else 5
        else:
            arrival = 2 * part + (kind > 0)
        return pltpu.make_async_remote_copy(
            src_ref=sources[kind].at[at],
            dst_ref=targets[kind].at[at],
            send_sem=send_sem.at[3 * second + kind],
            recv_sem=recv_sem.at[chunk * PER + arrival],
            device_id=place(axis, step),
            device_id_type=MESH,
        )

    ready = set()

    def send(chunk, part):
        if chunk not in ready:
            ready.add(chunk)
            if chunk == 1:
                loaded(chunk, mine.at[:, :, pl.ds(MIXED, 128)])
                loaded(COUNT, raw_norm, raw_bias)
                pack_small()
            else:
                loaded(chunk, mine.at[:, :, whole(chunk)])
        axis = CHUNKS[chunk][0]
        far = (position[axis] + 2) % SIDE
        pair, rows = pair_of(chunk, part), whole(chunk)

        def op(i, _):
            send_op[pair + i, rows, :] = to_wire(share(axis, far, pair + i)[rows, :], ONE)
            return 0

        lax.fori_loop(0, 2, op, 0)
        if waiting:
            waiting.pop()
            load_rest()
            pl.semaphore_wait(barrier, 4 + PEERS - 1)
        copies(chunk, 0, part).start()
        copies(chunk, 1, part).start()

    def send_direct(chunk, part):
        axis = CHUNKS[chunk][0]
        p = position[axis]
        a, b = halves(chunk)
        right, left = (p + 1) % SIDE, (p + SIDE - 1) % SIDE
        pair = pair_of(chunk, part)

        def direct(i, _):
            send_dir[pair + i, a, :] = to_wire(share(axis, right, pair + i)[a, :], ONE)
            send_dir[pair + i, b, :] = to_wire(share(axis, left, pair + i)[b, :], ONE)
            return 0

        lax.fori_loop(0, 2, direct, 0)
        copies(chunk, 2, part).start()
        copies(chunk, 3, part).start()

    def forward(chunk, part):
        axis = CHUNKS[chunk][0]
        a, b = halves(chunk)
        right, left = (position[axis] + 1) % SIDE, (position[axis] + SIDE - 1) % SIDE
        pair = pair_of(chunk, part)
        all_of(recv_op.at[pl.ds(pair, 2), whole(chunk)], recv_sem.at[chunk * PER + 2 * part])
        for number, rows, at in ((4, a, left), (5, b, right)):

            def body(i, _):
                own = share(axis, at, pair + i)[rows, :]
                term = from_wire(recv_op[pair + i, rows, :], ONE) + own
                send_fwd[pair + i, rows, :] = to_wire(term, TWO)
                return 0

            lax.fori_loop(0, 2, body, 0)
            copies(chunk, number, part).start()

    def finish(chunk, part):
        axis, row, first, second = CHUNKS[chunk]
        length = first + second
        p = position[axis]
        pair = pair_of(chunk, part)
        all_of(
            both.at[:, pl.ds(pair, 2), whole(chunk)], recv_sem.at[chunk * PER + 2 * part + 1]
        )

        def summed(i, rows):
            return (
                share(axis, p, i)[rows, :]
                + from_wire(recv_dir[i, rows, :], ONE)
                + from_wire(recv_fwd[i, rows, :], TWO)
            )

        paired = 64 if axis == "z" else 0
        if paired:
            rows = pl.ds(row, 64)
            low = low_lanes((64, 128))
            upper, lower = summed(pair, rows), summed(pair + 1, rows)
            first_sum[pair, rows, :] = jnp.where(low, upper, turn(lower))
            first_sum[pair + 1, rows, :] = jnp.where(low, turn(upper), lower)
        if paired < length:

            def plain(i, _):
                rows = pl.ds(row + paired, length - paired)
                first_sum[pair + i, rows, :] = summed(pair + i, rows)
                return 0

            lax.fori_loop(0, 2, plain, 0)

        p = position[other[axis]]
        a, b = halves(chunk)
        far, right, left = (p + 2) % SIDE, (p + 1) % SIDE, (p + SIDE - 1) % SIDE
        if part == 0:
            rows = whole(chunk)
            send_op2[rows, :] = to_wire(first_sum[far, rows, :], FOUR)
            copies(chunk, 6).start()
            copies(chunk, 7).start()
        else:
            send_dir2[a, :] = to_wire(first_sum[right, a, :], FOUR)
            copies(chunk, 8).start()
            send_dir2[b, :] = to_wire(first_sum[left, b, :], FOUR)
            copies(chunk, 9).start()

    def second_forward(chunk):
        p = position[other[CHUNKS[chunk][0]]]
        a, b = halves(chunk)
        right, left = (p + 1) % SIDE, (p + SIDE - 1) % SIDE
        all_of(recv_op2.at[whole(chunk)], recv_sem.at[chunk * PER + 4])
        for number, rows, at in ((6, a, left), (7, b, right)):
            part = from_wire(recv_op2[rows, :], FOUR) + first_sum[at, rows, :]
            send_fwd2[rows, :] = to_wire(part, EIGHT)
            copies(chunk, 4 + number).start()

    def second_finish(chunk):
        p = position[other[CHUNKS[chunk][0]]]
        all_of(both2.at[:, whole(chunk)], recv_sem.at[chunk * PER + 5])
        for rows in halves(chunk):
            mean[rows, :] = (
                first_sum[p, rows, :]
                + from_wire(recv_dir2[rows, :], FOUR)
                + from_wire(recv_fwd2[rows, :], EIGHT)
            ) * (SIDE * SIDE) ** (-0.5)

    def prepare():
        loaded(COUNT + 2, first_sum.at[0:2, 0:512], mean.at[0:512])
        loaded(COUNT + 4, params[6], params[7], states[6], states[7])
        for number, row, length in ((5, MIXED, 64), (1, DOWN, 256)):
            packed_param[pl.ds(row, length), :] = beside(params[number][...])
            packed_state[pl.ds(row, length), :] = beside(states[number][...])

    def row_squares(row, width, param, top, height):
        got = jnp.zeros((height, 128), jnp.float32)
        own = jnp.zeros((height, 128), jnp.float32)
        for c in range(width):
            m = mean[pl.ds(row + height * c, height), :]
            w = param[pl.ds(top, height), pl.ds(128 * c, 128)]
            got, own = got + m * m, own + w * w
        rest = [jnp.zeros((64 - height, 128), jnp.float32)] if height < 64 else []
        both = jnp.concatenate([got, *rest, own, *rest], axis=0)
        return jnp.sum(both, axis=1, keepdims=True)

    def column_squares(row, length):
        m = mean[pl.ds(row, length), :]
        w = packed_param[pl.ds(row, length), :]
        got = jnp.sum(m * m, axis=0, keepdims=True)
        own = jnp.sum(w * w, axis=0, keepdims=True)
        got, own = got + turn(got), own + turn(own)
        return jnp.where(low_lanes((1, 128)), got, own)

    def norm_copy(group, step):
        return pltpu.make_async_remote_copy(
            src_ref=squares.at[group, 0],
            dst_ref=squares.at[group, step],
            send_sem=send_sem.at[8],
            recv_sem=nrecv_sem.at[group],
            device_id=(replica, (model + step) % PEERS),
            device_id_type=MESH,
        )

    def norm_send(group):
        by_rows, by_columns = [], []
        if group in (0, 2):
            by_rows = [row_squares(UP + 64 * group, 4, params[0], 16 * group, 32)]
        if group == 1:
            by_rows = [row_squares(VALUE, 1, params[4], 0, 64)]
            by_columns = [column_squares(MIXED, 64)]
        if group == 3:
            by_rows = [
                row_squares(QUERY, 1, params[2], 0, 64),
                row_squares(KEY, 1, params[3], 0, 64),
            ]
        if group == 4:
            by_columns = [column_squares(DOWN, 256)]
        tile = jnp.zeros((8, 128), jnp.float32)
        if by_rows:
            lane = lax.broadcasted_iota(jnp.int32, (128, 128), 1)
            block = jnp.zeros((128, 128), jnp.float32)
            for k, column in enumerate(by_rows):
                block = jnp.where(lane == k, column, block)
            tile = block.T[0:8]
        sub = lax.broadcasted_iota(jnp.int32, (8, 128), 0)
        for k, line in enumerate(by_columns):
            tile = jnp.where(sub == len(by_rows) + k, line, tile)
        squares[group, 0] = tile
        for step in range(1, PEERS):
            norm_copy(group, step).start()

    ratios = {}

    def norm_ratios(group):
        all_of(squares.at[group, 1:PEERS], nrecv_sem.at[group])
        total = squares[group, 0]
        for step in range(1, PEERS):
            total = total + squares[group, step]
        low = low_lanes((8, 128))
        back = turn(total)
        got, own = jnp.where(low, total, back), jnp.where(low, back, total)
        ratio = jnp.sqrt(own) * lax.rsqrt(got + 1e-06)
        across = ratio
        down_rows = jnp.concatenate([ratio] * 16, axis=0).T if group != 4 else None
        ratios[group] = across, down_rows

    def stepped(m, param, state):
        state_new = hold_rate * state + (1.0 - hold_rate) * m * m
        return param - learn_rate * m * lax.rsqrt(state_new + 1e-06), state_new

    def updated(rows, m, param, state):
        scaled[rows, :] = m
        gathered[z, y, rows, :] = stepped(m, param, state)[0].astype(jnp.bfloat16)

    def row_update(row, width, ratio, number, top, height):
        for c in range(width):
            rows = pl.ds(row + height * c, height)
            at = (pl.ds(top, height), pl.ds(128 * c, 128))
            updated(rows, mean[rows, :] * ratio, params[number][at], states[number][at])

    def column_update(row, length, ratio):
        rows = pl.ds(row, length)
        updated(rows, mean[rows, :] * ratio, packed_param[rows, :], packed_state[rows, :])

    def update(chunk):
        across, down_rows = ratios[GATHERS[chunk][4]]
        if chunk in (0, 2):
            row_update(UP + 64 * chunk, 4, down_rows[0:32, 0:1], 0, 16 * chunk, 32)
        if chunk == 1:
            column_update(MIXED, 64, across[1:2])
            row_update(VALUE, 1, down_rows[0:64, 0:1], 4, 0, 64)
            small = pl.ds(SMALL, 16)
            updated(
                small,
                mean[small, :] * 2.0,
                jnp.concatenate([params[6][...], params[7][...]], axis=1),
                jnp.concatenate([states[6][...], states[7][...]], axis=1),
            )
        if chunk == 4:
            row_update(QUERY, 1, down_rows[0:64, 0:1], 2, 0, 64)
            row_update(KEY, 1, down_rows[0:64, 1:2], 3, 0, 64)
        if chunk in (3, 5):
            column_update(GATHERS[chunk][1], 128, across[0:1])

    def keep():
        def step(number, at, m):
            following[number][at], new[number][at] = stepped(
                m, params[number][at], states[number][at]
            )

        for part in range(2):
            for c in range(4):
                at = (pl.ds(32 * part, 32), pl.ds(128 * c, 128))
                step(0, at, scaled[pl.ds(UP + 128 * part + 32 * c, 32), :])
        everything = (slice(None), slice(None))
        for number, row in ((2, QUERY), (3, KEY), (4, VALUE)):
            step(number, everything, scaled[pl.ds(row, 64), :])
        for number, row, length in ((1, DOWN, 256), (5, MIXED, 64)):
            turned = scaled[pl.ds(row, length), :].T
            step(number, everything, jnp.concatenate([turned[:64], turned[64:]], axis=1))
        line = scaled[pl.ds(SMALL, 1), :]
        step(6, everything, line[:, :64])
        step(7, everything, turn(line)[:, :64])

    def gather_copies(chunk, number):
        name, row, first, second, _ = GATHERS[chunk]
        a, b = pl.ds(row, first), pl.ds(row + first, second)
        up_way = number % 2 == 0
        step = 1 if up_way else SIDE - 1
        behind = SIDE - 1 if up_way else 1
        p, q = position[name], position[other[name]]
        axis = name
        rows = whole(chunk, GATHERS)
        if number < 4:
            axis = other[name]
            if number >= 2:
                rows, q = (b if up_way else a), (q + behind) % SIDE
        else:
            block = (number - 4) // 2 % 4
            q = (q + (0, SIDE - 1, 1, 2)[block]) % SIDE
            if number >= 12:
                rows, p = (b if up_way else a), (p + behind) % SIDE
        ref = gathered.at[q, p, rows] if name == "y" else gathered.at[p, q, rows]
        arrival = min(number // 2, 6)
        return pltpu.make_async_remote_copy(
            src_ref=ref,
            dst_ref=ref,
            send_sem=send_sem.at[6 if number < 4 else 7],
            recv_sem=grecv_sem.at[chunk * PER_GATHER + arrival],
            device_id=place(axis, step),
            device_id_type=MESH,
        )

    def pass_on(chunk, arrival, started):
        rows = whole(chunk, GATHERS)
        if arrival is not None:
            ref = gathered.at[0, 0:2, rows]
            if arrival == 1:
                ref = gathered.at[0, 0, rows]
            if arrival == 6:
                ref = gathered.at[0, :, rows]
            all_of(ref, grecv_sem.at[chunk * PER_GATHER + arrival])
        for number in started:
            gather_copies(chunk, number).start()

    def widen(chunk):
        number, row, start, length = {
            1: (1, MIXED, 0, 64),
            3: (0, DOWN, 0, 128),
            5: (0, DOWN, 128, 128),
        }[chunk]
        out = wides[number]
        half = out.shape[0] // 2
        low = low_lanes((length, 128))
        rows = pl.ds(row + start, length)
        for pair in range(8):
            lanes = pl.ds(128 * pair, 128)
            zz, yy = (2 * pair) // SIDE, (2 * pair) % SIDE
            a = gathered[zz, yy, rows, :].astype(jnp.float32)
            b = gathered[zz, yy + 1, rows, :].astype(jnp.float32)
            out[pl.ds(start, length), lanes] = jnp.where(low, a, turn(b)).astype(jnp.bfloat16)
            out[pl.ds(half + start, length), lanes] = jnp.where(low, turn(a), b).astype(
                jnp.bfloat16
            )

    def small_out():
        sub = lax.broadcasted_iota(jnp.int32, (8, 128), 0)
        low = low_lanes((1, 128))
        lines = [jnp.zeros((8, 128), jnp.float32)] * 2
        for pair in range(8):
            zz, yy = (2 * pair) // SIDE, (2 * pair) % SIDE
            a = gathered[zz, yy, pl.ds(SMALL, 16), :].astype(jnp.float32)[0:1]
            b = gathered[zz, yy + 1, pl.ds(SMALL, 16), :].astype(jnp.float32)[0:1]
            lines[0] = jnp.where(sub == pair, jnp.where(low, a, turn(b)), lines[0])
            lines[1] = jnp.where(sub == pair, jnp.where(low, turn(a), b), lines[1])
        for k in range(2):
            small_halves[k][...] = lines[k].astype(jnp.bfloat16)

    def end(chunk):
        pass_on(chunk, 6, ())
        if chunk in (1, 3, 5):
            widen(chunk)
        if chunk == 1:
            small_out()

    def act(name, k):
        part = int(name.endswith("O"))
        if name in ("soF", "soO"):
            send(k, part)
        elif name in ("sdF", "sdO"):
            send_direct(k, part)
        elif name in ("fwdF", "fwdO"):
            forward(k, part)
        elif name in ("finF", "finO"):
            finish(k, part)
        elif name == "Fwd":
            second_forward(k)
        elif name == "Fin":
            second_finish(k)
        elif name == "prepare":
            prepare()
        elif name == "keep":
            keep()
        elif name == "norm":
            norm_send(k)
        elif name == "ratio":
            norm_ratios(k)
        elif name == "upd":
            update(k)
            pass_on(k, None, (0, 1, 4, 5))
        elif name == "xf":
            pass_on(k, 0, (2, 3, 6, 7, 8, 9))
        elif name == "far":
            pass_on(k, 1, (10, 11))
        elif name == "end":
            end(k)
        else:
            block = ("own", "l", "r", "f").index(name[:-1])
            pass_on(k, 2 + block, (12 + 2 * block, 13 + 2 * block))

    for name, k in ORDER:
        with stage(f"{name}_{k}"):
            act(name, k)

    with stage("sent"):
        for k, ref in enumerate((send_op, send_dir, send_fwd, send_op2, send_dir2, send_fwd2)):
            all_of(ref, send_sem.at[k])
        all_of(gathered.at[0, 0:3], send_sem.at[6])
        all_of(gathered.at[0:3], send_sem.at[7])
        all_of(squares.at[:, 1:PEERS], send_sem.at[8])


def output_kernel(*refs):
    gathered, laid, refs = refs[0], refs[1:21], refs[21:]
    half, rest, sem = refs[:8], refs[8:24], refs[24]
    up = [
        (
            gathered.at[:, pl.ds(UP + 128 * part + 32 * c, 32), :],
            half[0].at[:, pl.ds(32 * part, 32), pl.ds(128 * c, 128)],
        )
        for part in range(2)
        for c in range(4)
    ]
    square = [
        (gathered.at[:, pl.ds(row, 64), :], half[number])
        for number, row in ((2, QUERY), (3, KEY), (4, VALUE))
    ]
    kept = [*zip(laid[4:], rest)]
    groups = [
        (up, gathered.at[:, pl.ds(UP, 256)]),
        ([(laid[0], half[1])], laid[0]),
        (square, gathered.at[:, pl.ds(0, 192)]),
        ([kept[k] for k in (0, 1, 8, 9)], gathered.at[0:4, 0:512]),
        ([kept[k] for k in (2, 3, 4, 5, 10, 11, 12, 13)], gathered.at[0:2, 0:512]),
        *[([pair], pair[0]) for pair in zip(laid[1:4], half[5:])],
        *[([kept[k]], kept[k][0]) for k in (6, 7, 14, 15)],
    ]
    for k, (pairs, _) in enumerate(groups):
        for src, dst in pairs:
            pltpu.make_async_copy(src, dst, sem.at[k]).start()
    for k, (_, ref) in enumerate(groups):
        pltpu.make_async_copy(ref, ref, sem.at[k]).wait()


def stay(*arrays):
    return [pltpu.with_memory_space_constraint(a, pltpu.HBM) for a in arrays]


def local(*arrays):
    slopes, params, states = arrays[:8], arrays[8:16], arrays[16:]
    up, down, query, key, value, mixed, norm, bias = slopes

    def shown(group):
        up, down, query, key, value, mixed, norm, bias = group
        return up, down.T, query, key, value, mixed.T, norm[None], bias[None]

    params, states = shown(params), shown(states)
    vmem = pl.BlockSpec(memory_space=pltpu.VMEM)
    anywhere = pl.BlockSpec(memory_space=pl.ANY)
    f32, bf16 = jnp.float32, jnp.bfloat16
    wire = pltpu.VMEM((SIDE, ROWS, 128), bf16)
    wire2 = pltpu.VMEM((ROWS, 128), bf16)
    dma = pltpu.SemaphoreType.DMA
    held = [pltpu.VMEM(a.shape, f32) for a in params]
    gathered, *laid = pl.pallas_call(
        exchange_kernel,
        out_shape=(
            pltpu.VMEM((SIDE, SIDE, ROWS, 128), bf16),
            pltpu.VMEM((512, 1024), bf16),
            pltpu.VMEM((128, 1024), bf16),
            pltpu.VMEM((8, 128), bf16),
            pltpu.VMEM((8, 128), bf16),
            *held,
            *held,
        ),
        in_specs=[pl.BlockSpec(memory_space=pltpu.HBM)] * 24,
        out_specs=(vmem,) * 21,
        scratch_shapes=[
            *held,
            *held,
            pltpu.VMEM((ROWS, 128), f32),
            pltpu.VMEM((SIDE, SIDE, ROWS, 128), f32),
            pltpu.VMEM((1, 1024), f32),
            pltpu.VMEM((1, 1024), f32),
            pltpu.VMEM((ROWS, 128), f32),
            pltpu.VMEM((ROWS, 128), f32),
            *[wire] * 4,
            pltpu.VMEM((2, SIDE, ROWS, 128), bf16),
            pltpu.VMEM((SIDE, ROWS, 128), f32),
            *[wire2] * 4,
            pltpu.VMEM((2, ROWS, 128), bf16),
            pltpu.VMEM((ROWS, 128), f32),
            pltpu.VMEM((GROUPS, PEERS, 8, 128), f32),
            dma((LOADS,)),
            dma((SENDS,)),
            dma((COUNT * PER,)),
            dma((len(GATHERS) * PER_GATHER,)),
            dma((GROUPS,)),
        ],
        compiler_params=pltpu.CompilerParams(
            collective_id=0, has_side_effects=True, vmem_limit_bytes=40 * 2**20
        ),
        name="exchange",
    )(
        *stay(
            up.reshape(SIDE, SIDE, 64, 512),
            down.reshape(2, 256, 1024),
            query.reshape(SIDE, SIDE, 64, 128),
            key.reshape(SIDE, SIDE, 64, 128),
            value.reshape(SIDE, SIDE, 64, 128),
            mixed.reshape(2, 64, 1024),
            norm,
            bias,
            *params,
            *states,
        )
    )
    own = [jax.ShapeDtypeStruct(a.shape, f32) for a in params]
    full = [
        jax.ShapeDtypeStruct(s, bf16)
        for s in (
            (16, 64, 512),
            (512, 1024),
            (16, 64, 128),
            (16, 64, 128),
            (16, 64, 128),
            (128, 1024),
            (8, 128),
            (8, 128),
        )
    ]
    out = pl.pallas_call(
        output_kernel,
        out_shape=(*full, *own, *own),
        in_specs=[vmem] * 21,
        out_specs=(anywhere,) * 24,
        scratch_shapes=[dma((5 + 3 + 4,))],
        compiler_params=pltpu.CompilerParams(vmem_limit_bytes=8 * 2**20),
        name="outputs",
    )(gathered.reshape(SIDE * SIDE, ROWS, 128), *laid)
    half, following, new = out[:8], out[8:16], out[16:]
    half_up, half_down, half_query, half_key, half_value, half_mixed, half_norm, half_bias = half

    def back(group):
        up, down, query, key, value, mixed, norm, bias = group
        return up, down.T, query, key, value, mixed.T, norm[0], bias[0]

    return (
        half_up.reshape(1024, 512),
        half_down,
        half_query.reshape(1024, 128),
        half_key.reshape(1024, 128),
        half_value.reshape(1024, 128),
        half_mixed,
        half_norm.reshape(1024),
        half_bias.reshape(1024),
        *back(following),
        *back(new),
    )


def solution(mesh):
    def along(split):
        return [
            P(*(("replica", "model") if dim == 0 else ("model", "replica"))[:2])
            if dim < 2
            else P("replica")
            for dim in split
        ]

    shards = along((0, 1, 0, 0, 0, 1, 2, 2))
    slopes = [P("replica", None, "model"), P("replica", "model", None)]
    slopes = [slopes[k] for k in (0, 1, 0, 0, 0, 1)] + [P("replica", None)] * 2
    halves = [P(None, "model"), P("model", None)]
    halves = [halves[k] for k in (0, 1, 0, 0, 0, 1)] + [P()] * 2
    return jax.shard_map(
        local,
        mesh=mesh,
        in_specs=(*slopes, *shards, *shards),
        out_specs=(*halves, *shards, *shards),
        check_vma=False,
    )
```
